128 devices in a mesh: fsdp: 32 (over z, y, x_hi), sp: 4 (over x_lo, core).
Axes of the slice: x: 4 (x_hi: 2, x_lo: 2; x = x_hi * 2 + x_lo), y: 4, z: 4, core: 2. Of those that a mesh axis runs over, the one named last changes fastest.
Arguments:
- tokens: bfloat16 [32, 512, 1536], P('fsdp', 'sp'), may hold values from -6 to 6
- modulation: float32 [32, 1, 6, 1536], P('fsdp'), may hold values from -4 to 4
- w_qkv: bfloat16 [1, 1536, 3, 1536], P(None, 'fsdp', None, 'sp'), may hold values from -0.15625 to 0.15625
- w_out: bfloat16 [1, 1536, 1536], P(None, 'sp', 'fsdp'), may hold values from -0.15625 to 0.15625
- w_in: bfloat16 [1, 1536, 6144], P(None, 'fsdp', 'sp'), may hold values from -0.15625 to 0.15625
- w_back: bfloat16 [1, 6144, 1536], P(None, 'sp', 'fsdp'), may hold values from -0.078125 to 0.078125
- out_grad: bfloat16 [32, 512, 1536], P('fsdp', 'sp'), may hold values from -6 to 6
Outputs:
- final_out: bfloat16 [32, 512, 1536], P('fsdp', 'sp')
- input_grad: float32 [32, 512, 1536], P('fsdp', 'sp')
- grad_qkv: float32 [1, 1536, 3, 1536], P(None, 'fsdp', None, 'sp')
- grad_out: float32 [1, 1536, 1536], P(None, 'sp', 'fsdp')
- grad_in: float32 [1, 1536, 6144], P(None, 'fsdp', 'sp')
- grad_back: float32 [1, 6144, 1536], P(None, 'sp', 'fsdp')
The draws below stay inside these ranges and needn't reach their ends.
All inputs are finite; a program needn't handle non-finite values.
Results may differ from the reference program's by a relative error of at most 0.03.
Values may be sent and summed in bfloat16 or wider, within the bound.
A program may use at most 128 MiB of HBM per device.

```python
import math
import jax
import jax.numpy as jnp
from jax import lax

D = 1536
HEAD_DIM = 128
FF = 6144
LAYERS = 1
SEQ = 512
BATCH = 32
N_FSDP = 32


def block_scale(rng, dims, shards, smallest, top_value):
    def one(axis_at, parts):
        heights = jax.random.uniform(jax.random.fold_in(jax.random.fold_in(rng, 6), axis_at), (parts,), jnp.float32, smallest / len(shards), top_value / len(shards))
        return jnp.repeat(jnp.exp(heights), dims[axis_at] // parts).reshape((-1,) + (1,) * (len(dims) - axis_at - 1))

    gain = one(*shards[0])
    for cut in shards[1:]:
        gain = gain * one(*cut)
    return gain


def bell_draw(stream_key, shape, spread, limit, cuts=(), dtype=jnp.bfloat16):
    drawn = spread * jax.random.normal(stream_key, shape, jnp.float32)
    if cuts:
        drawn = drawn * block_scale(stream_key, shape, cuts, -0.22, 0.18)
    return jnp.clip(drawn, -limit, limit).astype(dtype)


def setup_inputs(seed: int = 0) -> dict:
    keys = jax.random.split(jax.random.key(seed), 8)
    tokens = bell_draw(keys[0], (BATCH, SEQ, D), 1.0, 6.0, ((0, 32), (1, 4)))
    modulation = bell_draw(keys[1], (BATCH, LAYERS, 6, D), 1.0, 4.0, ((0, 32),), jnp.float32)
    w_qkv = bell_draw(keys[2], (LAYERS, D, 3, D), D ** -0.5, 0.15625, ((1, 32), (3, 4)))
    w_out = bell_draw(keys[3], (LAYERS, D, D), D ** -0.5, 0.15625, ((1, 4), (2, 32)))
    w_in = bell_draw(keys[4], (LAYERS, D, FF), D ** -0.5, 0.15625, ((1, 32), (2, 4)))
    w_back = bell_draw(keys[5], (LAYERS, FF, D), FF ** -0.5, 0.078125, ((1, 4), (2, 32)))
    out_grad = bell_draw(keys[6], (BATCH, SEQ, D), 1.0, 6.0, ((0, 32), (1, 4)))
    return dict(tokens=tokens, modulation=modulation, w_qkv=w_qkv, w_out=w_out, w_in=w_in, w_back=w_back, out_grad=out_grad)


ln_eps = 1e-06
temper = 2.5
block_limit = 512

def normalize(stream):
    mean_part = lax.optimization_barrier(jnp.mean(stream, axis=-1, keepdims=True))
    centred = stream - mean_part
    rstd = lax.rsqrt(lax.optimization_barrier(jnp.mean(centred * centred, axis=-1, keepdims=True)) + ln_eps)
    return (centred * rstd, rstd)

def norm_back(normed, rstd, incoming):
    first = lax.optimization_barrier(jnp.mean(incoming, axis=-1, keepdims=True))
    second = lax.optimization_barrier(jnp.mean(incoming * normed, axis=-1, keepdims=True))
    return rstd * (incoming - first - normed * second)

def gelu_tanh(hidden):
    return jax.nn.gelu(hidden, approximate=True)

def project(left, weight):
    flat_rows = left.reshape(-1, left.shape[-1])
    result = jnp.dot(flat_rows, weight, preferred_element_type=jnp.float32)
    return result.reshape(left.shape[:-1] + (weight.shape[1],))

def project_back(left, weight):
    flat_rows = left.reshape(-1, left.shape[-1])
    result = lax.dot_general(flat_rows, weight, (((1,), (1,)), ((), ())), preferred_element_type=jnp.float32)
    return result.reshape(left.shape[:-1] + (weight.shape[0],))

def group_grad(left, right, grad_scale):
    width_left = left.shape[-1]
    width_right = right.shape[-1]
    left_groups = left.reshape(N_FSDP, -1, width_left)
    right_groups = right.reshape(N_FSDP, -1, width_right)

    def add_group(total, pair):
        left_part, right_part = pair
        term = lax.dot_general(left_part, right_part, (((0,), (0,)), ((), ())), preferred_element_type=jnp.float32) * grad_scale
        rounded = lax.optimization_barrier(term.astype(jnp.bfloat16))
        return (total + rounded.astype(jnp.float32), None)
    total, unused = lax.scan(add_group, jnp.zeros((width_left, width_right), jnp.float32), (left_groups, right_groups))
    return total

def split_heads(packed, head_count):
    return packed.reshape(packed.shape[:-1] + (head_count, packed.shape[-1] // head_count))

def heads_major(tensor):
    videos, seq_len, head_count, head_width = tensor.shape
    return tensor.transpose(0, 2, 1, 3).reshape(videos * head_count, seq_len, head_width)

def heads_minor(tensor, videos):
    merged, seq_len, head_width = tensor.shape
    return tensor.reshape(videos, merged // videos, seq_len, head_width).transpose(0, 2, 1, 3)

def attend_head(triple):
    queries, key_rows, values = triple
    seq_len, head_width = queries.shape
    block_size = min(block_limit, seq_len)
    score_factor = temper / math.sqrt(head_width)
    values_wide = values.astype(jnp.float32)

    def one_block(query_rows):
        scores = jnp.dot(query_rows, key_rows.T, preferred_element_type=jnp.float32) * score_factor
        softmaxed = jax.nn.softmax(scores, axis=-1)
        return jnp.dot(softmaxed, values_wide, precision=lax.Precision.HIGHEST).astype(jnp.bfloat16)
    attended = lax.map(one_block, queries.reshape(seq_len // block_size, block_size, head_width))
    return attended.reshape(seq_len, head_width)

def attend_back(quadruple):
    queries, key_rows, values, upstream = quadruple
    seq_len, head_width = queries.shape
    block_size = min(block_limit, seq_len)
    score_factor = temper / math.sqrt(head_width)
    keys_wide = key_rows.astype(jnp.float32)

    def one_block(running, block_pair):
        query_rows, grad_rows = block_pair
        scores = jnp.dot(query_rows, key_rows.T, preferred_element_type=jnp.float32) * score_factor
        softmaxed = jax.nn.softmax(scores, axis=-1)
        dprobs = jnp.dot(grad_rows, values.T, preferred_element_type=jnp.float32)
        dscores = softmaxed * (dprobs - lax.optimization_barrier(jnp.sum(softmaxed * dprobs, axis=-1, keepdims=True))) * score_factor
        dquery = jnp.dot(dscores, keys_wide, precision=lax.Precision.HIGHEST)
        grad_keys = running[0] + jnp.dot(dscores.T, query_rows.astype(jnp.float32), precision=lax.Precision.HIGHEST)
        dvalues = running[1] + jnp.dot(softmaxed.T, grad_rows.astype(jnp.float32), precision=lax.Precision.HIGHEST)
        return ((grad_keys, dvalues), dquery)
    zero_rows = jnp.zeros((seq_len, head_width), jnp.float32)
    count = seq_len // block_size
    blocks = (queries.reshape(count, block_size, head_width), upstream.reshape(count, block_size, head_width))
    (grad_keys, dvalues), dquery = lax.scan(one_block, (zero_rows, zero_rows), blocks)
    return (dquery.reshape(seq_len, head_width).astype(jnp.bfloat16), grad_keys.astype(jnp.bfloat16), dvalues.astype(jnp.bfloat16))

def attend_all(queries, key_rows, values):
    attended = lax.map(attend_head, (heads_major(queries), heads_major(key_rows), heads_major(values)))
    return heads_minor(attended, queries.shape[0])

def attend_all_back(queries, key_rows, values, upstream):
    grad_heads = lax.map(attend_back, (heads_major(queries), heads_major(key_rows), heads_major(values), heads_major(upstream)))
    return tuple((heads_minor(grad_piece, queries.shape[0]) for grad_piece in grad_heads))

def reference(tokens, modulation, w_qkv, w_out, w_in, w_back, out_grad):
    videos, seq_len, model_width = tokens.shape
    layers = w_qkv.shape[0]
    head_count = model_width // HEAD_DIM
    grad_scale = 1.0 / math.sqrt(videos * seq_len)
    stream = tokens.astype(jnp.float32)
    stored = []
    for layer_index in range(layers):
        layer_mod = modulation[:, layer_index][:, :, None, :]
        joint = w_qkv[layer_index].reshape(model_width, 3 * model_width)
        normed_first, rstd_first = normalize(stream)
        input_first = (normed_first * (1.0 + layer_mod[:, 1]) + layer_mod[:, 0]).astype(jnp.bfloat16)
        packed = project(input_first, joint).astype(jnp.bfloat16)
        queries = split_heads(packed[..., :model_width], head_count)
        key_rows = split_heads(packed[..., model_width:2 * model_width], head_count)
        values = split_heads(packed[..., 2 * model_width:], head_count)
        attended = attend_all(queries, key_rows, values).reshape(videos, seq_len, model_width)
        middle = stream + layer_mod[:, 2] * project(attended, w_out[layer_index])
        normed_second, rstd_second = normalize(middle)
        input_second = (normed_second * (1.0 + layer_mod[:, 4]) + layer_mod[:, 3]).astype(jnp.bfloat16)
        hidden = project(input_second, w_in[layer_index])
        activated = gelu_tanh(hidden).astype(jnp.bfloat16)
        stream = middle + layer_mod[:, 5] * project(activated, w_back[layer_index])
        stored.append((normed_first, rstd_first, input_first, queries, key_rows, values, attended, normed_second, rstd_second, input_second, hidden, activated))
    final_out = stream.astype(jnp.bfloat16)
    stream_grad = out_grad.astype(jnp.float32)
    results = [None] * layers
    for layer_index in range(layers - 1, -1, -1):
        normed_first, rstd_first, input_first, queries, key_rows, values, attended, normed_second, rstd_second, input_second, hidden, activated = stored[layer_index]
        layer_mod = modulation[:, layer_index][:, :, None, :]
        joint = w_qkv[layer_index].reshape(model_width, 3 * model_width)
        down_grad = (layer_mod[:, 5] * stream_grad).astype(jnp.bfloat16)
        back_hidden = project_back(down_grad, w_back[layer_index])
        unused, pullback = jax.vjp(gelu_tanh, hidden)
        up_grad = pullback(back_hidden)[0].astype(jnp.bfloat16)
        back_second = project_back(up_grad, w_in[layer_index])
        stream_grad = stream_grad + norm_back(normed_second, rstd_second, back_second * (1.0 + layer_mod[:, 4]))
        attn_grad = (layer_mod[:, 2] * stream_grad).astype(jnp.bfloat16)
        mixed_grad = split_heads(project_back(attn_grad, w_out[layer_index]).astype(jnp.bfloat16), head_count)
        grad_query, grad_keys, grad_values = attend_all_back(queries, key_rows, values, mixed_grad)
        packed_grad = jnp.concatenate([grad_query.reshape(videos, seq_len, model_width), grad_keys.reshape(videos, seq_len, model_width), grad_values.reshape(videos, seq_len, model_width)], axis=-1)
        back_first = project_back(packed_grad, joint)
        stream_grad = stream_grad + norm_back(normed_first, rstd_first, back_first * (1.0 + layer_mod[:, 1]))
        results[layer_index] = (group_grad(input_first, packed_grad, grad_scale).reshape(model_width, 3, model_width), group_grad(attended, attn_grad, grad_scale), group_grad(input_second, up_grad, grad_scale), group_grad(activated, down_grad, grad_scale))
    grad_qkv = jnp.stack([results[index][0] for index in range(layers)])
    grad_out = jnp.stack([results[index][1] for index in range(layers)])
    grad_in = jnp.stack([results[index][2] for index in range(layers)])
    grad_back = jnp.stack([results[index][3] for index in range(layers)])
    return (final_out, stream_grad, grad_qkv, grad_out, grad_in, grad_back)
```

```python
import functools
import math

import jax
import jax.numpy as jnp
from jax import lax
from jax.experimental import pallas as pl
from jax.experimental.pallas import tpu as pltpu
from jax.sharding import Mesh
from jax.sharding import PartitionSpec as P

HEAD_DIM = 128
MESH = pl.DeviceIdType.MESH
FSDP = ("z", "y", "xh")
SP = ("xl", "c")
BF = jnp.bfloat16
F32 = jnp.float32

ln_eps = 1e-06
temper = 2.5
VMEM_LIMIT = 66_000_000

CHUNKS = (
    ((0, 640), (640, 512)),
    ((1152, 128), (1280, 256)),
    ((1536, 768), (2304, 768)),
    ((3072, 768), (3840, 768)),
)
WIDTH = 4608


def turn(axis, step, size):
    return {axis: lax.rem(lax.axis_index(axis) + step + size, size)}


def near(axis, step):
    return lax.rem(lax.axis_index(axis) + step + 4, 4)


class Wires:
    def __init__(self, send, recv):
        self.send, self.recv, self.used, self.open = send, recv, 0, []

    def go(self, src, dst, device):
        at = self.used
        self.used += 1
        copy = pltpu.make_async_remote_copy(
            src_ref=src,
            dst_ref=dst,
            send_sem=self.send.at[at],
            recv_sem=self.recv.at[at],
            device_id=device,
            device_id_type=MESH,
        )
        copy.start()
        self.open.append(copy)
        return copy

    def drain(self):
        for copy in self.open:
            copy.wait_send()
        self.open = []


def greet(sp=False):
    barrier = pltpu.get_barrier_semaphore()
    targets = [turn("z", 1, 4), turn("z", -1, 4), turn("y", 1, 4), turn("y", -1, 4), turn("xh", 1, 2)]
    if sp:
        targets += [turn("xl", 1, 2), turn("c", 1, 2)]
    for device in targets:
        pl.semaphore_signal(barrier, inc=1, device_id=device, device_id_type=MESH)
    pl.semaphore_wait(barrier, len(targets))


def rows_of(start, count):
    return pl.ds(pl.multiple_of(start, 16), count)


def cols_of(cols):
    return pl.ds(cols[0], cols[1])


class Gather:
    def __init__(self, wires, w):
        self.wires, self.w = wires, w
        self.z, self.y, self.xh = (lax.axis_index(a) for a in FSDP)
        self.one, self.two, self.relay2, self.three, self.relay3 = {}, {}, {}, {}, {}

    def same(self, part, device):
        return self.wires.go(part, part, device)

    def s1(self, k):
        (a0, an), (b0, bn) = CHUNKS[k]
        part = self.w.at[self.z, rows_of(96 * self.y + 48 * self.xh, 48), pl.ds(a0, an + bn)]
        self.one[k] = self.same(part, turn("xh", 1, 2))

    def s2(self, k):
        self.one[k].wait_recv()
        ca, cb = map(cols_of, CHUNKS[k])
        pa = self.w.at[self.z, rows_of(96 * self.y, 96), ca]
        pb = self.w.at[self.z, rows_of(96 * self.y, 96), cb]
        self.two[k] = [
            self.same(pa, turn("y", 1, 4)),
            self.same(pa, turn("y", -1, 4)),
            self.same(pb, turn("z", 1, 4)),
            self.same(pb, turn("z", -1, 4)),
        ]

    def s2b(self, k):
        ca, cb = map(cols_of, CHUNKS[k])
        for copy in self.two[k]:
            copy.wait_recv()
        w, z, y = self.w, self.z, self.y
        self.relay2[k] = [
            self.same(w.at[z, rows_of(96 * near("y", -1), 48), ca], turn("y", 1, 4)),
            self.same(w.at[z, rows_of(96 * near("y", 1) + 48, 48), ca], turn("y", -1, 4)),
            self.same(w.at[near("z", -1), rows_of(96 * y, 48), cb], turn("z", 1, 4)),
            self.same(w.at[near("z", 1), rows_of(96 * y + 48, 48), cb], turn("z", -1, 4)),
        ]

    def s3(self, k):
        ca, cb = map(cols_of, CHUNKS[k])
        for copy in self.relay2[k]:
            copy.wait_recv()
        pa = self.w.at[self.z, :, ca]
        pb = self.w.at[:, rows_of(96 * self.y, 96), cb]
        self.three[k] = [
            self.same(pa, turn("z", 1, 4)),
            self.same(pa, turn("z", -1, 4)),
            self.same(pb, turn("y", 1, 4)),
            self.same(pb, turn("y", -1, 4)),
        ]

    def s3b(self, k):
        ca, cb = map(cols_of, CHUNKS[k])
        for copy in self.three[k]:
            copy.wait_recv()
        w = self.w
        self.relay3[k] = [
            self.same(w.at[near("z", -1), pl.ds(0, 192), ca], turn("z", 1, 4)),
            self.same(w.at[near("z", 1), pl.ds(192, 192), ca], turn("z", -1, 4)),
            self.same(w.at[:, rows_of(96 * near("y", -1), 48), cb], turn("y", 1, 4)),
            self.same(w.at[:, rows_of(96 * near("y", 1) + 48, 48), cb], turn("y", -1, 4)),
        ]

    def done(self, k):
        for copy in self.relay3[k]:
            copy.wait_recv()


def add_into(dst, *srcs):
    planes, rows, columns = dst.shape

    @pl.loop(0, planes * (rows // 48))
    def _(i):
        at = (i // (rows // 48), pl.ds(pl.multiple_of((i % (rows // 48)) * 48, 48), 48), slice(None))
        total = dst[at].astype(F32)
        for src in srcs:
            total = total + src[at].astype(F32)
        dst[at] = total.astype(dst.dtype)


class Scatter:
    def __init__(self, wires, g, half_a, full_a, half_b, full_b, half2, full2, last, out):
        self.wires, self.g, self.out = wires, g, out
        self.half_a, self.full_a, self.half_b, self.full_b = half_a, full_a, half_b, full_b
        self.half2, self.full2, self.last = half2, full2, last
        self.z, self.y, self.xh = (lax.axis_index(a) for a in FSDP)
        self.copies = {}

    def block_a(self, step, start, count, cols):
        return self.g.at[pl.ds(near("z", step), 1), pl.ds(start, count), cols]

    def block_b(self, step, start, count, cols):
        return self.g.at[:, rows_of(96 * near("y", step) + start, count), cols]

    def sub_a(self, step, start, count, cols):
        return self.g.at[pl.ds(self.z, 1), rows_of(96 * near("y", step) + start, count), cols]

    def sub_b(self, step, start, count, cols):
        return self.g.at[pl.ds(near("z", step), 1), rows_of(96 * self.y + start, count), cols]

    def r1(self, k):
        ca, cb = map(cols_of, CHUNKS[k])
        go = self.wires.go
        self.copies[k, 1] = [
            go(self.block_a(2, 0, 192, ca), self.half_a[k].at[pl.ds(0, 1)], turn("z", 1, 4)),
            go(self.block_a(2, 192, 192, ca), self.half_a[k].at[pl.ds(1, 1)], turn("z", -1, 4)),
            go(self.block_b(2, 0, 48, cb), self.half_b[k].at[0], turn("y", 1, 4)),
            go(self.block_b(2, 48, 48, cb), self.half_b[k].at[1], turn("y", -1, 4)),
        ]

    def r1b(self, k):
        ca, cb = map(cols_of, CHUNKS[k])
        go, copies = self.wires.go, self.copies[k, 1]
        sent = []
        copies[0].wait_recv()
        add_into(self.block_a(1, 0, 192, ca), self.half_a[k].at[pl.ds(0, 1)])
        sent.append(go(self.block_a(1, 0, 384, ca), self.full_a[k].at[pl.ds(0, 1)], turn("z", 1, 4)))
        copies[1].wait_recv()
        add_into(self.block_a(-1, 192, 192, ca), self.half_a[k].at[pl.ds(1, 1)])
        sent.append(go(self.block_a(-1, 0, 384, ca), self.full_a[k].at[pl.ds(1, 1)], turn("z", -1, 4)))
        copies[2].wait_recv()
        add_into(self.block_b(1, 0, 48, cb), self.half_b[k].at[0])
        sent.append(go(self.block_b(1, 0, 96, cb), self.full_b[k].at[0], turn("y", 1, 4)))
        copies[3].wait_recv()
        add_into(self.block_b(-1, 48, 48, cb), self.half_b[k].at[1])
        sent.append(go(self.block_b(-1, 0, 96, cb), self.full_b[k].at[1], turn("y", -1, 4)))
        self.copies[k, 2] = sent

    def r2(self, k):
        ca, cb = map(cols_of, CHUNKS[k])
        go, copies = self.wires.go, self.copies[k, 2]
        copies[0].wait_recv()
        copies[1].wait_recv()
        add_into(
            self.block_a(0, 0, 384, ca), self.full_a[k].at[pl.ds(0, 1)], self.full_a[k].at[pl.ds(1, 1)]
        )
        sent = [
            go(self.sub_a(2, 0, 48, ca), self.half2[k][0].at[pl.ds(0, 1)], turn("y", 1, 4)),
            go(self.sub_a(2, 48, 48, ca), self.half2[k][0].at[pl.ds(1, 1)], turn("y", -1, 4)),
        ]
        copies[2].wait_recv()
        copies[3].wait_recv()
        add_into(self.block_b(0, 0, 96, cb), self.full_b[k].at[0], self.full_b[k].at[1])
        sent += [
            go(self.sub_b(2, 0, 48, cb), self.half2[k][1].at[pl.ds(0, 1)], turn("z", 1, 4)),
            go(self.sub_b(2, 48, 48, cb), self.half2[k][1].at[pl.ds(1, 1)], turn("z", -1, 4)),
        ]
        self.copies[k, 3] = sent

    def r2b(self, k):
        go, copies = self.wires.go, self.copies[k, 3]
        sent = []
        for colour, (sub, axis) in enumerate(((self.sub_a, "y"), (self.sub_b, "z"))):
            cols = cols_of(CHUNKS[k][colour])
            half, full = self.half2[k][colour], self.full2[k][colour]
            copies[2 * colour].wait_recv()
            add_into(sub(1, 0, 48, cols), half.at[pl.ds(0, 1)])
            sent.append(go(sub(1, 0, 96, cols), full.at[pl.ds(0, 1)], turn(axis, 1, 4)))
            copies[2 * colour + 1].wait_recv()
            add_into(sub(-1, 48, 48, cols), half.at[pl.ds(1, 1)])
            sent.append(go(sub(-1, 0, 96, cols), full.at[pl.ds(1, 1)], turn(axis, -1, 4)))
        self.copies[k, 4] = sent

    def r3(self, k):
        go, copies = self.wires.go, self.copies[k, 4]
        (a0, an), (b0, bn) = CHUNKS[k]
        for colour, sub in enumerate((self.sub_a, self.sub_b)):
            cols, full = cols_of(CHUNKS[k][colour]), self.full2[k][colour]
            copies[2 * colour].wait_recv()
            copies[2 * colour + 1].wait_recv()
            add_into(sub(0, 0, 96, cols), full.at[pl.ds(0, 1)], full.at[pl.ds(1, 1)])
        part = self.g.at[self.z, rows_of(96 * self.y + 48 * (1 - self.xh), 48), pl.ds(a0, an + bn)]
        self.copies[k, 5] = [go(part, self.last.at[:, pl.ds(a0, an + bn)], turn("xh", 1, 2))]

    def done(self, k):
        (a0, an), (b0, bn) = CHUNKS[k]
        self.copies[k, 5][0].wait_recv()
        cols = pl.ds(a0, an + bn)
        own = self.g[self.z, rows_of(96 * self.y + 48 * self.xh, 48), cols]
        self.out[:, cols] = own.astype(F32) + self.last[:, cols].astype(F32)


def scatter_buffers():
    shapes = []
    for (a0, an), (b0, bn) in CHUNKS:
        shapes += [
            pltpu.VMEM((2, 192, an), BF),
            pltpu.VMEM((2, 384, an), BF),
            pltpu.VMEM((2, 4, 48, bn), BF),
            pltpu.VMEM((2, 4, 96, bn), BF),
            pltpu.VMEM((2, 48, an), BF),
            pltpu.VMEM((2, 96, an), BF),
            pltpu.VMEM((2, 48, bn), BF),
            pltpu.VMEM((2, 96, bn), BF),
        ]
    return shapes


def make_scatter(wires, g, bufs, last, out):
    n = len(CHUNKS)
    groups = [bufs[8 * k : 8 * k + 8] for k in range(n)]
    return Scatter(
        wires,
        g,
        [b[0] for b in groups],
        [b[1] for b in groups],
        [b[2] for b in groups],
        [b[3] for b in groups],
        [(b[4], b[6]) for b in groups],
        [(b[5], b[7]) for b in groups],
        last,
        out,
    )


def gather_kernel(shard_ref, out_ref, w, send, recv, local_sem):
    z, y, xh = (lax.axis_index(a) for a in FSDP)
    own = pltpu.make_async_copy(shard_ref, w.at[z, rows_of(96 * y + 48 * xh, 48), :], local_sem)
    own.start()
    greet()
    own.wait()
    wires = Wires(send, recv)
    ag = Gather(wires, w)
    n = len(CHUNKS)
    for k in range(n):
        ag.s1(k)
    ag.s2(0)
    ag.s2(1)
    ag.s2b(0)
    ag.s3(0)
    ag.s2b(1)
    ag.s2(2)
    ag.s3b(0)
    ag.s3(1)
    ag.s2b(2)
    ag.s2(3)
    ag.s3(2)
    ag.s3b(1)
    ag.s2b(3)
    ag.s3b(2)
    ag.s3(3)
    ag.s3b(3)
    for k in range(n):
        ag.done(k)
    wires.drain()
    back = pltpu.make_async_copy(w, out_ref, local_sem)
    back.start()
    back.wait()


def gather_rows(shard):
    return pl.pallas_call(
        gather_kernel,
        out_shape=jax.ShapeDtypeStruct((4, 384, WIDTH), BF),
        in_specs=[pl.BlockSpec(memory_space=pl.ANY)],
        out_specs=pl.BlockSpec(memory_space=pl.ANY),
        scratch_shapes=[
            pltpu.VMEM((4, 384, WIDTH), BF),
            pltpu.SemaphoreType.DMA((17 * len(CHUNKS),)),
            pltpu.SemaphoreType.DMA((17 * len(CHUNKS),)),
            pltpu.SemaphoreType.DMA,
        ],
        compiler_params=pltpu.CompilerParams(
            collective_id=0, has_side_effects=True, vmem_limit_bytes=VMEM_LIMIT
        ),
        name="gather_rows",
    )(shard)


def scatter_kernel(g_ref, out_ref, g, last, send, recv, local_sem, *bufs):
    own = pltpu.make_async_copy(g_ref, g, local_sem)
    own.start()
    greet()
    own.wait()
    wires = Wires(send, recv)
    rs = make_scatter(wires, g, bufs, last, out_ref)
    order = (3, 2, 1, 0)
    for k in order:
        rs.r1(k)
    for k in order:
        rs.r1b(k)
    for k in order:
        rs.r2(k)
    for k in order:
        rs.r2b(k)
    for k in order:
        rs.r3(k)
    for k in order:
        rs.done(k)
    wires.drain()


def scatter_rows(g):
    return pl.pallas_call(
        scatter_kernel,
        out_shape=jax.ShapeDtypeStruct((48, WIDTH), F32),
        in_specs=[pl.BlockSpec(memory_space=pl.ANY)],
        out_specs=pl.BlockSpec(memory_space=pltpu.VMEM),
        scratch_shapes=[
            pltpu.VMEM((4, 384, WIDTH), BF),
            pltpu.VMEM((48, WIDTH), BF),
            pltpu.SemaphoreType.DMA((17 * len(CHUNKS),)),
            pltpu.SemaphoreType.DMA((17 * len(CHUNKS),)),
            pltpu.SemaphoreType.DMA,
            *scatter_buffers(),
        ],
        compiler_params=pltpu.CompilerParams(
            collective_id=1, has_side_effects=True, vmem_limit_bytes=VMEM_LIMIT
        ),
        name="scatter_rows",
    )(g)


def normalize(stream):
    mean_part = jnp.mean(stream, axis=-1, keepdims=True)
    centred = stream - mean_part
    rstd = lax.rsqrt(jnp.mean(centred * centred, axis=-1, keepdims=True) + ln_eps)
    return (centred * rstd, rstd)


def norm_back(normed, rstd, incoming):
    first = jnp.mean(incoming, axis=-1, keepdims=True)
    second = jnp.mean(incoming * normed, axis=-1, keepdims=True)
    return rstd * (incoming - first - normed * second)


def gelu_tanh(hidden):
    return jax.nn.gelu(hidden, approximate=True)


def nn(a, b):
    return jnp.dot(a, b, preferred_element_type=F32)


def nt(a, b):
    return lax.dot_general(a, b, (((1,), (1,)), ((), ())), preferred_element_type=F32)


def tn(a, b):
    return lax.dot_general(a, b, (((0,), (0,)), ((), ())), preferred_element_type=F32)


def spread(rows):
    return lax.all_gather(rows, SP, axis=0, tiled=True)


def collect(part):
    return lax.psum_scatter(part.astype(BF), SP, scatter_dimension=0, tiled=True).astype(F32)


def body(tokens, modulation, w_qkv, w_out, w_in, w_back, out_grad):
    heads = w_qkv.shape[3] // HEAD_DIM
    own = w_qkv.shape[3]
    scale = 1.0 / math.sqrt(32 * 512)
    c = temper / math.sqrt(HEAD_DIM)
    shard = jnp.concatenate(
        [w_qkv[0].reshape(48, 3 * own), w_out[0].T, w_in[0], w_back[0].T], axis=1
    )
    w = gather_rows(shard).reshape(1536, WIDTH)
    wq, wot, wi, wbt = w[:, :1152], w[:, 1152:1536], w[:, 1536:3072], w[:, 3072:]
    m = modulation[0, 0][:, None, :]
    x = tokens[0].astype(F32)
    dx = out_grad[0].astype(F32)
    n1, r1 = normalize(x)
    a1 = spread((n1 * (1.0 + m[1]) + m[0]).astype(BF))
    dm = spread((m[5] * dx).astype(BF))
    qkv = nn(a1, wq).astype(BF).reshape(512, 3, heads, HEAD_DIM).transpose(1, 2, 0, 3)
    q, k, v = qkv[0], qkv[1], qkv[2]
    s = jnp.einsum("hqd,hkd->hqk", q, k, preferred_element_type=F32) * c
    p = jax.nn.softmax(s, axis=-1)
    o = jnp.einsum("hqk,hkd->hqd", p.astype(BF), v, preferred_element_type=F32)
    o = o.astype(BF).transpose(1, 0, 2).reshape(512, own)
    mid = x + m[2] * collect(nt(o, wot))
    n2, r2 = normalize(mid)
    a2 = spread((n2 * (1.0 + m[4]) + m[3]).astype(BF))
    u = nn(a2, wi)
    g, pull = jax.vjp(gelu_tanh, u)
    g = g.astype(BF)
    final = (mid + m[5] * collect(nt(g, wbt))).astype(BF)
    du = pull(nn(dm, wbt))[0].astype(BF)
    dmid = dx + norm_back(n2, r2, collect(nt(du, wi)) * (1.0 + m[4]))
    da = spread((m[2] * dmid).astype(BF))
    do = nn(da, wot).astype(BF).reshape(512, heads, HEAD_DIM).transpose(1, 0, 2)
    dp = jnp.einsum("hqd,hkd->hqk", do, v, preferred_element_type=F32)
    ds = c * p * (dp - jnp.sum(p * dp, axis=-1, keepdims=True))
    ds = ds.astype(BF)
    dq = jnp.einsum("hqk,hkd->hqd", ds, k, preferred_element_type=F32)
    dk = jnp.einsum("hqk,hqd->hkd", ds, q, preferred_element_type=F32)
    dv = jnp.einsum("hqk,hqd->hkd", p.astype(BF), do, preferred_element_type=F32)
    dqkv = jnp.stack([dq, dk, dv]).astype(BF).transpose(2, 0, 1, 3).reshape(512, 3 * own)
    dlast = dmid + norm_back(n1, r1, collect(nt(dqkv, wq)) * (1.0 + m[1]))
    grads = jnp.concatenate([tn(a1, dqkv), tn(da, o), tn(a2, du), tn(dm, g)], axis=1)
    sums = scatter_rows((grads * scale).astype(BF).reshape(4, 384, WIDTH))
    return (
        final[None],
        dlast[None],
        sums[:, :1152].reshape(1, 48, 3, own),
        sums[:, 1152:1536].T[None],
        sums[:, 1536:3072][None],
        sums[:, 3072:].T[None],
    )


def solution(mesh):
    torus = Mesh(mesh.devices.reshape(4, 4, 2, 2, 2), FSDP + SP)
    return jax.shard_map(
        body,
        mesh=torus,
        in_specs=(
            P(FSDP, SP, None),
            P(FSDP, None, None, None),
            P(None, FSDP, None, SP),
            P(None, SP, FSDP),
            P(None, FSDP, SP),
            P(None, SP, FSDP),
            P(FSDP, SP, None),
        ),
        out_specs=(
            P(FSDP, SP, None),
            P(FSDP, SP, None),
            P(None, FSDP, None, SP),
            P(None, SP, FSDP),
            P(None, FSDP, SP),
            P(None, SP, FSDP),
        ),
        check_vma=False,
    )
```

```python
import functools
import math

import jax
import jax.numpy as jnp
from jax import lax
from jax.experimental import pallas as pl
from jax.experimental.pallas import tpu as pltpu
from jax.sharding import Mesh
from jax.sharding import PartitionSpec as P

HEAD_DIM = 128
MESH = pl.DeviceIdType.MESH
FSDP = ("z", "y", "xh")
SP = ("xl", "c")
BF = jnp.bfloat16
F32 = jnp.float32

ln_eps = 1e-06
temper = 2.5
VMEM_LIMIT = 67_000_000

CHUNKS = (
    ((0, 640), (640, 512)),
    ((1152, 128), (1280, 256)),
    ((1536, 768), (2304, 768)),
    ((3072, 768), (3840, 768)),
)
WIDTH = 4608


def turn(axis, step, size):
    return {axis: lax.rem(lax.axis_index(axis) + step + size, size)}


def near(axis, step):
    return lax.rem(lax.axis_index(axis) + step + 4, 4)


class Wires:
    def __init__(self, send, recv):
        self.send, self.recv, self.used, self.open = send, recv, 0, []

    def go(self, src, dst, device):
        at = self.used
        self.used += 1
        copy = pltpu.make_async_remote_copy(
            src_ref=src,
            dst_ref=dst,
            send_sem=self.send.at[at],
            recv_sem=self.recv.at[at],
            device_id=device,
            device_id_type=MESH,
        )
        copy.start()
        self.open.append(copy)
        return copy

    def sent(self, copy):
        copy.wait_send()
        self.open = [other for other in self.open if other is not copy]

    def drain(self):
        for copy in self.open:
            copy.wait_send()
        self.open = []


def greet(sp=False):
    barrier = pltpu.get_barrier_semaphore()
    targets = [turn("z", 1, 4), turn("z", -1, 4), turn("y", 1, 4), turn("y", -1, 4), turn("xh", 1, 2)]
    if sp:
        targets += [turn("xl", 1, 2), turn("c", 1, 2)]
    for device in targets:
        pl.semaphore_signal(barrier, inc=1, device_id=device, device_id_type=MESH)
    pl.semaphore_wait(barrier, len(targets))


def rows_of(start, count):
    return pl.ds(pl.multiple_of(start, 16), count)


def cols_of(cols):
    return pl.ds(cols[0], cols[1])


class Gather:
    def __init__(self, wires, w):
        self.wires, self.w = wires, w
        self.z, self.y, self.xh = (lax.axis_index(a) for a in FSDP)
        self.one, self.two, self.relay2, self.three, self.relay3 = {}, {}, {}, {}, {}

    def same(self, part, device):
        return self.wires.go(part, part, device)

    def s1(self, k):
        (a0, an), (b0, bn) = CHUNKS[k]
        part = self.w.at[self.z, rows_of(96 * self.y + 48 * self.xh, 48), pl.ds(a0, an + bn)]
        self.one[k] = self.same(part, turn("xh", 1, 2))

    def s2(self, k):
        self.one[k].wait_recv()
        ca, cb = map(cols_of, CHUNKS[k])
        pa = self.w.at[self.z, rows_of(96 * self.y, 96), ca]
        pb = self.w.at[self.z, rows_of(96 * self.y, 96), cb]
        self.two[k] = [
            self.same(pa, turn("y", 1, 4)),
            self.same(pa, turn("y", -1, 4)),
            self.same(pb, turn("z", 1, 4)),
            self.same(pb, turn("z", -1, 4)),
        ]

    def s2b(self, k):
        ca, cb = map(cols_of, CHUNKS[k])
        for copy in self.two[k]:
            copy.wait_recv()
        w, z, y = self.w, self.z, self.y
        self.relay2[k] = [
            self.same(w.at[z, rows_of(96 * near("y", -1), 48), ca], turn("y", 1, 4)),
            self.same(w.at[z, rows_of(96 * near("y", 1) + 48, 48), ca], turn("y", -1, 4)),
            self.same(w.at[near("z", -1), rows_of(96 * y, 48), cb], turn("z", 1, 4)),
            self.same(w.at[near("z", 1), rows_of(96 * y + 48, 48), cb], turn("z", -1, 4)),
        ]

    def s3(self, k):
        ca, cb = map(cols_of, CHUNKS[k])
        for copy in self.relay2[k]:
            copy.wait_recv()
        pa = self.w.at[self.z, :, ca]
        pb = self.w.at[:, rows_of(96 * self.y, 96), cb]
        self.three[k] = [
            self.same(pa, turn("z", 1, 4)),
            self.same(pa, turn("z", -1, 4)),
            self.same(pb, turn("y", 1, 4)),
            self.same(pb, turn("y", -1, 4)),
        ]

    def s3b(self, k):
        ca, cb = map(cols_of, CHUNKS[k])
        for copy in self.three[k]:
            copy.wait_recv()
        w = self.w
        self.relay3[k] = [
            self.same(w.at[near("z", -1), pl.ds(0, 192), ca], turn("z", 1, 4)),
            self.same(w.at[near("z", 1), pl.ds(192, 192), ca], turn("z", -1, 4)),
            self.same(w.at[:, rows_of(96 * near("y", -1), 48), cb], turn("y", 1, 4)),
            self.same(w.at[:, rows_of(96 * near("y", 1) + 48, 48), cb], turn("y", -1, 4)),
        ]

    def done(self, k):
        for copy in self.relay3[k]:
            copy.wait_recv()


def add_into(dst, *srcs):
    planes, rows, columns = dst.shape

    @pl.loop(0, planes * (rows // 48))
    def _(i):
        at = (i // (rows // 48), pl.ds(pl.multiple_of((i % (rows // 48)) * 48, 48), 48), slice(None))
        total = dst[at].astype(F32)
        for src in srcs:
            total = total + src[at].astype(F32)
        dst[at] = total.astype(dst.dtype)


class Scatter:
    def __init__(self, wires, g, half_a, full_a, half_b, full_b, half2, full2, last, out):
        self.wires, self.g, self.out = wires, g, out
        self.half_a, self.full_a, self.half_b, self.full_b = half_a, full_a, half_b, full_b
        self.half2, self.full2, self.last = half2, full2, last
        self.z, self.y, self.xh = (lax.axis_index(a) for a in FSDP)
        self.copies = {}

    def block_a(self, step, start, count, cols):
        return self.g.at[pl.ds(near("z", step), 1), pl.ds(start, count), cols]

    def block_b(self, step, start, count, cols):
        return self.g.at[:, rows_of(96 * near("y", step) + start, count), cols]

    def sub_a(self, step, start, count, cols):
        return self.g.at[pl.ds(self.z, 1), rows_of(96 * near("y", step) + start, count), cols]

    def sub_b(self, step, start, count, cols):
        return self.g.at[pl.ds(near("z", step), 1), rows_of(96 * self.y + start, count), cols]

    def r1(self, k):
        ca, cb = map(cols_of, CHUNKS[k])
        go = self.wires.go
        self.copies[k, 1] = [
            go(self.block_a(2, 0, 192, ca), self.half_a[k].at[pl.ds(0, 1)], turn("z", 1, 4)),
            go(self.block_a(2, 192, 192, ca), self.half_a[k].at[pl.ds(1, 1)], turn("z", -1, 4)),
            go(self.block_b(2, 0, 48, cb), self.half_b[k].at[0], turn("y", 1, 4)),
            go(self.block_b(2, 48, 48, cb), self.half_b[k].at[1], turn("y", -1, 4)),
        ]

    def r1b(self, k):
        ca, cb = map(cols_of, CHUNKS[k])
        go, copies = self.wires.go, self.copies[k, 1]
        sent = []
        copies[0].wait_recv()
        add_into(self.block_a(1, 0, 192, ca), self.half_a[k].at[pl.ds(0, 1)])
        sent.append(go(self.block_a(1, 0, 384, ca), self.full_a[k].at[pl.ds(0, 1)], turn("z", 1, 4)))
        copies[1].wait_recv()
        add_into(self.block_a(-1, 192, 192, ca), self.half_a[k].at[pl.ds(1, 1)])
        sent.append(go(self.block_a(-1, 0, 384, ca), self.full_a[k].at[pl.ds(1, 1)], turn("z", -1, 4)))
        copies[2].wait_recv()
        add_into(self.block_b(1, 0, 48, cb), self.half_b[k].at[0])
        sent.append(go(self.block_b(1, 0, 96, cb), self.full_b[k].at[0], turn("y", 1, 4)))
        copies[3].wait_recv()
        add_into(self.block_b(-1, 48, 48, cb), self.half_b[k].at[1])
        sent.append(go(self.block_b(-1, 0, 96, cb), self.full_b[k].at[1], turn("y", -1, 4)))
        self.copies[k, 2] = sent

    def r2(self, k):
        ca, cb = map(cols_of, CHUNKS[k])
        go, copies = self.wires.go, self.copies[k, 2]
        copies[0].wait_recv()
        copies[1].wait_recv()
        add_into(
            self.block_a(0, 0, 384, ca), self.full_a[k].at[pl.ds(0, 1)], self.full_a[k].at[pl.ds(1, 1)]
        )
        sent = [
            go(self.sub_a(2, 0, 48, ca), self.half2[k][0].at[pl.ds(0, 1)], turn("y", 1, 4)),
            go(self.sub_a(2, 48, 48, ca), self.half2[k][0].at[pl.ds(1, 1)], turn("y", -1, 4)),
        ]
        copies[2].wait_recv()
        copies[3].wait_recv()
        add_into(self.block_b(0, 0, 96, cb), self.full_b[k].at[0], self.full_b[k].at[1])
        sent += [
            go(self.sub_b(2, 0, 48, cb), self.half2[k][1].at[pl.ds(0, 1)], turn("z", 1, 4)),
            go(self.sub_b(2, 48, 48, cb), self.half2[k][1].at[pl.ds(1, 1)], turn("z", -1, 4)),
        ]
        self.copies[k, 3] = sent

    def r2b(self, k):
        go, copies = self.wires.go, self.copies[k, 3]
        sent = []
        for colour, (sub, axis) in enumerate(((self.sub_a, "y"), (self.sub_b, "z"))):
            cols = cols_of(CHUNKS[k][colour])
            half, full = self.half2[k][colour], self.full2[k][colour]
            copies[2 * colour].wait_recv()
            add_into(sub(1, 0, 48, cols), half.at[pl.ds(0, 1)])
            sent.append(go(sub(1, 0, 96, cols), full.at[pl.ds(0, 1)], turn(axis, 1, 4)))
            copies[2 * colour + 1].wait_recv()
            add_into(sub(-1, 48, 48, cols), half.at[pl.ds(1, 1)])
            sent.append(go(sub(-1, 0, 96, cols), full.at[pl.ds(1, 1)], turn(axis, -1, 4)))
        self.copies[k, 4] = sent

    def r3(self, k):
        go, copies = self.wires.go, self.copies[k, 4]
        (a0, an), (b0, bn) = CHUNKS[k]
        for colour, sub in enumerate((self.sub_a, self.sub_b)):
            cols, full = cols_of(CHUNKS[k][colour]), self.full2[k][colour]
            copies[2 * colour].wait_recv()
            copies[2 * colour + 1].wait_recv()
            add_into(sub(0, 0, 96, cols), full.at[pl.ds(0, 1)], full.at[pl.ds(1, 1)])
        part = self.g.at[self.z, rows_of(96 * self.y + 48 * (1 - self.xh), 48), pl.ds(a0, an + bn)]
        self.copies[k, 5] = [go(part, self.last.at[:, pl.ds(a0, an + bn)], turn("xh", 1, 2))]

    def done(self, k):
        (a0, an), (b0, bn) = CHUNKS[k]
        self.copies[k, 5][0].wait_recv()
        cols = pl.ds(a0, an + bn)
        own = self.g[self.z, rows_of(96 * self.y + 48 * self.xh, 48), cols]
        self.out[:, cols] = own.astype(F32) + self.last[:, cols].astype(F32)


def scatter_buffers():
    shapes = []
    for (a0, an), (b0, bn) in CHUNKS:
        shapes += [
            pltpu.VMEM((2, 192, an), BF),
            pltpu.VMEM((2, 384, an), BF),
            pltpu.VMEM((2, 4, 48, bn), BF),
            pltpu.VMEM((2, 4, 96, bn), BF),
            pltpu.VMEM((2, 48, an), BF),
            pltpu.VMEM((2, 96, an), BF),
            pltpu.VMEM((2, 48, bn), BF),
            pltpu.VMEM((2, 96, bn), BF),
        ]
    return shapes


def make_scatter(wires, g, bufs, last, out):
    n = len(CHUNKS)
    groups = [bufs[8 * k : 8 * k + 8] for k in range(n)]
    return Scatter(
        wires,
        g,
        [b[0] for b in groups],
        [b[1] for b in groups],
        [b[2] for b in groups],
        [b[3] for b in groups],
        [(b[4], b[6]) for b in groups],
        [(b[5], b[7]) for b in groups],
        last,
        out,
    )


def nn(a, b):
    return jnp.dot(a, b, preferred_element_type=F32)


def nt(a, b):
    return lax.dot_general(a, b, (((1,), (1,)), ((), ())), preferred_element_type=F32)


def tn(a, b):
    return lax.dot_general(a, b, (((0,), (0,)), ((), ())), preferred_element_type=F32)


class Spread:
    def __init__(self, wires, buf):
        self.wires, self.buf = wires, buf
        self.xl, self.c = (lax.axis_index(a) for a in SP)

    def block(self, xl, c, start=0, count=128):
        return self.buf.at[rows_of(256 * xl + 128 * c + start, count), :]

    def start(self):
        own = self.block(self.xl, self.c)
        go = self.wires.go
        self.far = []
        for i in range(2):
            part = self.block(self.xl, self.c, 64 * i, 64)
            self.far.append(go(part, part, turn("xl", 1, 2)))
        self.near = go(own, own, turn("c", 1, 2))

    def relay(self):
        self.relays = []
        for i in range(2):
            self.far[i].wait_recv()
            part = self.block(1 - self.xl, self.c, 64 * i, 64)
            self.relays.append(self.wires.go(part, part, turn("c", 1, 2)))

    def own_half(self):
        self.near.wait_recv()

    def done(self):
        for copy in self.relays:
            copy.wait_recv()


class Collect:
    def __init__(self, wires, part, pair, cross):
        self.wires, self.part, self.pair, self.cross = wires, part, pair, cross
        self.xl, self.c = (lax.axis_index(a) for a in SP)

    def block(self, xl, c):
        return self.part.at[rows_of(256 * xl + 128 * c, 128), :]

    def other(self):
        self.first = self.wires.go(self.block(1 - self.xl, 1 - self.c), self.pair.at[0], turn("c", 1, 2))

    def send(self):
        self.first.wait_recv()
        mine = self.block(1 - self.xl, self.c)
        for i in range(2):
            rows = pl.ds(64 * i, 64)
            add2(mine.at[rows, :], self.pair.at[0, rows, :])
        self.third = self.wires.go(mine, self.cross, turn("xl", 1, 2))

    def own(self):
        self.second = self.wires.go(self.block(self.xl, 1 - self.c), self.pair.at[1], turn("c", 1, 2))

    def wait(self):
        self.second.wait_recv()
        self.third.wait_recv()

    def release(self):
        for copy in (self.first, self.second, self.third):
            self.wires.sent(copy)

    def rows(self, start, count):
        at = rows_of(256 * self.xl + 128 * self.c + start, count)
        total = self.part[at, :].astype(F32) + self.pair[1, pl.ds(start, count), :].astype(F32)
        return total + self.cross[pl.ds(start, count), :].astype(F32)


def add2(dst, src):
    rows = dst.shape[0]

    @pl.loop(0, rows // 16)
    def _(i):
        at = (pl.ds(pl.multiple_of(i * 16, 16), 16), slice(None))
        dst[at] = (dst[at].astype(F32) + src[at].astype(F32)).astype(dst.dtype)


def normalize(stream):
    mean_part = jnp.mean(stream, axis=-1, keepdims=True)
    centred = stream - mean_part
    rstd = lax.rsqrt(jnp.mean(centred * centred, axis=-1, keepdims=True) + ln_eps)
    return (centred * rstd, rstd)


def norm_back(normed, rstd, incoming):
    first = jnp.mean(incoming, axis=-1, keepdims=True)
    second = jnp.mean(incoming * normed, axis=-1, keepdims=True)
    return rstd * (incoming - first - normed * second)


BLOCK = 16
ROOT = math.sqrt(2.0 / math.pi)


def by_rows(fn):
    @pl.loop(0, 128 // BLOCK)
    def _(i):
        fn(pl.multiple_of(i * BLOCK, BLOCK))


def block_kernel(
    x_ref, m_ref, og_ref, wq_ref, wo_ref, wi_ref, wb_ref,
    final_ref, ig_ref, sums_ref,
    w, g, last, a1, dm, a2, da, qkv, o, do, gp, act, part0, part1, pair0, cross0, pair1, cross1,
    mid, dmid, acck, accv, send, recv, local_sem, *bufs,
):
    z, y, xh, xl, c = (lax.axis_index(a) for a in FSDP + SP)
    shard_rows = rows_of(96 * y + 48 * xh, 48)
    loads = []
    for i, (ref, at, count) in enumerate(
        ((wq_ref, 0, 1152), (wo_ref, 1152, 384), (wi_ref, 1536, 1536), (wb_ref, 3072, 1536))
    ):
        load = pltpu.make_async_copy(ref, w.at[z, shard_rows, pl.ds(at, count)], local_sem.at[i])
        load.start()
        loads.append(load)
    greet(sp=True)
    wires = Wires(send, recv)
    ag = Gather(wires, w)
    rs = make_scatter(wires, g, bufs, last, sums_ref)
    own_row = 256 * xl + 128 * c
    own_start, other_start = 256 * xl, 256 * (1 - xl)
    scale = 1.0 / math.sqrt(32 * 512)
    factor = temper / math.sqrt(HEAD_DIM)

    def mod(i):
        return m_ref[pl.ds(i, 1), :]

    def own(start):
        return (rows_of(own_row + start, BLOCK), slice(None))

    def weights(start, count):
        return w[:, :, pl.ds(start, count)].reshape(1536, count)

    loads[0].wait()
    ag.s1(0)

    def first_norm(r):
        n1, _ = normalize(x_ref[pl.ds(r, BLOCK), :].astype(F32))
        a1[own(r)] = (n1 * (1.0 + mod(1)) + mod(0)).astype(BF)

    by_rows(first_norm)
    sp1 = Spread(wires, a1)
    sp1.start()
    for load in loads[1:]:
        load.wait()
    ag.s1(1)
    ag.s1(2)
    ag.s2(0)

    def gate_grad(r):
        dm[own(r)] = (mod(5) * og_ref[pl.ds(r, BLOCK), :].astype(F32)).astype(BF)

    by_rows(gate_grad)
    ag.s2b(0)
    ag.s3(0)
    ag.s2(1)
    ag.s1(3)
    sp1.relay()
    spm = Spread(wires, dm)
    spm.start()
    ag.s2b(1)
    ag.s2(2)
    ag.s3b(0)
    ag.s3(1)
    ag.s2b(2)
    ag.s2(3)
    sp1.own_half()
    sp1.done()
    ag.done(0)

    def project_qkv(start, count):
        qkv[:, pl.ds(start, count)] = nn(a1[...], weights(start, count)).astype(BF)

    @pl.loop(0, 4)
    def _(j):
        project_qkv(pl.multiple_of(j * 256, 256), 256)

    project_qkv(1024, 128)
    ag.s3b(1)
    ag.s3(2)
    ag.s2b(3)

    def probs(q, k):
        s = nt(q, k) * factor
        e = jnp.exp(s - jnp.max(s, axis=-1, keepdims=True))
        return e, 1.0 / jnp.sum(e, axis=-1, keepdims=True)

    def lanes(h, which):
        return pl.ds(pl.multiple_of(384 * which + 128 * h, 128), 128)

    @pl.loop(0, 3)
    def _(h):
        k, v = qkv[:, lanes(h, 1)], qkv[:, lanes(h, 2)]

        @pl.loop(0, 4)
        def _(i):
            rows = pl.ds(pl.multiple_of(i * 128, 128), 128)
            e, inv = probs(qkv[rows, lanes(h, 0)], k)
            o[rows, lanes(h, 0)] = (nn(e.astype(BF), v) * inv).astype(BF)

    ag.done(1)

    def back_half(dst, lhs, start, at, count):
        rows = rows_of(start, 256)

        @pl.loop(0, 2)
        def _(j):
            rhs = w[pl.ds(2 * j, 2), :, pl.ds(at, count)].reshape(768, count)
            dst[rows, pl.ds(pl.multiple_of(768 * j, 128), 768)] = nt(lhs[rows, :], rhs).astype(BF)

    def collect(red, dst, lhs, at, count):
        back_half(dst, lhs, other_start, at, count)
        red.other()
        back_half(dst, lhs, own_start, at, count)
        red.own()
        red.send()

    red1 = Collect(wires, part0, pair0, cross0)
    collect(red1, part0, o, 1152, 384)
    spm.relay()
    red1.wait()

    def second_norm(r):
        rows = pl.ds(r, BLOCK)
        value = x_ref[rows, :].astype(F32) + mod(2) * red1.rows(r, BLOCK)
        mid[rows, :] = value
        n2, _ = normalize(value)
        a2[own(r)] = (n2 * (1.0 + mod(4)) + mod(3)).astype(BF)

    by_rows(second_norm)
    sp2 = Spread(wires, a2)
    sp2.start()
    ag.s3b(2)
    ag.s3(3)
    sp2.relay()
    sp2.own_half()
    ag.done(2)

    def hidden(start):
        rows = rows_of(start, 256)

        @pl.loop(0, 6)
        def _(j):
            at = pl.multiple_of(j * 256, 256)
            u = nn(a2[rows, :], weights(pl.multiple_of(1536 + at, 256), 256))
            sq = u * u
            t = jnp.tanh(ROOT * u * (1.0 + 0.044715 * sq))
            half = 0.5 * (1.0 + t)
            act[rows, pl.ds(at, 256)] = (u * half).astype(BF)
            slope = half + (0.5 * ROOT) * u * (1.0 - t * t) * (1.0 + (3 * 0.044715) * sq)
            gp[rows, pl.ds(at, 256)] = slope.astype(BF)

    hidden(own_start)
    sp2.done()
    hidden(other_start)
    spm.own_half()
    spm.done()

    def grad(left, right, right_at, at, count):
        @pl.loop(0, 4)
        def _(j):
            lhs = left[:, pl.ds(pl.multiple_of(384 * j, 128), 384)]
            value = tn(lhs, right[:, pl.ds(right_at, count)]) * scale
            g[j, :, pl.ds(at, count)] = value.astype(BF)

    grad(dm, act, 0, 3072, 768)
    grad(dm, act, 768, 3840, 768)
    rs.r1(3)
    ag.s3b(3)
    ag.done(3)

    @pl.loop(0, 6)
    def _(j):
        at = pl.multiple_of(j * 256, 256)
        cols = pl.ds(at, 256)
        dg = nn(dm[...], weights(pl.multiple_of(3072 + at, 256), 256))
        gp[:, cols] = (gp[:, cols].astype(F32) * dg).astype(BF)

    du = gp
    red1.release()
    red2 = Collect(wires, part0, pair0, cross0)
    collect(red2, part0, du, 1536, 1536)
    rs.r1b(3)
    grad(a2, du, 0, 1536, 768)
    grad(a2, du, 768, 2304, 768)
    rs.r1(2)
    red2.wait()

    def mid_grad(r):
        rows = pl.ds(r, BLOCK)
        n2, r2 = normalize(mid[rows, :])
        value = og_ref[rows, :].astype(F32) + norm_back(n2, r2, red2.rows(r, BLOCK) * (1.0 + mod(4)))
        dmid[rows, :] = value
        da[own(r)] = (mod(2) * value).astype(BF)

    by_rows(mid_grad)
    spa = Spread(wires, da)
    spa.start()
    rs.r2(3)
    back_half(part1, act, other_start, 3072, 1536)
    back_half(part1, act, own_start, 3072, 1536)
    spa.relay()
    rs.r1b(2)
    redf = Collect(wires, part1, pair1, cross1)
    redf.other()
    redf.own()
    redf.send()
    spa.own_half()

    def head_grads(start):
        rows = rows_of(start, 256)
        do[rows, :] = nn(da[rows, :], weights(1152, 384)).astype(BF)

    head_grads(own_start)
    spa.done()
    head_grads(other_start)
    grad(da, o, 0, 1152, 128)
    grad(da, o, 128, 1280, 256)
    rs.r1(1)
    rs.r2b(3)

    @pl.loop(0, 3)
    def _(h):
        k, v = qkv[:, lanes(h, 1)], qkv[:, lanes(h, 2)]
        acck[...] = jnp.zeros_like(acck)
        accv[...] = jnp.zeros_like(accv)

        @pl.loop(0, 4)
        def _(i):
            rows = pl.ds(pl.multiple_of(i * 128, 128), 128)
            q = qkv[rows, lanes(h, 0)]
            up = do[rows, lanes(h, 0)]
            e, inv = probs(q, k)
            p = e * inv
            dp = nt(up, v)
            ds = factor * p * (dp - jnp.sum(p * dp, axis=-1, keepdims=True))
            ds = ds.astype(BF)
            qkv[rows, lanes(h, 0)] = nn(ds, k).astype(BF)
            acck[...] += tn(ds, q)
            accv[...] += tn(p.astype(BF), up)

        qkv[:, lanes(h, 1)] = acck[...].astype(BF)
        qkv[:, lanes(h, 2)] = accv[...].astype(BF)

    grad(a1, qkv, 0, 0, 640)
    grad(a1, qkv, 640, 640, 512)
    rs.r1(0)
    red2.release()
    red3 = Collect(wires, part0, pair0, cross0)
    collect(red3, part0, qkv, 0, 1152)
    rs.r2(2)
    rs.r1b(1)
    rs.r3(3)
    rs.r1b(0)
    rs.r2b(2)
    rs.r2(1)
    redf.wait()

    def last_out(r):
        rows = pl.ds(r, BLOCK)
        final_ref[rows, :] = (mid[rows, :] + mod(5) * redf.rows(r, BLOCK)).astype(BF)

    by_rows(last_out)
    rs.done(3)
    red3.wait()

    def first_grad(r):
        rows = pl.ds(r, BLOCK)
        n1, r1 = normalize(x_ref[rows, :].astype(F32))
        ig_ref[rows, :] = dmid[rows, :] + norm_back(n1, r1, red3.rows(r, BLOCK) * (1.0 + mod(1)))

    by_rows(first_grad)
    rs.r3(2)
    rs.r2b(1)
    rs.r2(0)
    rs.done(2)
    rs.r3(1)
    rs.r2b(0)
    rs.done(1)
    rs.r3(0)
    rs.done(0)
    wires.drain()


def body(tokens, modulation, w_qkv, w_out, w_in, w_back, out_grad):
    own = w_qkv.shape[3]
    vmem = pl.BlockSpec(memory_space=pltpu.VMEM)
    far = pl.BlockSpec(memory_space=pl.ANY)
    copies = 34 * len(CHUNKS) + 32
    rows = lambda n, dtype=BF: pltpu.VMEM((512, n), dtype)
    final, grad_in_rows, sums = pl.pallas_call(
        block_kernel,
        out_shape=(
            jax.ShapeDtypeStruct((128, 1536), BF),
            jax.ShapeDtypeStruct((128, 1536), F32),
            jax.ShapeDtypeStruct((48, WIDTH), F32),
        ),
        in_specs=[vmem, vmem, vmem, far, far, far, far],
        out_specs=(vmem, vmem, vmem),
        scratch_shapes=[
            pltpu.VMEM((4, 384, WIDTH), BF),
            pltpu.VMEM((4, 384, WIDTH), BF),
            pltpu.VMEM((48, WIDTH), BF),
            rows(1536), rows(1536), rows(1536), rows(1536),
            rows(1152), rows(384), rows(384),
            rows(1536), rows(1536), rows(1536), rows(1536),
            pltpu.VMEM((2, 128, 1536), BF),
            pltpu.VMEM((128, 1536), BF),
            pltpu.VMEM((2, 128, 1536), BF),
            pltpu.VMEM((128, 1536), BF),
            pltpu.VMEM((128, 1536), F32),
            pltpu.VMEM((128, 1536), F32),
            rows(128, F32), rows(128, F32),
            pltpu.SemaphoreType.DMA((copies,)),
            pltpu.SemaphoreType.DMA((copies,)),
            pltpu.SemaphoreType.DMA((4,)),
            *scatter_buffers(),
        ],
        compiler_params=pltpu.CompilerParams(
            collective_id=0, has_side_effects=True, vmem_limit_bytes=VMEM_LIMIT
        ),
        name="block",
    )(
        tokens[0],
        modulation[0, 0],
        out_grad[0],
        w_qkv[0].reshape(48, 3 * own),
        w_out[0].T,
        w_in[0],
        w_back[0].T,
    )
    return (
        final[None],
        grad_in_rows[None],
        sums[:, :1152].reshape(1, 48, 3, own),
        sums[:, 1152:1536].T[None],
        sums[:, 1536:3072][None],
        sums[:, 3072:].T[None],
    )


def solution(mesh):
    torus = Mesh(mesh.devices.reshape(4, 4, 2, 2, 2), FSDP + SP)
    return jax.shard_map(
        body,
        mesh=torus,
        in_specs=(
            P(FSDP, SP, None),
            P(FSDP, None, None, None),
            P(None, FSDP, None, SP),
            P(None, SP, FSDP),
            P(None, FSDP, SP),
            P(None, SP, FSDP),
            P(FSDP, SP, None),
        ),
        out_specs=(
            P(FSDP, SP, None),
            P(FSDP, SP, None),
            P(None, FSDP, None, SP),
            P(None, SP, FSDP),
            P(None, FSDP, SP),
            P(None, SP, FSDP),
        ),
        check_vma=False,
    )
```

```python
import functools
import math

import jax
import jax.numpy as jnp
from jax import lax
from jax.experimental import pallas as pl
from jax.experimental.pallas import tpu as pltpu
from jax.sharding import Mesh
from jax.sharding import PartitionSpec as P

HEAD_DIM = 128
MESH = pl.DeviceIdType.MESH
FSDP = ("z", "y", "xh")
SP = ("xl", "c")
BF = jnp.bfloat16
F32 = jnp.float32

ln_eps = 1e-06
temper = 2.5
VMEM_LIMIT = 67_000_000

CHUNKS = (
    ((0, 256), (256, 128)),
    ((384, 384), (768, 384)),
    ((1152, 128), (1280, 256)),
    ((1536, 384), (1920, 384)),
    ((2304, 384), (2688, 384)),
    ((3072, 384), (3456, 384)),
    ((3840, 384), (4224, 384)),
)
WIDTH = 4608
ORDER = (
    "load_first",
    "ag_s1_0",
    "load_inputs",
    "first_norm_0",
    "load_rest",
    "ag_s1_2",
    "ag_s1_1",
    "ag_s1_3",
    "ag_s2_0",
    "gate_grad",
    "ag_s1_6",
    "ag_s2_2",
    "first_norm_1",
    "ag_s2b_0",
    "a1_start_1",
    "ag_s2b_2",
    "ag_s2_1",
    "a1_start_0",
    "ag_s3_0",
    "ag_s3_2",
    "ag_s1_4",
    "dm_start_0",
    "ag_s2b_1",
    "ag_s2_3",
    "ag_s3b_2",
    "ag_s3_1",
    "ag_s2b_3",
    "a1_relay_0",
    "dm_start_1",
    "ag_s3b_0",
    "ag_done_2",
    "ag_s3b_1",
    "a1_relay_1",
    "ag_s2_6",
    "ag_s2_4",
    "a1_own_half",
    "ag_s1_5",
    "a1_done",
    "ag_done_0",
    "project_0",
    "ag_s3_3",
    "attend_0",
    "ag_done_1",
    "dm_relay_0",
    "dm_relay_1",
    "project_1",
    "attend_other",
    "dm_release",
    "att_mm_other",
    "ag_s2b_4",
    "ag_s2_5",
    "dm_own_half",
    "ag_s2b_6",
    "att_other",
    "attend_own",
    "att_mm_own",
    "att_own",
    "att_send",
    "ag_s3_4",
    "ag_s2b_5",
    "att_wait_0",
    "ag_s3b_3",
    "second_norm_0",
    "ag_s3b_4",
    "a2_start_0",
    "att_wait_1",
    "ag_s3_5",
    "second_norm_1",
    "att_release",
    "ag_s3_6",
    "a2_relay_0",
    "a2_start_1",
    "a2_relay_1",
    "ag_s3b_5",
    "a2_done",
    "a2_own_half",
    "ag_done_4",
    "ag_done_3",
    "hidden_other_1",
    "hidden_other_0",
    "dm_done",
    "hidden_own_0",
    "hidden_own_1",
    "ag_s3b_6",
    "grad_back_1",
    "rs_r1_6",
    "grad_back_0",
    "ag_done_5",
    "rs_r1_5",
    "hidden_grad_0",
    "ag_done_6",
    "hidden_grad_1",
    "da2_mm_other",
    "da2_other",
    "rs_r1b_6",
    "da2_mm_own",
    "da2_send",
    "grad_in_1",
    "grad_in_0",
    "da2_own",
    "rs_r1b_5",
    "da2_wait_0",
    "rs_r1_4",
    "mid_grad_0",
    "ffn_mm_own",
    "rs_r1_3",
    "da_start_0",
    "da2_wait_1",
    "mid_grad_1",
    "da_start_1",
    "rs_r2_6",
    "rs_r2_5",
    "rs_r1b_4",
    "da_own_half",
    "da_relay_0",
    "ffn_mm_other",
    "ffn_other",
    "da2_release",
    "ffn_own",
    "da_relay_1",
    "ffn_send",
    "heads_own",
    "rs_r1b_3",
    "da_done",
    "heads_other",
    "attend_back_0",
    "attend_back_1",
    "da1_mm_own",
    "ffn_wait_0",
    "grad_q_1",
    "rs_r2_4",
    "rs_r1_1",
    "da1_own",
    "da1_mm_other",
    "da1_other",
    "rs_r2b_5",
    "grad_out",
    "rs_r2_3",
    "rs_r2b_6",
    "rs_r1b_1",
    "rs_r1_2",
    "da1_send",
    "ffn_wait_1",
    "rs_r3_5",
    "grad_q_0",
    "rs_r2b_3",
    "rs_r1_0",
    "rs_r2b_4",
    "rs_r2_1",
    "last_out",
    "rs_r1b_0",
    "rs_r3_3",
    "da1_wait_0",
    "rs_r1b_2",
    "rs_r2b_1",
    "da1_wait_1",
    "rs_r3_6",
    "rs_r3_4",
    "rs_r2_0",
    "rs_r2_2",
    "rs_done_6",
    "rs_r3_1",
    "rs_r2b_0",
    "rs_done_3",
    "rs_r2b_2",
    "rs_r3_0",
    "rs_r3_2",
    "first_grad",
    "rs_done_5",
    "rs_done_4",
    "rs_done_0",
    "rs_done_1",
    "rs_done_2",
    "finish",
)


def turn(axis, step, size):
    return {axis: lax.rem(lax.axis_index(axis) + step + size, size)}


def near(axis, step):
    return lax.rem(lax.axis_index(axis) + step + 4, 4)


class Wires:
    def __init__(self, send, recv):
        self.send, self.recv, self.used, self.open = send, recv, 0, []

    def go(self, src, dst, device):
        at = self.used
        self.used += 1
        copy = pltpu.make_async_remote_copy(
            src_ref=src,
            dst_ref=dst,
            send_sem=self.send.at[at],
            recv_sem=self.recv.at[at],
            device_id=device,
            device_id_type=MESH,
        )
        copy.start()
        self.open.append(copy)
        return copy

    def sent(self, copy):
        copy.wait_send()
        self.open = [other for other in self.open if other is not copy]

    def drain(self):
        for copy in self.open:
            copy.wait_send()
        self.open = []


def greet(sp=False):
    barrier = pltpu.get_barrier_semaphore()
    targets = [turn("z", 1, 4), turn("z", -1, 4), turn("y", 1, 4), turn("y", -1, 4), turn("xh", 1, 2)]
    if sp:
        targets += [turn("xl", 1, 2), turn("c", 1, 2)]
    for device in targets:
        pl.semaphore_signal(barrier, inc=1, device_id=device, device_id_type=MESH)
    pl.semaphore_wait(barrier, len(targets))


def rows_of(start, count):
    return pl.ds(pl.multiple_of(start, 16), count)


def cols_of(cols):
    return pl.ds(cols[0], cols[1])


class Gather:
    def __init__(self, wires, w):
        self.wires, self.w = wires, w
        self.z, self.y, self.xh = (lax.axis_index(a) for a in FSDP)
        self.one, self.two, self.relay2, self.three, self.relay3 = {}, {}, {}, {}, {}

    def same(self, part, device):
        return self.wires.go(part, part, device)

    def s1(self, k):
        (a0, an), (b0, bn) = CHUNKS[k]
        part = self.w.at[self.z, rows_of(96 * self.y + 48 * self.xh, 48), pl.ds(a0, an + bn)]
        self.one[k] = self.same(part, turn("xh", 1, 2))

    def s2(self, k):
        self.one[k].wait_recv()
        ca, cb = map(cols_of, CHUNKS[k])
        pa = self.w.at[self.z, rows_of(96 * self.y, 96), ca]
        pb = self.w.at[self.z, rows_of(96 * self.y, 96), cb]
        self.two[k] = [
            self.same(pa, turn("y", 1, 4)),
            self.same(pa, turn("y", -1, 4)),
            self.same(pb, turn("z", 1, 4)),
            self.same(pb, turn("z", -1, 4)),
        ]

    def s2b(self, k):
        ca, cb = map(cols_of, CHUNKS[k])
        for copy in self.two[k]:
            copy.wait_recv()
        w, z, y = self.w, self.z, self.y
        self.relay2[k] = [
            self.same(w.at[z, rows_of(96 * near("y", -1), 48), ca], turn("y", 1, 4)),
            self.same(w.at[z, rows_of(96 * near("y", 1) + 48, 48), ca], turn("y", -1, 4)),
            self.same(w.at[near("z", -1), rows_of(96 * y, 48), cb], turn("z", 1, 4)),
            self.same(w.at[near("z", 1), rows_of(96 * y + 48, 48), cb], turn("z", -1, 4)),
        ]

    def s3(self, k):
        ca, cb = map(cols_of, CHUNKS[k])
        for copy in self.relay2[k]:
            copy.wait_recv()
        pa = self.w.at[self.z, :, ca]
        pb = self.w.at[:, rows_of(96 * self.y, 96), cb]
        self.three[k] = [
            self.same(pa, turn("z", 1, 4)),
            self.same(pa, turn("z", -1, 4)),
            self.same(pb, turn("y", 1, 4)),
            self.same(pb, turn("y", -1, 4)),
        ]

    def s3b(self, k):
        ca, cb = map(cols_of, CHUNKS[k])
        for copy in self.three[k]:
            copy.wait_recv()
        w = self.w
        self.relay3[k] = [
            self.same(w.at[near("z", -1), pl.ds(0, 192), ca], turn("z", 1, 4)),
            self.same(w.at[near("z", 1), pl.ds(192, 192), ca], turn("z", -1, 4)),
            self.same(w.at[:, rows_of(96 * near("y", -1), 48), cb], turn("y", 1, 4)),
            self.same(w.at[:, rows_of(96 * near("y", 1) + 48, 48), cb], turn("y", -1, 4)),
        ]

    def done(self, k):
        for copy in self.relay3[k]:
            copy.wait_recv()


def add_into(dst, *srcs):
    planes, rows, columns = dst.shape

    @pl.loop(0, planes * (rows // 48))
    def _(i):
        at = (i // (rows // 48), pl.ds(pl.multiple_of((i % (rows // 48)) * 48, 48), 48), slice(None))
        total = dst[at].astype(F32)
        for src in srcs:
            total = total + src[at].astype(F32)
        dst[at] = total.astype(dst.dtype)


class Scatter:
    def __init__(self, wires, g, half_a, full_a, half_b, full_b, half2, full2, last, out):
        self.wires, self.g, self.out = wires, g, out
        self.half_a, self.full_a, self.half_b, self.full_b = half_a, full_a, half_b, full_b
        self.half2, self.full2, self.last = half2, full2, last
        self.z, self.y, self.xh = (lax.axis_index(a) for a in FSDP)
        self.copies = {}

    def block_a(self, step, start, count, cols):
        return self.g.at[pl.ds(near("z", step), 1), pl.ds(start, count), cols]

    def block_b(self, step, start, count, cols):
        return self.g.at[:, rows_of(96 * near("y", step) + start, count), cols]

    def sub_a(self, step, start, count, cols):
        return self.g.at[pl.ds(self.z, 1), rows_of(96 * near("y", step) + start, count), cols]

    def sub_b(self, step, start, count, cols):
        return self.g.at[pl.ds(near("z", step), 1), rows_of(96 * self.y + start, count), cols]

    def r1(self, k):
        ca, cb = map(cols_of, CHUNKS[k])
        go = self.wires.go
        self.copies[k, 1] = [
            go(self.block_a(2, 0, 192, ca), self.half_a[k].at[pl.ds(0, 1)], turn("z", 1, 4)),
            go(self.block_a(2, 192, 192, ca), self.half_a[k].at[pl.ds(1, 1)], turn("z", -1, 4)),
            go(self.block_b(2, 0, 48, cb), self.half_b[k].at[0], turn("y", 1, 4)),
            go(self.block_b(2, 48, 48, cb), self.half_b[k].at[1], turn("y", -1, 4)),
        ]

    def r1b(self, k):
        ca, cb = map(cols_of, CHUNKS[k])
        go, copies = self.wires.go, self.copies[k, 1]
        sent = []
        copies[0].wait_recv()
        add_into(self.block_a(1, 0, 192, ca), self.half_a[k].at[pl.ds(0, 1)])
        sent.append(go(self.block_a(1, 0, 384, ca), self.full_a[k].at[pl.ds(0, 1)], turn("z", 1, 4)))
        copies[1].wait_recv()
        add_into(self.block_a(-1, 192, 192, ca), self.half_a[k].at[pl.ds(1, 1)])
        sent.append(go(self.block_a(-1, 0, 384, ca), self.full_a[k].at[pl.ds(1, 1)], turn("z", -1, 4)))
        copies[2].wait_recv()
        add_into(self.block_b(1, 0, 48, cb), self.half_b[k].at[0])
        sent.append(go(self.block_b(1, 0, 96, cb), self.full_b[k].at[0], turn("y", 1, 4)))
        copies[3].wait_recv()
        add_into(self.block_b(-1, 48, 48, cb), self.half_b[k].at[1])
        sent.append(go(self.block_b(-1, 0, 96, cb), self.full_b[k].at[1], turn("y", -1, 4)))
        self.copies[k, 2] = sent

    def r2(self, k):
        ca, cb = map(cols_of, CHUNKS[k])
        go, copies = self.wires.go, self.copies[k, 2]
        copies[0].wait_recv()
        copies[1].wait_recv()
        add_into(
            self.block_a(0, 0, 384, ca), self.full_a[k].at[pl.ds(0, 1)], self.full_a[k].at[pl.ds(1, 1)]
        )
        sent = [
            go(self.sub_a(2, 0, 48, ca), self.half2[k][0].at[pl.ds(0, 1)], turn("y", 1, 4)),
            go(self.sub_a(2, 48, 48, ca), self.half2[k][0].at[pl.ds(1, 1)], turn("y", -1, 4)),
        ]
        copies[2].wait_recv()
        copies[3].wait_recv()
        add_into(self.block_b(0, 0, 96, cb), self.full_b[k].at[0], self.full_b[k].at[1])
        sent += [
            go(self.sub_b(2, 0, 48, cb), self.half2[k][1].at[pl.ds(0, 1)], turn("z", 1, 4)),
            go(self.sub_b(2, 48, 48, cb), self.half2[k][1].at[pl.ds(1, 1)], turn("z", -1, 4)),
        ]
        self.copies[k, 3] = sent

    def r2b(self, k):
        go, copies = self.wires.go, self.copies[k, 3]
        sent = []
        for colour, (sub, axis) in enumerate(((self.sub_a, "y"), (self.sub_b, "z"))):
            cols = cols_of(CHUNKS[k][colour])
            half, full = self.half2[k][colour], self.full2[k][colour]
            copies[2 * colour].wait_recv()
            add_into(sub(1, 0, 48, cols), half.at[pl.ds(0, 1)])
            sent.append(go(sub(1, 0, 96, cols), full.at[pl.ds(0, 1)], turn(axis, 1, 4)))
            copies[2 * colour + 1].wait_recv()
            add_into(sub(-1, 48, 48, cols), half.at[pl.ds(1, 1)])
            sent.append(go(sub(-1, 0, 96, cols), full.at[pl.ds(1, 1)], turn(axis, -1, 4)))
        self.copies[k, 4] = sent

    def r3(self, k):
        go, copies = self.wires.go, self.copies[k, 4]
        (a0, an), (b0, bn) = CHUNKS[k]
        for colour, sub in enumerate((self.sub_a, self.sub_b)):
            cols, full = cols_of(CHUNKS[k][colour]), self.full2[k][colour]
            copies[2 * colour].wait_recv()
            copies[2 * colour + 1].wait_recv()
            add_into(sub(0, 0, 96, cols), full.at[pl.ds(0, 1)], full.at[pl.ds(1, 1)])
        part = self.g.at[self.z, rows_of(96 * self.y + 48 * (1 - self.xh), 48), pl.ds(a0, an + bn)]
        self.copies[k, 5] = [go(part, self.last.at[:, pl.ds(a0, an + bn)], turn("xh", 1, 2))]

    def done(self, k):
        (a0, an), (b0, bn) = CHUNKS[k]
        self.copies[k, 5][0].wait_recv()
        cols = pl.ds(a0, an + bn)
        own = self.g[self.z, rows_of(96 * self.y + 48 * self.xh, 48), cols]
        total = own.astype(F32) + self.last[:, cols].astype(F32)
        if a0 >= 1152:
            self.out[:, cols] = total
            return
        for at in range(0, an + bn, 128):
            head, which = (a0 + at) // 384, (a0 + at) % 384 // 128
            self.out[:, pl.ds(384 * which + 128 * head, 128)] = total[:, at : at + 128]


def scatter_buffers():
    shapes = []
    for (a0, an), (b0, bn) in CHUNKS:
        shapes += [
            pltpu.VMEM((2, 192, an), BF),
            pltpu.VMEM((2, 384, an), BF),
            pltpu.VMEM((2, 4, 48, bn), BF),
            pltpu.VMEM((2, 4, 96, bn), BF),
            pltpu.VMEM((2, 48, an), BF),
            pltpu.VMEM((2, 96, an), BF),
            pltpu.VMEM((2, 48, bn), BF),
            pltpu.VMEM((2, 96, bn), BF),
        ]
    return shapes


def make_scatter(wires, g, bufs, last, out):
    n = len(CHUNKS)
    groups = [bufs[8 * k : 8 * k + 8] for k in range(n)]
    return Scatter(
        wires,
        g,
        [b[0] for b in groups],
        [b[1] for b in groups],
        [b[2] for b in groups],
        [b[3] for b in groups],
        [(b[4], b[6]) for b in groups],
        [(b[5], b[7]) for b in groups],
        last,
        out,
    )


def nn(a, b):
    return jnp.dot(a, b, preferred_element_type=F32)


def nt(a, b):
    return lax.dot_general(a, b, (((1,), (1,)), ((), ())), preferred_element_type=F32)


def tn(a, b):
    return lax.dot_general(a, b, (((0,), (0,)), ((), ())), preferred_element_type=F32)


class Spread:
    def __init__(self, wires, buf):
        self.wires, self.buf = wires, buf
        self.xl, self.c = (lax.axis_index(a) for a in SP)
        self.far, self.near, self.relays = {}, {}, {}

    def block(self, xl, c, start=0, count=128):
        return self.buf.at[rows_of(256 * xl + 128 * c + start, count), :]

    def start(self, i):
        part = self.block(self.xl, self.c, 64 * i, 64)
        self.far[i] = self.wires.go(part, part, turn("xl", 1, 2))
        self.near[i] = self.wires.go(part, part, turn("c", 1, 2))

    def relay(self, i):
        self.far[i].wait_recv()
        part = self.block(1 - self.xl, self.c, 64 * i, 64)
        self.relays[i] = self.wires.go(part, part, turn("c", 1, 2))

    def own_half(self):
        for copy in self.near.values():
            copy.wait_recv()

    def done(self):
        for copy in self.relays.values():
            copy.wait_recv()

    def release(self):
        for group in (self.far, self.near, self.relays):
            for copy in group.values():
                self.wires.sent(copy)


class Collect:
    def __init__(self, wires, part, pair, cross):
        self.wires, self.part, self.pair, self.cross = wires, part, pair, cross
        self.xl, self.c = (lax.axis_index(a) for a in SP)

    def block(self, xl, c):
        return self.part.at[rows_of(256 * xl + 128 * c, 128), :]

    def other(self):
        self.first = self.wires.go(self.block(1 - self.xl, 1 - self.c), self.pair.at[0], turn("c", 1, 2))

    def send(self):
        self.first.wait_recv()
        self.third = []
        for i in range(2):
            rows = pl.ds(64 * i, 64)
            mine = self.block(1 - self.xl, self.c).at[rows, :]
            add2(mine, self.pair.at[0, rows, :])
            self.third.append(self.wires.go(mine, self.cross.at[rows, :], turn("xl", 1, 2)))

    def own(self):
        self.second = self.wires.go(self.block(self.xl, 1 - self.c), self.pair.at[1], turn("c", 1, 2))

    def wait(self, i):
        if i == 0:
            self.second.wait_recv()
        self.third[i].wait_recv()

    def release(self):
        for copy in (self.first, self.second, *self.third):
            self.wires.sent(copy)

    def rows(self, start, count):
        at = rows_of(256 * self.xl + 128 * self.c + start, count)
        total = self.part[at, :].astype(F32) + self.pair[1, pl.ds(start, count), :].astype(F32)
        return total + self.cross[pl.ds(start, count), :].astype(F32)


def add2(dst, src):
    rows = dst.shape[0]

    @pl.loop(0, rows // 16)
    def _(i):
        at = (pl.ds(pl.multiple_of(i * 16, 16), 16), slice(None))
        dst[at] = (dst[at].astype(F32) + src[at].astype(F32)).astype(dst.dtype)


def normalize(stream):
    mean_part = jnp.mean(stream, axis=-1, keepdims=True)
    centred = stream - mean_part
    rstd = lax.rsqrt(jnp.mean(centred * centred, axis=-1, keepdims=True) + ln_eps)
    return (centred * rstd, rstd)


def norm_back(normed, rstd, incoming):
    first = jnp.mean(incoming, axis=-1, keepdims=True)
    second = jnp.mean(incoming * normed, axis=-1, keepdims=True)
    return rstd * (incoming - first - normed * second)


BLOCK = 16
ROOT = math.sqrt(2.0 / math.pi)


def by_rows(fn, start=0, count=128):
    @pl.loop(start // BLOCK, (start + count) // BLOCK)
    def _(i):
        fn(pl.multiple_of(i * BLOCK, BLOCK))


def block_kernel(
    x_in, m_in, og_in, wq_ref, wo_ref, wi_ref, wb_ref,
    final_out, ig_out, sums_out,
    x_ref, m_ref, og_ref, final_ref, ig_ref, sums_ref,
    w, g, last, a1, dm, a2, da, qkv, o, do, gp, act, part, probs, dv, pair0, cross0, pair1, cross1,
    mid, dmid, send, recv, local_sem, *bufs,
):
    z, y, xh, xl, c = (lax.axis_index(a) for a in FSDP + SP)
    shard_rows = rows_of(96 * y + 48 * xh, 48)
    pieces = [(wq_ref, 384 * which + 128 * h, 384 * h + 128 * which, 128) for h in range(3) for which in range(3)]
    pieces += [(wo_ref, 0, 1152, 384), (wi_ref, 0, 1536, 1536), (wb_ref, 0, 3072, 1536)]
    loads = [
        pltpu.make_async_copy(
            ref.at[:, pl.ds(at, count)], w.at[z, shard_rows, pl.ds(to, count)], local_sem.at[i]
        )
        for i, (ref, at, to, count) in enumerate(pieces)
    ]
    inputs = [
        pltpu.make_async_copy(a, b, local_sem.at[12 + i])
        for i, (a, b) in enumerate(((x_in, x_ref), (m_in, m_ref), (og_in, og_ref)))
    ]
    outputs = {
        name: pltpu.make_async_copy(a, b, local_sem.at[15 + i])
        for i, (name, a, b) in enumerate(
            (("final", final_ref, final_out), ("ig", ig_ref, ig_out), ("sums", sums_ref, sums_out))
        )
    }
    for load in loads[:3] + inputs[:2] + loads[3:] + inputs[2:]:
        load.start()
    with jax.named_scope("greet"):
        greet(sp=True)
    wires = Wires(send, recv)
    ag = Gather(wires, w)
    rs = make_scatter(wires, g, bufs, last, sums_ref)
    own_row = 256 * xl + 128 * c
    own_start, other_start = 256 * xl, 256 * (1 - xl)
    scale = 1.0 / math.sqrt(32 * 512)
    factor = temper / math.sqrt(HEAD_DIM)
    steps = {}

    def step(fn):
        steps[fn.__name__] = fn
        return fn

    def mod(i):
        return m_ref[pl.ds(i, 1), :]

    def own(start):
        return (rows_of(own_row + start, BLOCK), slice(None))

    def weights(start, count):
        return w[:, :, pl.ds(start, count)].reshape(1536, count)

    for k in range(len(CHUNKS)):
        for name in ("s1", "s2", "s2b", "s3", "s3b", "done"):
            steps[f"ag_{name}_{k}"] = functools.partial(getattr(ag, name), k)
        for name in ("r1", "r1b", "r2", "r2b", "r3", "done"):
            steps[f"rs_{name}_{k}"] = functools.partial(getattr(rs, name), k)
    for key, buf in (("a1", a1), ("dm", dm), ("a2", a2), ("da", da)):
        spread = Spread(wires, buf)
        for i in range(2):
            steps[f"{key}_start_{i}"] = functools.partial(spread.start, i)
            steps[f"{key}_relay_{i}"] = functools.partial(spread.relay, i)
        steps[f"{key}_own_half"] = spread.own_half
        steps[f"{key}_done"] = spread.done
        steps[f"{key}_release"] = spread.release
    reds = {
        "att": Collect(wires, part, pair0, cross0),
        "da2": Collect(wires, part, pair0, cross0),
        "da1": Collect(wires, part, pair0, cross0),
        "ffn": Collect(wires, dm, pair1, cross1),
    }
    for key, red in reds.items():
        for name in ("other", "own", "send", "release"):
            steps[f"{key}_{name}"] = getattr(red, name)
        for i in range(2):
            steps[f"{key}_wait_{i}"] = functools.partial(red.wait, i)

    @step
    def load_first():
        for load in loads[:3]:
            load.wait()

    @step
    def load_inputs():
        inputs[0].wait()
        inputs[1].wait()

    @step
    def load_rest():
        for load in loads[3:]:
            load.wait()
        inputs[2].wait()

    def first_norm(r):
        n1, _ = normalize(x_ref[pl.ds(r, BLOCK), :].astype(F32))
        a1[own(r)] = (n1 * (1.0 + mod(1)) + mod(0)).astype(BF)

    def second_norm(r):
        rows = pl.ds(r, BLOCK)
        value = x_ref[rows, :].astype(F32) + mod(2) * reds["att"].rows(r, BLOCK)
        mid[rows, :] = value
        n2, _ = normalize(value)
        a2[own(r)] = (n2 * (1.0 + mod(4)) + mod(3)).astype(BF)

    def mid_grad(r):
        rows = pl.ds(r, BLOCK)
        n2, r2 = normalize(mid[rows, :])
        inner = norm_back(n2, r2, reds["da2"].rows(r, BLOCK) * (1.0 + mod(4)))
        value = og_ref[rows, :].astype(F32) + inner
        dmid[rows, :] = value
        da[own(r)] = (mod(2) * value).astype(BF)

    for i in range(2):
        for fn in (first_norm, second_norm, mid_grad):
            steps[f"{fn.__name__}_{i}"] = functools.partial(by_rows, fn, 64 * i, 64)

    @step
    def gate_grad():
        def rows(r):
            dm[own(r)] = (mod(5) * og_ref[pl.ds(r, BLOCK), :].astype(F32)).astype(BF)

        by_rows(rows)

    def lanes(h, which):
        return pl.ds(384 * h + 128 * which, 128)

    def project(start, count):
        qkv[:, pl.ds(start, count)] = nn(a1[...], weights(start, count)).astype(BF)

    @step
    def project_0():
        project(0, 256)
        project(256, 128)

    @step
    def project_1():
        @pl.loop(0, 3)
        def _(j):
            project(pl.multiple_of(384 + j * 256, 128), 256)

    def attend(heads, start, blocks):
        @pl.loop(0, blocks)
        def _(i):
            rows = rows_of(start + i * 128, 128)
            for h in heads:
                s = nt(qkv[rows, lanes(h, 0)], qkv[:, lanes(h, 1)]) * factor
                e = jnp.exp(s - jnp.max(s, axis=-1, keepdims=True))
                p = (e * (1.0 / jnp.sum(e, axis=-1, keepdims=True))).astype(BF)
                probs[h, rows, :] = p
                o[rows, pl.ds(128 * h, 128)] = nn(p, qkv[:, lanes(h, 2)]).astype(BF)

    steps["attend_0"] = functools.partial(attend, (0,), 0, 4)
    steps["attend_other"] = functools.partial(attend, (1, 2), other_start, 2)
    steps["attend_own"] = functools.partial(attend, (1, 2), own_start, 2)

    def back_half(dst, lhs, start, at, count):
        rows = rows_of(start, 256)

        @pl.loop(0, 2)
        def _(j):
            rhs = w[pl.ds(2 * j, 2), :, pl.ds(at, count)].reshape(768, count)
            dst[rows, pl.ds(pl.multiple_of(768 * j, 128), 768)] = nt(lhs[rows, :], rhs).astype(BF)

    for key, dst, lhs, at, count in (
        ("att", part, o, 1152, 384),
        ("da2", part, gp, 1536, 1536),
        ("da1", part, qkv, 0, 1152),
        ("ffn", dm, act, 3072, 1536),
    ):
        steps[f"{key}_mm_other"] = functools.partial(back_half, dst, lhs, other_start, at, count)
        steps[f"{key}_mm_own"] = functools.partial(back_half, dst, lhs, own_start, at, count)

    def hidden(start, half):
        rows = rows_of(start, 256)

        @pl.loop(3 * half, 3 * half + 3)
        def _(j):
            at = pl.multiple_of(j * 256, 256)
            u = nn(a2[rows, :], weights(pl.multiple_of(1536 + at, 256), 256))
            sq = u * u
            t = jnp.tanh(ROOT * u * (1.0 + 0.044715 * sq))
            half = 0.5 * (1.0 + t)
            act[rows, pl.ds(at, 256)] = (u * half).astype(BF)
            slope = half + (0.5 * ROOT) * u * (1.0 - t * t) * (1.0 + (3 * 0.044715) * sq)
            gp[rows, pl.ds(at, 256)] = slope.astype(BF)

    def hidden_grad(half):
        @pl.loop(3 * half, 3 * half + 3)
        def _(j):
            at = pl.multiple_of(j * 256, 256)
            cols = pl.ds(at, 256)
            dg = nn(dm[...], weights(pl.multiple_of(3072 + at, 256), 256))
            gp[:, cols] = (gp[:, cols].astype(F32) * dg).astype(BF)

    def grad(left, right, right_at, at, count):
        @pl.loop(0, 4)
        def _(j):
            lhs = left[:, pl.ds(pl.multiple_of(384 * j, 128), 384)]
            value = tn(lhs, right[:, pl.ds(right_at, count)]) * scale
            g[j, :, pl.ds(at, count)] = value.astype(BF)

    for i in range(2):
        steps[f"hidden_own_{i}"] = functools.partial(hidden, own_start, i)
        steps[f"hidden_other_{i}"] = functools.partial(hidden, other_start, i)
        steps[f"hidden_grad_{i}"] = functools.partial(hidden_grad, i)
        steps[f"grad_in_{i}"] = functools.partial(grad, a2, gp, 768 * i, 1536 + 768 * i, 768)
        steps[f"grad_back_{i}"] = functools.partial(grad, dm, act, 768 * i, 3072 + 768 * i, 768)
    steps["grad_out"] = functools.partial(grad, da, o, 0, 1152, 384)
    steps["grad_q_0"] = functools.partial(grad, a1, qkv, 0, 0, 384)
    steps["grad_q_1"] = functools.partial(grad, a1, qkv, 384, 384, 768)

    def head_grads(start):
        rows = rows_of(start, 256)
        do[rows, :] = nn(da[rows, :], weights(1152, 384)).astype(BF)

    steps["heads_own"] = functools.partial(head_grads, own_start)
    steps["heads_other"] = functools.partial(head_grads, other_start)

    def attend_back(heads):
        for n, h in enumerate(heads):
            dv[n] = tn(probs[h], do[:, pl.ds(128 * h, 128)]).astype(BF)

        @pl.loop(0, 4)
        def _(i):
            rows = pl.ds(pl.multiple_of(i * 128, 128), 128)
            for h in heads:
                dp = nt(do[rows, pl.ds(128 * h, 128)], qkv[:, lanes(h, 2)])
                p = probs[h, rows, :].astype(F32)
                ds = factor * p * (dp - jnp.sum(p * dp, axis=-1, keepdims=True))
                probs[h, rows, :] = ds.astype(BF)

        for n, h in enumerate(heads):
            dk = tn(probs[h], qkv[:, lanes(h, 0)]).astype(BF)
            qkv[:, lanes(h, 0)] = nn(probs[h], qkv[:, lanes(h, 1)]).astype(BF)
            qkv[:, lanes(h, 1)] = dk
            qkv[:, lanes(h, 2)] = dv[n]

    steps["attend_back_0"] = functools.partial(attend_back, (0,))
    steps["attend_back_1"] = functools.partial(attend_back, (1, 2))

    @step
    def last_out():
        def each(r):
            rows = pl.ds(r, BLOCK)
            final_ref[rows, :] = (mid[rows, :] + mod(5) * reds["ffn"].rows(r, BLOCK)).astype(BF)

        by_rows(each)
        outputs["final"].start()

    @step
    def first_grad():
        def each(r):
            rows = pl.ds(r, BLOCK)
            n1, r1 = normalize(x_ref[rows, :].astype(F32))
            inner = norm_back(n1, r1, reds["da1"].rows(r, BLOCK) * (1.0 + mod(1)))
            ig_ref[rows, :] = dmid[rows, :] + inner

        by_rows(each)
        outputs["ig"].start()

    @step
    def finish():
        outputs["sums"].start()
        wires.drain()
        for copy in outputs.values():
            copy.wait()

    for name in ORDER:
        with jax.named_scope(name):
            steps[name]()


def body(tokens, modulation, w_qkv, w_out, w_in, w_back, out_grad):
    own = w_qkv.shape[3]
    far = pl.BlockSpec(memory_space=pl.ANY)
    copies = 34 * len(CHUNKS) + 40
    rows = lambda n, dtype=BF: pltpu.VMEM((512, n), dtype)
    final, grad_in_rows, sums = pl.pallas_call(
        block_kernel,
        out_shape=(
            jax.ShapeDtypeStruct((128, 1536), BF),
            jax.ShapeDtypeStruct((128, 1536), F32),
            jax.ShapeDtypeStruct((48, WIDTH), F32),
        ),
        in_specs=[far] * 7,
        out_specs=(far, far, far),
        scratch_shapes=[
            pltpu.VMEM((128, 1536), BF),
            pltpu.VMEM((6, 1536), F32),
            pltpu.VMEM((128, 1536), BF),
            pltpu.VMEM((128, 1536), BF),
            pltpu.VMEM((128, 1536), F32),
            pltpu.VMEM((48, WIDTH), F32),
            pltpu.VMEM((4, 384, WIDTH), BF),
            pltpu.VMEM((4, 384, WIDTH), BF),
            pltpu.VMEM((48, WIDTH), BF),
            rows(1536), rows(1536), rows(1536), rows(1536),
            rows(1152), rows(384), rows(384),
            rows(1536), rows(1536), rows(1536),
            pltpu.VMEM((3, 512, 512), BF),
            pltpu.VMEM((2, 512, 128), BF),
            pltpu.VMEM((2, 128, 1536), BF),
            pltpu.VMEM((128, 1536), BF),
            pltpu.VMEM((2, 128, 1536), BF),
            pltpu.VMEM((128, 1536), BF),
            pltpu.VMEM((128, 1536), F32),
            pltpu.VMEM((128, 1536), F32),
            pltpu.SemaphoreType.DMA((copies,)),
            pltpu.SemaphoreType.DMA((copies,)),
            pltpu.SemaphoreType.DMA((18,)),
            *scatter_buffers(),
        ],
        compiler_params=pltpu.CompilerParams(
            collective_id=0, has_side_effects=True, vmem_limit_bytes=VMEM_LIMIT
        ),
        name="block",
    )(
        tokens[0],
        modulation[0, 0],
        out_grad[0],
        w_qkv[0].reshape(48, 3 * own),
        w_out[0].T,
        w_in[0],
        w_back[0].T,
    )
    return (
        final[None],
        grad_in_rows[None],
        sums[:, :1152].reshape(1, 48, 3, own),
        sums[:, 1152:1536].T[None],
        sums[:, 1536:3072][None],
        sums[:, 3072:].T[None],
    )


def solution(mesh):
    torus = Mesh(mesh.devices.reshape(4, 4, 2, 2, 2), FSDP + SP)
    return jax.shard_map(
        body,
        mesh=torus,
        in_specs=(
            P(FSDP, SP, None),
            P(FSDP, None, None, None),
            P(None, FSDP, None, SP),
            P(None, SP, FSDP),
            P(None, FSDP, SP),
            P(None, SP, FSDP),
            P(FSDP, SP, None),
        ),
        out_specs=(
            P(FSDP, SP, None),
            P(FSDP, SP, None),
            P(None, FSDP, None, SP),
            P(None, SP, FSDP),
            P(None, FSDP, SP),
            P(None, SP, FSDP),
        ),
        check_vma=False,
    )
```

```python
import functools
import math

import jax
import jax.numpy as jnp
from jax import lax
from jax.experimental import pallas as pl
from jax.experimental.pallas import tpu as pltpu
from jax.sharding import Mesh
from jax.sharding import PartitionSpec as P

HEAD_DIM = 128
MESH = pl.DeviceIdType.MESH
FSDP = ("z", "y", "xh")
SP = ("xl", "c")
BF = jnp.bfloat16
F32 = jnp.float32

ln_eps = 1e-06
temper = 2.5
VMEM_LIMIT = 67_000_000

TILES = ((2, 1, 0), (3, 2, 1), (1, 2, 0), (2, 3, 1), (3, 2, 1), (2, 3, 1), (3, 2, 1))


def split_chunks():
    chunks, at = [], 0
    for tiles in TILES:
        parts = []
        for count in tiles:
            parts.append((at, 128 * count))
            at += 128 * count
        chunks.append(tuple(parts))
    return tuple(chunks)


CHUNKS = split_chunks()
WIDTH = 4608
ORDER = (
    "load_first",
    "met",
    "load_rest",
    "ag_c1_1",
    "ag_c1_4",
    "ag_s1_0",
    "ag_s1_4",
    "ag_s1_1",
    "load_inputs",
    "ag_s1_2",
    "ag_c2_1",
    "ag_s1_3",
    "ag_c1_5",
    "ag_c2_4",
    "first_norm_0",
    "a1_start_0",
    "ag_s2_0",
    "gate_grad",
    "ag_s2_4",
    "ag_s2_1",
    "ag_c1_3",
    "first_norm_1",
    "ag_s2_2",
    "dm_start_1",
    "ag_s2b_0",
    "ag_s2b_4",
    "dm_start_0",
    "ag_s2b_1",
    "ag_s2b_2",
    "ag_c2b_1",
    "ag_c1_6",
    "ag_s1_5",
    "ag_c2_5",
    "ag_s3_0",
    "ag_c2_6",
    "a1_relay_0",
    "ag_s1_6",
    "ag_s3_1",
    "a1_start_1",
    "ag_c2_3",
    "ag_c3_1",
    "ag_s2_3",
    "ag_s3b_0",
    "dm_own_half",
    "ag_c2b_4",
    "ag_s3_2",
    "ag_c2b_3",
    "ag_s3b_1",
    "dm_relay_0",
    "ag_c3_4",
    "a1_relay_1",
    "a1_done",
    "ag_done_0",
    "ag_s2b_3",
    "ag_s3b_2",
    "a1_own_half",
    "project_0",
    "ag_s2_5",
    "ag_s3_4",
    "dm_relay_1",
    "attend_0",
    "ag_c2b_6",
    "ag_done_1",
    "ag_s2_6",
    "project_1",
    "ag_c3_3",
    "ag_done_2",
    "attend_other",
    "att_mm_other",
    "att_other",
    "ag_s3_3",
    "attend_own",
    "att_send",
    "dm_done",
    "ag_c2b_5",
    "ag_s3b_4",
    "ag_s2b_5",
    "att_mm_own",
    "att_own",
    "att_wait_0",
    "second_norm_0",
    "a2_start_0",
    "ag_s2b_6",
    "ag_s3b_3",
    "att_wait_1",
    "second_norm_1",
    "a2_start_1",
    "ag_s3_6",
    "ag_c3_6",
    "a2_own_half",
    "ag_s3_5",
    "a2_relay_0",
    "a2_relay_1",
    "ag_done_3",
    "ag_done_4",
    "hidden_own_1",
    "hidden_own_0",
    "ag_c3_5",
    "att_release",
    "a2_done",
    "dm_release",
    "ag_s3b_6",
    "hidden_other_1",
    "hidden_other_0",
    "grad_back_1",
    "rs_c1_6",
    "ag_s3b_5",
    "grad_back_0",
    "ag_done_6",
    "rs_c1_5",
    "rs_r1_6",
    "rs_r1_5",
    "hidden_grad_1",
    "grad_in_1",
    "rs_r1_4",
    "ag_done_5",
    "hidden_grad_0",
    "rs_c1_4",
    "rs_r1b_6",
    "da2_mm_other",
    "da2_other",
    "da2_send",
    "da2_mm_own",
    "rs_r1b_5",
    "da2_own",
    "ffn_mm_other",
    "rs_c2_5",
    "grad_in_0",
    "da2_wait_0",
    "mid_grad_0",
    "rs_c2_6",
    "rs_c2_4",
    "da_start_0",
    "rs_r1b_4",
    "rs_c2b_6",
    "rs_c2b_5",
    "rs_r2_5",
    "rs_c2b_4",
    "da2_wait_1",
    "mid_grad_1",
    "da_start_1",
    "da_own_half",
    "rs_r2_6",
    "da2_release",
    "da_relay_0",
    "heads_own",
    "rs_r1_3",
    "ffn_other",
    "rs_c1_3",
    "rs_r2b_5",
    "da_relay_1",
    "ffn_mm_own",
    "rs_r2b_6",
    "da_done",
    "rs_c3_5",
    "grad_out",
    "heads_other",
    "rs_r1_2",
    "ffn_send",
    "rs_r1b_3",
    "rs_c3_6",
    "attend_back_1",
    "grad_q_1",
    "rs_r3_6",
    "rs_c4_5",
    "rs_r1b_2",
    "rs_r1_1",
    "attend_back_0",
    "ffn_own",
    "da1_mm_other",
    "rs_c1_1",
    "rs_r3_5",
    "ffn_wait_0",
    "rs_r2_4",
    "grad_q_0",
    "rs_r1_0",
    "da1_other",
    "da1_send",
    "rs_r2_3",
    "rs_c3_4",
    "rs_done_6",
    "rs_r1b_1",
    "da1_mm_own",
    "da1_own",
    "rs_c2_3",
    "rs_r1b_0",
    "rs_r2b_3",
    "da1_wait_0",
    "rs_r2_1",
    "rs_c4_6",
    "rs_r2_2",
    "rs_r2b_4",
    "da1_wait_1",
    "first_grad",
    "rs_r2_0",
    "rs_r2b_1",
    "rs_r2b_2",
    "ffn_wait_1",
    "rs_r3_3",
    "rs_c2_1",
    "rs_r3_4",
    "rs_r2b_0",
    "rs_c2b_3",
    "rs_r3_1",
    "rs_c2b_1",
    "rs_done_3",
    "rs_c4_4",
    "rs_r3_2",
    "rs_done_5",
    "rs_r3_0",
    "rs_c3_3",
    "rs_done_4",
    "rs_c3_1",
    "rs_done_1",
    "last_out",
    "rs_c4_3",
    "rs_done_2",
    "rs_done_0",
    "rs_c4_1",
    "finish",
)


def turn(axis, step, size):
    return {axis: lax.rem(lax.axis_index(axis) + step + size, size)}


def near(axis, step):
    return lax.rem(lax.axis_index(axis) + step + 4, 4)


class Wires:
    def __init__(self, send, recv):
        self.send, self.recv, self.used, self.open = send, recv, 0, []

    def go(self, src, dst, device):
        at = self.used
        self.used += 1
        copy = pltpu.make_async_remote_copy(
            src_ref=src,
            dst_ref=dst,
            send_sem=self.send.at[at],
            recv_sem=self.recv.at[at],
            device_id=device,
            device_id_type=MESH,
        )
        copy.start()
        self.open.append(copy)
        return copy

    def sent(self, copy):
        copy.wait_send()
        self.open = [other for other in self.open if other is not copy]

    def drain(self):
        for copy in self.open:
            copy.wait_send()
        self.open = []


def partners():
    return [turn("z", 1, 4), turn("z", -1, 4), turn("z", 2, 4), turn("y", 1, 4), turn("y", -1, 4)] + [
        turn(axis, 1, 2) for axis in ("xh", "xl", "c")
    ]


def greet():
    for device in partners():
        pl.semaphore_signal(
            pltpu.get_barrier_semaphore(), inc=1, device_id=device, device_id_type=MESH
        )


def met():
    pl.semaphore_wait(pltpu.get_barrier_semaphore(), len(partners()))


def rows_of(start, count):
    return pl.ds(pl.multiple_of(start, 16), count)


def cols_of(cols):
    return pl.ds(cols[0], cols[1])


class Gather:
    def __init__(self, wires, w):
        self.wires, self.w = wires, w
        self.z, self.y, self.xh = (lax.axis_index(a) for a in FSDP)
        self.one, self.two, self.relay2, self.three, self.relay3, self.third = {}, {}, {}, {}, {}, {}

    def same(self, part, device):
        return self.wires.go(part, part, device)

    def s1(self, k):
        (a0, an), (b0, bn), _ = CHUNKS[k]
        part = self.w.at[self.z, rows_of(96 * self.y + 48 * self.xh, 48), pl.ds(a0, an + bn)]
        self.one[k] = self.same(part, turn("xh", 1, 2))

    def s2(self, k):
        self.one[k].wait_recv()
        ca, cb, _ = map(cols_of, CHUNKS[k])
        pa = self.w.at[self.z, rows_of(96 * self.y, 96), ca]
        pb = self.w.at[self.z, rows_of(96 * self.y, 96), cb]
        self.two[k] = [
            self.same(pa, turn("y", 1, 4)),
            self.same(pa, turn("y", -1, 4)),
            self.same(pb, turn("z", 1, 4)),
            self.same(pb, turn("z", -1, 4)),
        ]

    def s2b(self, k):
        ca, cb, _ = map(cols_of, CHUNKS[k])
        for copy in self.two[k]:
            copy.wait_recv()
        w, z, y = self.w, self.z, self.y
        self.relay2[k] = [
            self.same(w.at[z, rows_of(96 * near("y", -1), 48), ca], turn("y", 1, 4)),
            self.same(w.at[z, rows_of(96 * near("y", 1) + 48, 48), ca], turn("y", -1, 4)),
            self.same(w.at[near("z", -1), rows_of(96 * y, 48), cb], turn("z", 1, 4)),
            self.same(w.at[near("z", 1), rows_of(96 * y + 48, 48), cb], turn("z", -1, 4)),
        ]

    def s3(self, k):
        ca, cb, _ = map(cols_of, CHUNKS[k])
        for copy in self.relay2[k]:
            copy.wait_recv()
        pa = self.w.at[self.z, :, ca]
        pb = self.w.at[:, rows_of(96 * self.y, 96), cb]
        self.three[k] = [
            self.same(pa, turn("z", 1, 4)),
            self.same(pa, turn("z", -1, 4)),
            self.same(pb, turn("y", 1, 4)),
            self.same(pb, turn("y", -1, 4)),
        ]

    def s3b(self, k):
        ca, cb, _ = map(cols_of, CHUNKS[k])
        for copy in self.three[k]:
            copy.wait_recv()
        w = self.w
        self.relay3[k] = [
            self.same(w.at[near("z", -1), pl.ds(0, 192), ca], turn("z", 1, 4)),
            self.same(w.at[near("z", 1), pl.ds(192, 192), ca], turn("z", -1, 4)),
            self.same(w.at[:, rows_of(96 * near("y", -1), 48), cb], turn("y", 1, 4)),
            self.same(w.at[:, rows_of(96 * near("y", 1) + 48, 48), cb], turn("y", -1, 4)),
        ]

    def c1(self, k):
        part = self.w.at[self.z, rows_of(96 * self.y + 48 * self.xh, 48), cols_of(CHUNKS[k][2])]
        self.third[k, 1] = [self.same(part, turn("z", step, 4)) for step in (1, -1, 2)]

    def column(self, y, planes, k):
        return self.w.at[planes, rows_of(96 * y + 48 * self.xh, 48), cols_of(CHUNKS[k][2])]

    def c2(self, k):
        for copy in self.third[k, 1]:
            copy.wait_recv()
        part = self.column(self.y, pl.ds(0, 4), k)
        self.third[k, 2] = [self.same(part, turn("y", step, 4)) for step in (1, -1)]

    def c2b(self, k):
        for copy in self.third[k, 2]:
            copy.wait_recv()
        self.third[k, 3] = [
            self.same(self.column(near("y", -1), pl.ds(0, 2), k), turn("y", 1, 4)),
            self.same(self.column(near("y", 1), pl.ds(2, 2), k), turn("y", -1, 4)),
        ]

    def c3(self, k):
        for copy in self.third[k, 3]:
            copy.wait_recv()
        self.third[k, 4] = [
            self.same(self.column(y, pl.ds(0, 4), k), turn("xh", 1, 2)) for y in range(4)
        ]

    def done(self, k):
        for copy in self.relay3[k] + self.third.get((k, 4), []):
            copy.wait_recv()


def add_into(dst, *srcs):
    planes, rows, columns = dst.shape

    @pl.loop(0, planes * (rows // 48))
    def _(i):
        at = (i // (rows // 48), pl.ds(pl.multiple_of((i % (rows // 48)) * 48, 48), 48), slice(None))
        total = dst[at].astype(F32)
        for src in srcs:
            total = total + src[at].astype(F32)
        dst[at] = total.astype(dst.dtype)


class Scatter:
    def __init__(self, wires, g, half_a, full_a, half_b, full_b, half2, full2, third, last, out):
        self.wires, self.g, self.out, self.third = wires, g, out, third
        self.half_a, self.full_a, self.half_b, self.full_b = half_a, full_a, half_b, full_b
        self.half2, self.full2, self.last = half2, full2, last
        self.z, self.y, self.xh = (lax.axis_index(a) for a in FSDP)
        self.copies = {}

    def block_a(self, step, start, count, cols):
        return self.g.at[pl.ds(near("z", step), 1), pl.ds(start, count), cols]

    def block_b(self, step, start, count, cols):
        return self.g.at[:, rows_of(96 * near("y", step) + start, count), cols]

    def sub_a(self, step, start, count, cols):
        return self.g.at[pl.ds(self.z, 1), rows_of(96 * near("y", step) + start, count), cols]

    def sub_b(self, step, start, count, cols):
        return self.g.at[pl.ds(near("z", step), 1), rows_of(96 * self.y + start, count), cols]

    def r1(self, k):
        ca, cb, _ = map(cols_of, CHUNKS[k])
        go = self.wires.go
        self.copies[k, 1] = [
            go(self.block_a(2, 0, 192, ca), self.half_a[k].at[pl.ds(0, 1)], turn("z", 1, 4)),
            go(self.block_a(2, 192, 192, ca), self.half_a[k].at[pl.ds(1, 1)], turn("z", -1, 4)),
            go(self.block_b(2, 0, 48, cb), self.half_b[k].at[0], turn("y", 1, 4)),
            go(self.block_b(2, 48, 48, cb), self.half_b[k].at[1], turn("y", -1, 4)),
        ]

    def r1b(self, k):
        ca, cb, _ = map(cols_of, CHUNKS[k])
        go, copies = self.wires.go, self.copies[k, 1]
        sent = []
        copies[0].wait_recv()
        add_into(self.block_a(1, 0, 192, ca), self.half_a[k].at[pl.ds(0, 1)])
        sent.append(go(self.block_a(1, 0, 384, ca), self.full_a[k].at[pl.ds(0, 1)], turn("z", 1, 4)))
        copies[1].wait_recv()
        add_into(self.block_a(-1, 192, 192, ca), self.half_a[k].at[pl.ds(1, 1)])
        sent.append(go(self.block_a(-1, 0, 384, ca), self.full_a[k].at[pl.ds(1, 1)], turn("z", -1, 4)))
        copies[2].wait_recv()
        add_into(self.block_b(1, 0, 48, cb), self.half_b[k].at[0])
        sent.append(go(self.block_b(1, 0, 96, cb), self.full_b[k].at[0], turn("y", 1, 4)))
        copies[3].wait_recv()
        add_into(self.block_b(-1, 48, 48, cb), self.half_b[k].at[1])
        sent.append(go(self.block_b(-1, 0, 96, cb), self.full_b[k].at[1], turn("y", -1, 4)))
        self.copies[k, 2] = sent

    def r2(self, k):
        ca, cb, _ = map(cols_of, CHUNKS[k])
        go, copies = self.wires.go, self.copies[k, 2]
        copies[0].wait_recv()
        copies[1].wait_recv()
        add_into(
            self.block_a(0, 0, 384, ca), self.full_a[k].at[pl.ds(0, 1)], self.full_a[k].at[pl.ds(1, 1)]
        )
        sent = [
            go(self.sub_a(2, 0, 48, ca), self.half2[k][0].at[pl.ds(0, 1)], turn("y", 1, 4)),
            go(self.sub_a(2, 48, 48, ca), self.half2[k][0].at[pl.ds(1, 1)], turn("y", -1, 4)),
        ]
        copies[2].wait_recv()
        copies[3].wait_recv()
        add_into(self.block_b(0, 0, 96, cb), self.full_b[k].at[0], self.full_b[k].at[1])
        sent += [
            go(self.sub_b(2, 0, 48, cb), self.half2[k][1].at[pl.ds(0, 1)], turn("z", 1, 4)),
            go(self.sub_b(2, 48, 48, cb), self.half2[k][1].at[pl.ds(1, 1)], turn("z", -1, 4)),
        ]
        self.copies[k, 3] = sent

    def r2b(self, k):
        go, copies = self.wires.go, self.copies[k, 3]
        sent = []
        for colour, (sub, axis) in enumerate(((self.sub_a, "y"), (self.sub_b, "z"))):
            cols = cols_of(CHUNKS[k][colour])
            half, full = self.half2[k][colour], self.full2[k][colour]
            copies[2 * colour].wait_recv()
            add_into(sub(1, 0, 48, cols), half.at[pl.ds(0, 1)])
            sent.append(go(sub(1, 0, 96, cols), full.at[pl.ds(0, 1)], turn(axis, 1, 4)))
            copies[2 * colour + 1].wait_recv()
            add_into(sub(-1, 48, 48, cols), half.at[pl.ds(1, 1)])
            sent.append(go(sub(-1, 0, 96, cols), full.at[pl.ds(1, 1)], turn(axis, -1, 4)))
        self.copies[k, 4] = sent

    def r3(self, k):
        go, copies = self.wires.go, self.copies[k, 4]
        (a0, an), (b0, bn), _ = CHUNKS[k]
        for colour, sub in enumerate((self.sub_a, self.sub_b)):
            cols, full = cols_of(CHUNKS[k][colour]), self.full2[k][colour]
            copies[2 * colour].wait_recv()
            copies[2 * colour + 1].wait_recv()
            add_into(sub(0, 0, 96, cols), full.at[pl.ds(0, 1)], full.at[pl.ds(1, 1)])
        part = self.g.at[self.z, rows_of(96 * self.y + 48 * (1 - self.xh), 48), pl.ds(a0, an + bn)]
        self.copies[k, 5] = [go(part, self.last.at[:, pl.ds(a0, an + bn)], turn("xh", 1, 2))]

    def done(self, k):
        (a0, an), (b0, bn), _ = CHUNKS[k]
        self.copies[k, 5][0].wait_recv()
        cols = pl.ds(a0, an + bn)
        own = self.g[self.z, rows_of(96 * self.y + 48 * self.xh, 48), cols]
        self.store(a0, own.astype(F32) + self.last[:, cols].astype(F32))

    def store(self, start, total):
        if start >= 1152:
            self.out[:, pl.ds(start, total.shape[1])] = total
            return
        for at in range(0, total.shape[1], 128):
            head, which = (start + at) // 384, (start + at) % 384 // 128
            self.out[:, pl.ds(384 * which + 128 * head, 128)] = total[:, at : at + 128]

    def column(self, y, xh, planes, k):
        return self.g.at[planes, rows_of(96 * y + 48 * xh, 48), cols_of(CHUNKS[k][2])]

    def c1(self, k):
        self.copies[k, 6] = [
            self.wires.go(
                self.column(y, 1 - self.xh, pl.ds(0, 4), k), self.third[k][0].at[y], turn("xh", 1, 2)
            )
            for y in range(4)
        ]

    def c2(self, k):
        for y, copy in enumerate(self.copies[k, 6]):
            copy.wait_recv()
            add_into(self.column(y, self.xh, pl.ds(0, 4), k), self.third[k][0].at[y])
        half, far = self.third[k][1], near("y", 2)
        self.copies[k, 7] = [
            self.wires.go(self.column(far, self.xh, pl.ds(0, 2), k), half.at[0], turn("y", 1, 4)),
            self.wires.go(self.column(far, self.xh, pl.ds(2, 2), k), half.at[1], turn("y", -1, 4)),
        ]

    def c2b(self, k):
        half, full = self.third[k][1], self.third[k][2]
        sent = []
        for i, step in enumerate((1, -1)):
            self.copies[k, 7][i].wait_recv()
            add_into(self.column(near("y", step), self.xh, pl.ds(2 * i, 2), k), half.at[i])
            part = self.column(near("y", step), self.xh, pl.ds(0, 4), k)
            sent.append(self.wires.go(part, full.at[i], turn("y", step, 4)))
        self.copies[k, 8] = sent

    def c3(self, k):
        for copy in self.copies[k, 8]:
            copy.wait_recv()
        full, pieces = self.third[k][2], self.third[k][3]
        add_into(self.column(self.y, self.xh, pl.ds(0, 4), k), full.at[0], full.at[1])
        self.copies[k, 9] = [
            self.wires.go(
                self.column(self.y, self.xh, near("z", step), k), pieces.at[i], turn("z", step, 4)
            )
            for i, step in enumerate((1, -1, 2))
        ]

    def c4(self, k):
        start, count = CHUNKS[k][2]
        total = self.g[self.z, rows_of(96 * self.y + 48 * self.xh, 48), pl.ds(start, count)].astype(F32)
        for i, copy in enumerate(self.copies[k, 9]):
            copy.wait_recv()
            total = total + self.third[k][3][i].astype(F32)
        self.store(start, total)


def scatter_buffers():
    shapes = []
    for (_, an), (_, bn), (_, cn) in CHUNKS:
        shapes += [
            pltpu.VMEM((2, 192, an), BF),
            pltpu.VMEM((2, 384, an), BF),
            pltpu.VMEM((2, 4, 48, bn), BF),
            pltpu.VMEM((2, 4, 96, bn), BF),
            pltpu.VMEM((2, 48, an), BF),
            pltpu.VMEM((2, 96, an), BF),
            pltpu.VMEM((2, 48, bn), BF),
            pltpu.VMEM((2, 96, bn), BF),
        ]
        if cn:
            shapes += [
                pltpu.VMEM((4, 4, 48, cn), BF),
                pltpu.VMEM((2, 2, 48, cn), BF),
                pltpu.VMEM((2, 4, 48, cn), BF),
                pltpu.VMEM((3, 48, cn), BF),
            ]
    return shapes


def make_scatter(wires, g, bufs, last, out):
    groups, bufs = [], list(bufs)
    for chunk in CHUNKS:
        count = 12 if chunk[2][1] else 8
        groups.append(bufs[:count])
        bufs = bufs[count:]
    return Scatter(
        wires,
        g,
        [b[0] for b in groups],
        [b[1] for b in groups],
        [b[2] for b in groups],
        [b[3] for b in groups],
        [(b[4], b[6]) for b in groups],
        [(b[5], b[7]) for b in groups],
        [b[8:] for b in groups],
        last,
        out,
    )


def nn(a, b):
    return jnp.dot(a, b, preferred_element_type=F32)


def nt(a, b):
    return lax.dot_general(a, b, (((1,), (1,)), ((), ())), preferred_element_type=F32)


def tn(a, b):
    return lax.dot_general(a, b, (((0,), (0,)), ((), ())), preferred_element_type=F32)


class Spread:
    def __init__(self, wires, buf):
        self.wires, self.buf = wires, buf
        self.xl, self.c = (lax.axis_index(a) for a in SP)
        self.far, self.near, self.relays = {}, {}, {}

    def block(self, xl, c, start=0, count=128):
        return self.buf.at[rows_of(256 * xl + 128 * c + start, count), :]

    def start(self, i):
        part = self.block(self.xl, self.c, 64 * i, 64)
        self.far[i] = self.wires.go(part, part, turn("xl", 1, 2))
        self.near[i] = self.wires.go(part, part, turn("c", 1, 2))

    def relay(self, i):
        self.far[i].wait_recv()
        part = self.block(1 - self.xl, self.c, 64 * i, 64)
        self.relays[i] = self.wires.go(part, part, turn("c", 1, 2))

    def own_half(self):
        for copy in self.near.values():
            copy.wait_recv()

    def done(self):
        for copy in self.relays.values():
            copy.wait_recv()

    def release(self):
        for group in (self.far, self.near, self.relays):
            for copy in group.values():
                self.wires.sent(copy)


class Collect:
    def __init__(self, wires, part, pair, cross):
        self.wires, self.part, self.pair, self.cross = wires, part, pair, cross
        self.xl, self.c = (lax.axis_index(a) for a in SP)

    def block(self, xl, c):
        return self.part.at[rows_of(256 * xl + 128 * c, 128), :]

    def other(self):
        self.first = self.wires.go(self.block(1 - self.xl, 1 - self.c), self.pair.at[0], turn("c", 1, 2))

    def send(self):
        self.first.wait_recv()
        self.third = []
        for i in range(2):
            rows = pl.ds(64 * i, 64)
            mine = self.block(1 - self.xl, self.c).at[rows, :]
            add2(mine, self.pair.at[0, rows, :])
            self.third.append(self.wires.go(mine, self.cross.at[rows, :], turn("xl", 1, 2)))

    def own(self):
        self.second = self.wires.go(self.block(self.xl, 1 - self.c), self.pair.at[1], turn("c", 1, 2))

    def wait(self, i):
        if i == 0:
            self.second.wait_recv()
        self.third[i].wait_recv()

    def release(self):
        for copy in (self.first, self.second, *self.third):
            self.wires.sent(copy)

    def rows(self, start, count):
        at = rows_of(256 * self.xl + 128 * self.c + start, count)
        total = self.part[at, :].astype(F32) + self.pair[1, pl.ds(start, count), :].astype(F32)
        return total + self.cross[pl.ds(start, count), :].astype(F32)


def add2(dst, src):
    rows = dst.shape[0]

    @pl.loop(0, rows // 16)
    def _(i):
        at = (pl.ds(pl.multiple_of(i * 16, 16), 16), slice(None))
        dst[at] = (dst[at].astype(F32) + src[at].astype(F32)).astype(dst.dtype)


def normalize(stream):
    mean_part = jnp.mean(stream, axis=-1, keepdims=True)
    centred = stream - mean_part
    rstd = lax.rsqrt(jnp.mean(centred * centred, axis=-1, keepdims=True) + ln_eps)
    return (centred * rstd, rstd)


def norm_back(normed, rstd, incoming):
    first = jnp.mean(incoming, axis=-1, keepdims=True)
    second = jnp.mean(incoming * normed, axis=-1, keepdims=True)
    return rstd * (incoming - first - normed * second)


BLOCK = 16
ROOT = math.sqrt(2.0 / math.pi)


def by_rows(fn, start=0, count=128):
    @pl.loop(start // BLOCK, (start + count) // BLOCK)
    def _(i):
        fn(pl.multiple_of(i * BLOCK, BLOCK))


def block_kernel(
    x_in, m_in, og_in, wq_ref, wo_ref, wi_ref, wb_ref,
    final_out, ig_out, sums_out,
    x_ref, m_ref, og_ref, final_ref, ig_ref, sums_ref,
    w, g, last, a1, dm, a2, da, qkv, o, do, gp, act, part, probs, dv, pair0, cross0, pair1, cross1,
    mid, dmid, send, recv, local_sem, *bufs,
):
    z, y, xh, xl, c = (lax.axis_index(a) for a in FSDP + SP)
    shard_rows = rows_of(96 * y + 48 * xh, 48)
    pieces = [
        (wq_ref.at[which, :, pl.ds(128 * h, 128)], 384 * h + 128 * which, 128)
        for h in range(3)
        for which in range(3)
    ]
    pieces += [(wo_ref, 1152, 384), (wi_ref, 1536, 1536), (wb_ref, 3072, 1536)]
    loads = [
        pltpu.make_async_copy(part, w.at[z, shard_rows, pl.ds(at, count)], local_sem.at[i])
        for i, (part, at, count) in enumerate(pieces)
    ]
    inputs = [
        pltpu.make_async_copy(a, b, local_sem.at[12 + i])
        for i, (a, b) in enumerate(((x_in, x_ref), (m_in, m_ref), (og_in, og_ref)))
    ]
    outputs = {
        name: pltpu.make_async_copy(a, b, local_sem.at[15 + i])
        for i, (name, a, b) in enumerate(
            (("final", final_ref, final_out), ("ig", ig_ref, ig_out), ("sums", sums_ref, sums_out))
        )
    }
    greet()
    for load in loads[:3] + inputs[:2] + loads[3:] + inputs[2:]:
        load.start()
    wires = Wires(send, recv)
    ag = Gather(wires, w)
    rs = make_scatter(wires, g, bufs, last, sums_ref)
    own_row = 256 * xl + 128 * c
    own_start, other_start = 256 * xl, 256 * (1 - xl)
    scale = 1.0 / math.sqrt(32 * 512)
    factor = temper / math.sqrt(HEAD_DIM)
    steps = {}

    def step(fn):
        steps[fn.__name__] = fn
        return fn

    def mod(i):
        return m_ref[pl.ds(i, 1), :]

    def own(start):
        return (rows_of(own_row + start, BLOCK), slice(None))

    def weights(start, count):
        return w[:, :, pl.ds(start, count)].reshape(1536, count)

    for k in range(len(CHUNKS)):
        third = ("c1", "c2", "c2b", "c3") if CHUNKS[k][2][1] else ()
        for name in ("s1", "s2", "s2b", "s3", "s3b", "done", *third):
            steps[f"ag_{name}_{k}"] = functools.partial(getattr(ag, name), k)
        for name in ("r1", "r1b", "r2", "r2b", "r3", "done", *third, *(("c4",) if third else ())):
            steps[f"rs_{name}_{k}"] = functools.partial(getattr(rs, name), k)
    for key, buf in (("a1", a1), ("dm", dm), ("a2", a2), ("da", da)):
        spread = Spread(wires, buf)
        for i in range(2):
            steps[f"{key}_start_{i}"] = functools.partial(spread.start, i)
            steps[f"{key}_relay_{i}"] = functools.partial(spread.relay, i)
        steps[f"{key}_own_half"] = spread.own_half
        steps[f"{key}_done"] = spread.done
        steps[f"{key}_release"] = spread.release
    reds = {
        "att": Collect(wires, part, pair0, cross0),
        "da2": Collect(wires, part, pair0, cross0),
        "da1": Collect(wires, part, pair0, cross0),
        "ffn": Collect(wires, dm, pair1, cross1),
    }
    for key, red in reds.items():
        for name in ("other", "own", "send", "release"):
            steps[f"{key}_{name}"] = getattr(red, name)
        for i in range(2):
            steps[f"{key}_wait_{i}"] = functools.partial(red.wait, i)

    @step
    def load_first():
        for load in loads[:3]:
            load.wait()

    steps["met"] = met

    @step
    def load_inputs():
        inputs[0].wait()
        inputs[1].wait()

    @step
    def load_rest():
        for load in loads[3:]:
            load.wait()
        inputs[2].wait()

    def first_norm(r):
        n1, _ = normalize(x_ref[pl.ds(r, BLOCK), :].astype(F32))
        a1[own(r)] = (n1 * (1.0 + mod(1)) + mod(0)).astype(BF)

    def second_norm(r):
        rows = pl.ds(r, BLOCK)
        value = x_ref[rows, :].astype(F32) + mod(2) * reds["att"].rows(r, BLOCK)
        mid[rows, :] = value
        n2, _ = normalize(value)
        a2[own(r)] = (n2 * (1.0 + mod(4)) + mod(3)).astype(BF)

    def mid_grad(r):
        rows = pl.ds(r, BLOCK)
        n2, r2 = normalize(mid[rows, :])
        inner = norm_back(n2, r2, reds["da2"].rows(r, BLOCK) * (1.0 + mod(4)))
        value = og_ref[rows, :].astype(F32) + inner
        dmid[rows, :] = value
        da[own(r)] = (mod(2) * value).astype(BF)

    for i in range(2):
        for fn in (first_norm, second_norm, mid_grad):
            steps[f"{fn.__name__}_{i}"] = functools.partial(by_rows, fn, 64 * i, 64)

    @step
    def gate_grad():
        def rows(r):
            dm[own(r)] = (mod(5) * og_ref[pl.ds(r, BLOCK), :].astype(F32)).astype(BF)

        by_rows(rows)

    def lanes(h, which):
        return pl.ds(384 * h + 128 * which, 128)

    def project(start, count):
        qkv[:, pl.ds(start, count)] = nn(a1[...], weights(start, count)).astype(BF)

    @step
    def project_0():
        project(0, 256)
        project(256, 128)

    @step
    def project_1():
        @pl.loop(0, 3)
        def _(j):
            project(pl.multiple_of(384 + j * 256, 128), 256)

    def attend(heads, start, blocks):
        @pl.loop(0, blocks)
        def _(i):
            rows = rows_of(start + i * 128, 128)
            for h in heads:
                s = nt(qkv[rows, lanes(h, 0)], qkv[:, lanes(h, 1)]) * factor
                e = jnp.exp(s - jnp.max(s, axis=-1, keepdims=True))
                p = (e * (1.0 / jnp.sum(e, axis=-1, keepdims=True))).astype(BF)
                probs[h, rows, :] = p
                o[rows, pl.ds(128 * h, 128)] = nn(p, qkv[:, lanes(h, 2)]).astype(BF)

    steps["attend_0"] = functools.partial(attend, (0,), 0, 4)
    steps["attend_other"] = functools.partial(attend, (1, 2), other_start, 2)
    steps["attend_own"] = functools.partial(attend, (1, 2), own_start, 2)

    def back_half(dst, lhs, start, at, count):
        rows = rows_of(start, 256)

        @pl.loop(0, 2)
        def _(j):
            rhs = w[pl.ds(2 * j, 2), :, pl.ds(at, count)].reshape(768, count)
            dst[rows, pl.ds(pl.multiple_of(768 * j, 128), 768)] = nt(lhs[rows, :], rhs).astype(BF)

    for key, dst, lhs, at, count in (
        ("att", part, o, 1152, 384),
        ("da2", part, gp, 1536, 1536),
        ("da1", part, qkv, 0, 1152),
        ("ffn", dm, act, 3072, 1536),
    ):
        steps[f"{key}_mm_other"] = functools.partial(back_half, dst, lhs, other_start, at, count)
        steps[f"{key}_mm_own"] = functools.partial(back_half, dst, lhs, own_start, at, count)

    def hidden(start, half):
        rows = rows_of(start, 256)

        @pl.loop(3 * half, 3 * half + 3)
        def _(j):
            at = pl.multiple_of(j * 256, 256)
            u = nn(a2[rows, :], weights(pl.multiple_of(1536 + at, 256), 256))
            sq = u * u
            t = jnp.tanh(ROOT * u * (1.0 + 0.044715 * sq))
            half = 0.5 * (1.0 + t)
            act[rows, pl.ds(at, 256)] = (u * half).astype(BF)
            slope = half + (0.5 * ROOT) * u * (1.0 - t * t) * (1.0 + (3 * 0.044715) * sq)
            gp[rows, pl.ds(at, 256)] = slope.astype(BF)

    def hidden_grad(half):
        @pl.loop(3 * half, 3 * half + 3)
        def _(j):
            at = pl.multiple_of(j * 256, 256)
            cols = pl.ds(at, 256)
            dg = nn(dm[...], weights(pl.multiple_of(3072 + at, 256), 256))
            gp[:, cols] = (gp[:, cols].astype(F32) * dg).astype(BF)

    def grad(left, right, right_at, at, count):
        @pl.loop(0, 4)
        def _(j):
            lhs = left[:, pl.ds(pl.multiple_of(384 * j, 128), 384)]
            value = tn(lhs, right[:, pl.ds(right_at, count)]) * scale
            g[j, :, pl.ds(at, count)] = value.astype(BF)

    for i in range(2):
        steps[f"hidden_own_{i}"] = functools.partial(hidden, own_start, i)
        steps[f"hidden_other_{i}"] = functools.partial(hidden, other_start, i)
        steps[f"hidden_grad_{i}"] = functools.partial(hidden_grad, i)
        steps[f"grad_in_{i}"] = functools.partial(grad, a2, gp, 768 * i, 1536 + 768 * i, 768)
        steps[f"grad_back_{i}"] = functools.partial(grad, dm, act, 768 * i, 3072 + 768 * i, 768)
    steps["grad_out"] = functools.partial(grad, da, o, 0, 1152, 384)
    steps["grad_q_0"] = functools.partial(grad, a1, qkv, 0, 0, 384)
    steps["grad_q_1"] = functools.partial(grad, a1, qkv, 384, 384, 768)

    def head_grads(start):
        rows = rows_of(start, 256)
        do[rows, :] = nn(da[rows, :], weights(1152, 384)).astype(BF)

    steps["heads_own"] = functools.partial(head_grads, own_start)
    steps["heads_other"] = functools.partial(head_grads, other_start)

    def attend_back(heads):
        for n, h in enumerate(heads):
            dv[n] = tn(probs[h], do[:, pl.ds(128 * h, 128)]).astype(BF)

        @pl.loop(0, 4)
        def _(i):
            rows = pl.ds(pl.multiple_of(i * 128, 128), 128)
            for h in heads:
                dp = nt(do[rows, pl.ds(128 * h, 128)], qkv[:, lanes(h, 2)])
                p = probs[h, rows, :].astype(F32)
                ds = factor * p * (dp - jnp.sum(p * dp, axis=-1, keepdims=True))
                probs[h, rows, :] = ds.astype(BF)

        for n, h in enumerate(heads):
            dk = tn(probs[h], qkv[:, lanes(h, 0)]).astype(BF)
            qkv[:, lanes(h, 0)] = nn(probs[h], qkv[:, lanes(h, 1)]).astype(BF)
            qkv[:, lanes(h, 1)] = dk
            qkv[:, lanes(h, 2)] = dv[n]

    steps["attend_back_0"] = functools.partial(attend_back, (0,))
    steps["attend_back_1"] = functools.partial(attend_back, (1, 2))

    @step
    def last_out():
        def each(r):
            rows = pl.ds(r, BLOCK)
            final_ref[rows, :] = (mid[rows, :] + mod(5) * reds["ffn"].rows(r, BLOCK)).astype(BF)

        by_rows(each)
        outputs["final"].start()

    @step
    def first_grad():
        def each(r):
            rows = pl.ds(r, BLOCK)
            n1, r1 = normalize(x_ref[rows, :].astype(F32))
            inner = norm_back(n1, r1, reds["da1"].rows(r, BLOCK) * (1.0 + mod(1)))
            ig_ref[rows, :] = dmid[rows, :] + inner

        by_rows(each)
        outputs["ig"].start()

    @step
    def finish():
        outputs["sums"].start()
        wires.drain()
        for copy in outputs.values():
            copy.wait()

    for name in ORDER:
        with jax.named_scope(name):
            steps[name]()


def finish_kernel(
    final_in, ig_in, sums_in, final_out, ig_out, gq_out, go_out, gi_out, gb_out, final, ig, sums, sem
):
    cuts = [(384 * which, 384, gq_out.at[which]) for which in range(3)]
    cuts += [(1152, 384, go_out), (1536, 1536, gi_out), (3072, 1536, gb_out)]
    pairs = [(sums_in.at[:, pl.ds(at, n)], sums.at[:, pl.ds(at, n)], out) for at, n, out in cuts]
    pairs += [(ig_in, ig, ig_out), (final_in, final, final_out)]
    loads, stores = [], []
    for i, (source, held, out) in enumerate(pairs):
        loads.append(pltpu.make_async_copy(source, held, sem.at[0, i]))
        stores.append(pltpu.make_async_copy(held, out, sem.at[1, i]))
    for load in loads:
        load.start()
    for load, store in zip(loads, stores):
        load.wait()
        store.start()
    for store in stores:
        store.wait()


def body(tokens, modulation, w_qkv, w_out, w_in, w_back, out_grad):
    own = w_qkv.shape[3]
    far = pl.BlockSpec(memory_space=pl.ANY)
    copies = 54 * len(CHUNKS) + 40
    rows = lambda n, dtype=BF: pltpu.VMEM((512, n), dtype)
    final, grad_in_rows, sums = pl.pallas_call(
        block_kernel,
        out_shape=(
            jax.ShapeDtypeStruct((128, 1536), BF),
            jax.ShapeDtypeStruct((128, 1536), F32),
            jax.ShapeDtypeStruct((48, WIDTH), F32),
        ),
        in_specs=[far] * 7,
        out_specs=(far, far, far),
        scratch_shapes=[
            pltpu.VMEM((128, 1536), BF),
            pltpu.VMEM((6, 1536), F32),
            pltpu.VMEM((128, 1536), BF),
            pltpu.VMEM((128, 1536), BF),
            pltpu.VMEM((128, 1536), F32),
            pltpu.VMEM((48, WIDTH), F32),
            pltpu.VMEM((4, 384, WIDTH), BF),
            pltpu.VMEM((4, 384, WIDTH), BF),
            pltpu.VMEM((48, WIDTH), BF),
            rows(1536), rows(1536), rows(1536), rows(1536),
            rows(1152), rows(384), rows(384),
            rows(1536), rows(1536), rows(1536),
            pltpu.VMEM((3, 512, 512), BF),
            pltpu.VMEM((2, 512, 128), BF),
            pltpu.VMEM((2, 128, 1536), BF),
            pltpu.VMEM((128, 1536), BF),
            pltpu.VMEM((2, 128, 1536), BF),
            pltpu.VMEM((128, 1536), BF),
            pltpu.VMEM((128, 1536), F32),
            pltpu.VMEM((128, 1536), F32),
            pltpu.SemaphoreType.DMA((copies,)),
            pltpu.SemaphoreType.DMA((copies,)),
            pltpu.SemaphoreType.DMA((18,)),
            *scatter_buffers(),
        ],
        compiler_params=pltpu.CompilerParams(
            collective_id=0, has_side_effects=True, vmem_limit_bytes=VMEM_LIMIT
        ),
        name="block",
    )(
        tokens[0],
        modulation[0, 0],
        out_grad[0],
        w_qkv[0].transpose(1, 0, 2),
        w_out[0].T,
        w_in[0],
        w_back[0].T,
    )
    outs = pl.pallas_call(
        finish_kernel,
        out_shape=(
            jax.ShapeDtypeStruct((128, 1536), BF),
            jax.ShapeDtypeStruct((128, 1536), F32),
            jax.ShapeDtypeStruct((3, 48, own), F32),
            jax.ShapeDtypeStruct((48, own), F32),
            jax.ShapeDtypeStruct((48, 4 * own), F32),
            jax.ShapeDtypeStruct((48, 4 * own), F32),
        ),
        in_specs=[far] * 3,
        out_specs=(far,) * 6,
        scratch_shapes=[
            pltpu.VMEM((128, 1536), BF),
            pltpu.VMEM((128, 1536), F32),
            pltpu.VMEM((48, WIDTH), F32),
            pltpu.SemaphoreType.DMA((2, 8)),
        ],
        name="finish",
    )(final, grad_in_rows, sums)
    final, grad_in_rows, gq, go, gi, gb = outs
    return (final[None], grad_in_rows[None], gq.transpose(1, 0, 2)[None], go.T[None], gi[None], gb.T[None])


def solution(mesh):
    torus = Mesh(mesh.devices.reshape(4, 4, 2, 2, 2), FSDP + SP)
    return jax.shard_map(
        body,
        mesh=torus,
        in_specs=(
            P(FSDP, SP, None),
            P(FSDP, None, None, None),
            P(None, FSDP, None, SP),
            P(None, SP, FSDP),
            P(None, FSDP, SP),
            P(None, SP, FSDP),
            P(FSDP, SP, None),
        ),
        out_specs=(
            P(FSDP, SP, None),
            P(FSDP, SP, None),
            P(None, FSDP, None, SP),
            P(None, SP, FSDP),
            P(None, FSDP, SP),
            P(None, SP, FSDP),
        ),
        check_vma=False,
    )
```

```python
import functools
import math

import jax
import jax.numpy as jnp
from jax import lax
from jax.experimental import pallas as pl
from jax.experimental.pallas import tpu as pltpu
from jax.sharding import Mesh
from jax.sharding import PartitionSpec as P

HEAD_DIM = 128
MESH = pl.DeviceIdType.MESH
FSDP = ("z", "y", "xh")
SP = ("xl", "c")
BF = jnp.bfloat16
F32 = jnp.float32

ln_eps = 1e-06
temper = 2.5
VMEM_LIMIT = 67_000_000

TILES = ((2, 1, 0), (3, 2, 1), (1, 1, 1), (2, 3, 1), (3, 2, 1), (2, 3, 1), (3, 2, 1))


def split_chunks():
    chunks, at = [], 0
    for tiles in TILES:
        parts = []
        for count in tiles:
            parts.append((at, 128 * count))
            at += 128 * count
        chunks.append(tuple(parts))
    return tuple(chunks)


CHUNKS = split_chunks()
WIDTH = 4608
ORDER = (
    "load_first",
    "met",
    "load_rest",
    "ag_s1_2",
    "ag_c1_2",
    "ag_s1_0",
    "load_inputs",
    "ag_s1_1",
    "ag_c1_1",
    "ag_s1_4",
    "ag_s1_3",
    "ag_c1_3",
    "ag_s1_5",
    "first_norm_1",
    "ag_c1_6",
    "ag_s2_2",
    "ag_c2_2",
    "ag_s2_0",
    "gate_grad",
    "first_norm_0",
    "a1_start_0",
    "dm_start_1",
    "ag_s1_6",
    "ag_s2_1",
    "ag_c2_3",
    "ag_c1_5",
    "ag_c1_4",
    "ag_s2_4",
    "ag_s2b_0",
    "ag_s2b_2",
    "ag_c2_1",
    "ag_s2_3",
    "a1_start_1",
    "ag_c2_4",
    "ag_c2_6",
    "ag_s2b_1",
    "ag_s3_0",
    "ag_c2b_1",
    "ag_s3_2",
    "a1_relay_0",
    "ag_c2b_3",
    "ag_c2b_2",
    "ag_s2b_4",
    "ag_s3b_0",
    "ag_c2_5",
    "dm_start_0",
    "ag_s3_1",
    "ag_c2b_4",
    "ag_c3_1",
    "ag_c2b_6",
    "dm_relay_0",
    "a1_relay_1",
    "ag_s2_6",
    "dm_relay_1",
    "a1_done",
    "ag_s2b_3",
    "ag_done_0",
    "ag_c3_2",
    "ag_s3b_1",
    "dm_own_half",
    "ag_s2_5",
    "dm_release",
    "ag_c3_3",
    "a1_own_half",
    "project_0",
    "ag_c3_4",
    "attend_0",
    "ag_s3b_2",
    "ag_done_1",
    "ag_s3_4",
    "project_1",
    "attend_other",
    "ag_c2b_5",
    "ag_done_2",
    "att_mm_other",
    "att_other",
    "ag_s3_3",
    "dm_done",
    "att_send",
    "attend_own",
    "att_mm_own",
    "att_own",
    "att_release",
    "ag_s2b_6",
    "ag_s2b_5",
    "att_wait_0",
    "ag_s3b_4",
    "second_norm_0",
    "ag_s3b_3",
    "a2_start_0",
    "ag_done_4",
    "ag_s3_5",
    "att_wait_1",
    "ag_s3_6",
    "second_norm_1",
    "a2_start_1",
    "ag_done_3",
    "a2_relay_0",
    "a2_own_half",
    "hidden_own_1",
    "a2_relay_1",
    "ag_c3_5",
    "ag_c3_6",
    "hidden_own_0",
    "a2_done",
    "hidden_other_0",
    "ag_s3b_5",
    "hidden_other_1",
    "grad_back_1",
    "ag_s3b_6",
    "rs_r1_6",
    "grad_back_0",
    "rs_r1_5",
    "ag_done_5",
    "rs_c1_5",
    "hidden_grad_0",
    "grad_in_0",
    "rs_r1_3",
    "ag_done_6",
    "rs_c1_3",
    "hidden_grad_1",
    "da2_mm_other",
    "da2_other",
    "rs_r1b_5",
    "da2_send",
    "ffn_mm_other",
    "da2_mm_own",
    "rs_r1b_3",
    "grad_in_1",
    "rs_c2_3",
    "da2_own",
    "rs_r1_4",
    "da2_wait_0",
    "ffn_other",
    "mid_grad_0",
    "da_start_0",
    "rs_r2_5",
    "rs_r1b_6",
    "da2_wait_1",
    "mid_grad_1",
    "ffn_mm_own",
    "da_start_1",
    "rs_r1b_4",
    "rs_c1_6",
    "da_relay_0",
    "da_own_half",
    "rs_r2_3",
    "rs_c2_5",
    "da_relay_1",
    "ffn_own",
    "heads_own",
    "rs_c2b_3",
    "da_done",
    "rs_c1_4",
    "heads_other",
    "rs_r2b_5",
    "rs_r2_6",
    "ffn_send",
    "attend_back_1",
    "grad_q_1",
    "rs_r1_1",
    "rs_c2b_5",
    "attend_back_0",
    "rs_r2_4",
    "rs_c1_1",
    "grad_q_0",
    "rs_c2_4",
    "rs_r1_0",
    "rs_r2b_3",
    "grad_out",
    "rs_c2b_4",
    "rs_r3_5",
    "rs_c1_2",
    "rs_r1_2",
    "rs_c2_6",
    "da2_release",
    "rs_r2b_4",
    "da1_mm_own",
    "ffn_wait_0",
    "rs_r2b_6",
    "rs_r3_3",
    "rs_r1b_1",
    "da1_mm_other",
    "rs_c3_5",
    "da1_other",
    "da1_own",
    "rs_c2b_6",
    "rs_r1b_0",
    "ffn_wait_1",
    "rs_r3_4",
    "da1_send",
    "rs_c2_1",
    "rs_r2_1",
    "rs_done_5",
    "rs_c2_2",
    "rs_r1b_2",
    "rs_c4_5",
    "rs_r2_0",
    "rs_c3_4",
    "rs_r3_6",
    "rs_done_3",
    "rs_r2b_1",
    "last_out",
    "rs_c3_6",
    "rs_r2_2",
    "rs_c3_3",
    "rs_r2b_0",
    "rs_done_4",
    "rs_c2b_1",
    "rs_c2b_2",
    "rs_r2b_2",
    "da1_wait_0",
    "rs_r3_0",
    "rs_r3_1",
    "rs_c4_4",
    "rs_c3_1",
    "rs_c4_6",
    "rs_c3_2",
    "rs_r3_2",
    "da1_wait_1",
    "rs_c4_3",
    "first_grad",
    "rs_done_6",
    "rs_done_0",
    "rs_done_1",
    "rs_c4_2",
    "rs_c4_1",
    "rs_done_2",
    "finish",
)


def turn(axis, step, size):
    return {axis: lax.rem(lax.axis_index(axis) + step + size, size)}


def near(axis, step):
    return lax.rem(lax.axis_index(axis) + step + 4, 4)


class Wires:
    def __init__(self, send, recv):
        self.send, self.recv, self.used, self.open = send, recv, 0, []

    def go(self, src, dst, device):
        at = self.used
        self.used += 1
        copy = pltpu.make_async_remote_copy(
            src_ref=src,
            dst_ref=dst,
            send_sem=self.send.at[at],
            recv_sem=self.recv.at[at],
            device_id=device,
            device_id_type=MESH,
        )
        copy.start()
        self.open.append(copy)
        return copy

    def sent(self, copy):
        copy.wait_send()
        self.open = [other for other in self.open if other is not copy]

    def drain(self):
        for copy in self.open:
            copy.wait_send()
        self.open = []


def partners():
    return [turn("z", 1, 4), turn("z", -1, 4), turn("z", 2, 4), turn("y", 1, 4), turn("y", -1, 4)] + [
        turn(axis, 1, 2) for axis in ("xh", "xl", "c")
    ]


def greet():
    for device in partners():
        pl.semaphore_signal(
            pltpu.get_barrier_semaphore(), inc=1, device_id=device, device_id_type=MESH
        )


def met():
    pl.semaphore_wait(pltpu.get_barrier_semaphore(), len(partners()))


def rows_of(start, count):
    return pl.ds(pl.multiple_of(start, 16), count)


def cols_of(cols):
    return pl.ds(cols[0], cols[1])


class Gather:
    def __init__(self, wires, w):
        self.wires, self.w = wires, w
        self.z, self.y, self.xh = (lax.axis_index(a) for a in FSDP)
        self.one, self.two, self.relay2, self.three, self.relay3, self.third = {}, {}, {}, {}, {}, {}

    def same(self, part, device):
        return self.wires.go(part, part, device)

    def s1(self, k):
        (a0, an), (b0, bn), _ = CHUNKS[k]
        part = self.w.at[self.z, rows_of(96 * self.y + 48 * self.xh, 48), pl.ds(a0, an + bn)]
        self.one[k] = self.same(part, turn("xh", 1, 2))

    def s2(self, k):
        self.one[k].wait_recv()
        ca, cb, _ = map(cols_of, CHUNKS[k])
        pa = self.w.at[self.z, rows_of(96 * self.y, 96), ca]
        pb = self.w.at[self.z, rows_of(96 * self.y, 96), cb]
        self.two[k] = [
            self.same(pa, turn("y", 1, 4)),
            self.same(pa, turn("y", -1, 4)),
            self.same(pb, turn("z", 1, 4)),
            self.same(pb, turn("z", -1, 4)),
        ]

    def s2b(self, k):
        ca, cb, _ = map(cols_of, CHUNKS[k])
        for copy in self.two[k]:
            copy.wait_recv()
        w, z, y = self.w, self.z, self.y
        self.relay2[k] = [
            self.same(w.at[z, rows_of(96 * near("y", -1), 48), ca], turn("y", 1, 4)),
            self.same(w.at[z, rows_of(96 * near("y", 1) + 48, 48), ca], turn("y", -1, 4)),
            self.same(w.at[near("z", -1), rows_of(96 * y, 48), cb], turn("z", 1, 4)),
            self.same(w.at[near("z", 1), rows_of(96 * y + 48, 48), cb], turn("z", -1, 4)),
        ]

    def s3(self, k):
        ca, cb, _ = map(cols_of, CHUNKS[k])
        for copy in self.relay2[k]:
            copy.wait_recv()
        pa = self.w.at[self.z, :, ca]
        pb = self.w.at[:, rows_of(96 * self.y, 96), cb]
        self.three[k] = [
            self.same(pa, turn("z", 1, 4)),
            self.same(pa, turn("z", -1, 4)),
            self.same(pb, turn("y", 1, 4)),
            self.same(pb, turn("y", -1, 4)),
        ]

    def s3b(self, k):
        ca, cb, _ = map(cols_of, CHUNKS[k])
        for copy in self.three[k]:
            copy.wait_recv()
        w = self.w
        self.relay3[k] = [
            self.same(w.at[near("z", -1), pl.ds(0, 192), ca], turn("z", 1, 4)),
            self.same(w.at[near("z", 1), pl.ds(192, 192), ca], turn("z", -1, 4)),
            self.same(w.at[:, rows_of(96 * near("y", -1), 48), cb], turn("y", 1, 4)),
            self.same(w.at[:, rows_of(96 * near("y", 1) + 48, 48), cb], turn("y", -1, 4)),
        ]

    def c1(self, k):
        part = self.w.at[self.z, rows_of(96 * self.y + 48 * self.xh, 48), cols_of(CHUNKS[k][2])]
        self.third[k, 1] = [self.same(part, turn("z", step, 4)) for step in (1, -1, 2)]

    def column(self, y, planes, k):
        return self.w.at[planes, rows_of(96 * y + 48 * self.xh, 48), cols_of(CHUNKS[k][2])]

    def c2(self, k):
        for copy in self.third[k, 1]:
            copy.wait_recv()
        part = self.column(self.y, pl.ds(0, 4), k)
        self.third[k, 2] = [self.same(part, turn("y", step, 4)) for step in (1, -1)]

    def c2b(self, k):
        for copy in self.third[k, 2]:
            copy.wait_recv()
        self.third[k, 3] = [
            self.same(self.column(near("y", -1), pl.ds(0, 2), k), turn("y", 1, 4)),
            self.same(self.column(near("y", 1), pl.ds(2, 2), k), turn("y", -1, 4)),
        ]

    def c3(self, k):
        for copy in self.third[k, 3]:
            copy.wait_recv()
        self.third[k, 4] = [
            self.same(self.column(y, pl.ds(0, 4), k), turn("xh", 1, 2)) for y in range(4)
        ]

    def done(self, k):
        for copy in self.relay3[k] + self.third.get((k, 4), []):
            copy.wait_recv()


def add_into(dst, *srcs):
    planes, rows, columns = dst.shape

    @pl.loop(0, planes * (rows // 48))
    def _(i):
        at = (i // (rows // 48), pl.ds(pl.multiple_of((i % (rows // 48)) * 48, 48), 48), slice(None))
        total = dst[at].astype(F32)
        for src in srcs:
            total = total + src[at].astype(F32)
        dst[at] = total.astype(dst.dtype)


class Scatter:
    def __init__(self, wires, g, half_a, full_a, half_b, full_b, half2, full2, third, last, out):
        self.wires, self.g, self.out, self.third = wires, g, out, third
        self.half_a, self.full_a, self.half_b, self.full_b = half_a, full_a, half_b, full_b
        self.half2, self.full2, self.last = half2, full2, last
        self.z, self.y, self.xh = (lax.axis_index(a) for a in FSDP)
        self.copies = {}

    def block_a(self, step, start, count, cols):
        return self.g.at[pl.ds(near("z", step), 1), pl.ds(start, count), cols]

    def block_b(self, step, start, count, cols):
        return self.g.at[:, rows_of(96 * near("y", step) + start, count), cols]

    def sub_a(self, step, start, count, cols):
        return self.g.at[pl.ds(self.z, 1), rows_of(96 * near("y", step) + start, count), cols]

    def sub_b(self, step, start, count, cols):
        return self.g.at[pl.ds(near("z", step), 1), rows_of(96 * self.y + start, count), cols]

    def r1(self, k):
        ca, cb, _ = map(cols_of, CHUNKS[k])
        go = self.wires.go
        self.copies[k, 1] = [
            go(self.block_a(2, 0, 192, ca), self.half_a[k].at[pl.ds(0, 1)], turn("z", 1, 4)),
            go(self.block_a(2, 192, 192, ca), self.half_a[k].at[pl.ds(1, 1)], turn("z", -1, 4)),
            go(self.block_b(2, 0, 48, cb), self.half_b[k].at[0], turn("y", 1, 4)),
            go(self.block_b(2, 48, 48, cb), self.half_b[k].at[1], turn("y", -1, 4)),
        ]

    def r1b(self, k):
        ca, cb, _ = map(cols_of, CHUNKS[k])
        go, copies = self.wires.go, self.copies[k, 1]
        sent = []
        copies[0].wait_recv()
        add_into(self.block_a(1, 0, 192, ca), self.half_a[k].at[pl.ds(0, 1)])
        sent.append(go(self.block_a(1, 0, 384, ca), self.full_a[k].at[pl.ds(0, 1)], turn("z", 1, 4)))
        copies[1].wait_recv()
        add_into(self.block_a(-1, 192, 192, ca), self.half_a[k].at[pl.ds(1, 1)])
        sent.append(go(self.block_a(-1, 0, 384, ca), self.full_a[k].at[pl.ds(1, 1)], turn("z", -1, 4)))
        copies[2].wait_recv()
        add_into(self.block_b(1, 0, 48, cb), self.half_b[k].at[0])
        sent.append(go(self.block_b(1, 0, 96, cb), self.full_b[k].at[0], turn("y", 1, 4)))
        copies[3].wait_recv()
        add_into(self.block_b(-1, 48, 48, cb), self.half_b[k].at[1])
        sent.append(go(self.block_b(-1, 0, 96, cb), self.full_b[k].at[1], turn("y", -1, 4)))
        self.copies[k, 2] = sent

    def r2(self, k):
        ca, cb, _ = map(cols_of, CHUNKS[k])
        go, copies = self.wires.go, self.copies[k, 2]
        copies[0].wait_recv()
        copies[1].wait_recv()
        add_into(
            self.block_a(0, 0, 384, ca), self.full_a[k].at[pl.ds(0, 1)], self.full_a[k].at[pl.ds(1, 1)]
        )
        sent = [
            go(self.sub_a(2, 0, 48, ca), self.half2[k][0].at[pl.ds(0, 1)], turn("y", 1, 4)),
            go(self.sub_a(2, 48, 48, ca), self.half2[k][0].at[pl.ds(1, 1)], turn("y", -1, 4)),
        ]
        copies[2].wait_recv()
        copies[3].wait_recv()
        add_into(self.block_b(0, 0, 96, cb), self.full_b[k].at[0], self.full_b[k].at[1])
        sent += [
            go(self.sub_b(2, 0, 48, cb), self.half2[k][1].at[pl.ds(0, 1)], turn("z", 1, 4)),
            go(self.sub_b(2, 48, 48, cb), self.half2[k][1].at[pl.ds(1, 1)], turn("z", -1, 4)),
        ]
        self.copies[k, 3] = sent

    def r2b(self, k):
        go, copies = self.wires.go, self.copies[k, 3]
        sent = []
        for colour, (sub, axis) in enumerate(((self.sub_a, "y"), (self.sub_b, "z"))):
            cols = cols_of(CHUNKS[k][colour])
            half, full = self.half2[k][colour], self.full2[k][colour]
            copies[2 * colour].wait_recv()
            add_into(sub(1, 0, 48, cols), half.at[pl.ds(0, 1)])
            sent.append(go(sub(1, 0, 96, cols), full.at[pl.ds(0, 1)], turn(axis, 1, 4)))
            copies[2 * colour + 1].wait_recv()
            add_into(sub(-1, 48, 48, cols), half.at[pl.ds(1, 1)])
            sent.append(go(sub(-1, 0, 96, cols), full.at[pl.ds(1, 1)], turn(axis, -1, 4)))
        self.copies[k, 4] = sent

    def r3(self, k):
        go, copies = self.wires.go, self.copies[k, 4]
        (a0, an), (b0, bn), _ = CHUNKS[k]
        for colour, sub in enumerate((self.sub_a, self.sub_b)):
            cols, full = cols_of(CHUNKS[k][colour]), self.full2[k][colour]
            copies[2 * colour].wait_recv()
            copies[2 * colour + 1].wait_recv()
            add_into(sub(0, 0, 96, cols), full.at[pl.ds(0, 1)], full.at[pl.ds(1, 1)])
        part = self.g.at[self.z, rows_of(96 * self.y + 48 * (1 - self.xh), 48), pl.ds(a0, an + bn)]
        self.copies[k, 5] = [go(part, self.last.at[:, pl.ds(a0, an + bn)], turn("xh", 1, 2))]

    def done(self, k):
        (a0, an), (b0, bn), _ = CHUNKS[k]
        self.copies[k, 5][0].wait_recv()
        cols = pl.ds(a0, an + bn)
        own = self.g[self.z, rows_of(96 * self.y + 48 * self.xh, 48), cols]
        self.store(a0, own.astype(F32) + self.last[:, cols].astype(F32))

    def store(self, start, total):
        if start >= 1152:
            self.out[:, pl.ds(start, total.shape[1])] = total
            return
        for at in range(0, total.shape[1], 128):
            head, which = (start + at) // 384, (start + at) % 384 // 128
            self.out[:, pl.ds(384 * which + 128 * head, 128)] = total[:, at : at + 128]

    def column(self, y, xh, planes, k):
        return self.g.at[planes, rows_of(96 * y + 48 * xh, 48), cols_of(CHUNKS[k][2])]

    def c1(self, k):
        self.copies[k, 6] = [
            self.wires.go(
                self.column(y, 1 - self.xh, pl.ds(0, 4), k), self.third[k][0].at[y], turn("xh", 1, 2)
            )
            for y in range(4)
        ]

    def c2(self, k):
        for y, copy in enumerate(self.copies[k, 6]):
            copy.wait_recv()
            add_into(self.column(y, self.xh, pl.ds(0, 4), k), self.third[k][0].at[y])
        half, far = self.third[k][1], near("y", 2)
        self.copies[k, 7] = [
            self.wires.go(self.column(far, self.xh, pl.ds(0, 2), k), half.at[0], turn("y", 1, 4)),
            self.wires.go(self.column(far, self.xh, pl.ds(2, 2), k), half.at[1], turn("y", -1, 4)),
        ]

    def c2b(self, k):
        half, full = self.third[k][1], self.third[k][2]
        sent = []
        for i, step in enumerate((1, -1)):
            self.copies[k, 7][i].wait_recv()
            add_into(self.column(near("y", step), self.xh, pl.ds(2 * i, 2), k), half.at[i])
            part = self.column(near("y", step), self.xh, pl.ds(0, 4), k)
            sent.append(self.wires.go(part, full.at[i], turn("y", step, 4)))
        self.copies[k, 8] = sent

    def c3(self, k):
        for copy in self.copies[k, 8]:
            copy.wait_recv()
        full, pieces = self.third[k][2], self.third[k][3]
        add_into(self.column(self.y, self.xh, pl.ds(0, 4), k), full.at[0], full.at[1])
        self.copies[k, 9] = [
            self.wires.go(
                self.column(self.y, self.xh, near("z", step), k), pieces.at[i], turn("z", step, 4)
            )
            for i, step in enumerate((1, -1, 2))
        ]

    def c4(self, k):
        start, count = CHUNKS[k][2]
        total = self.g[self.z, rows_of(96 * self.y + 48 * self.xh, 48), pl.ds(start, count)].astype(F32)
        for i, copy in enumerate(self.copies[k, 9]):
            copy.wait_recv()
            total = total + self.third[k][3][i].astype(F32)
        self.store(start, total)


def scatter_buffers():
    shapes = []
    for (_, an), (_, bn), (_, cn) in CHUNKS:
        shapes += [
            pltpu.VMEM((2, 192, an), BF),
            pltpu.VMEM((2, 384, an), BF),
            pltpu.VMEM((2, 4, 48, bn), BF),
            pltpu.VMEM((2, 4, 96, bn), BF),
            pltpu.VMEM((2, 48, an), BF),
            pltpu.VMEM((2, 96, an), BF),
            pltpu.VMEM((2, 48, bn), BF),
            pltpu.VMEM((2, 96, bn), BF),
        ]
        if cn:
            shapes += [
                pltpu.VMEM((4, 4, 48, cn), BF),
                pltpu.VMEM((2, 2, 48, cn), BF),
                pltpu.VMEM((2, 4, 48, cn), BF),
                pltpu.VMEM((3, 48, cn), BF),
            ]
    return shapes


def make_scatter(wires, g, bufs, last, out):
    groups, bufs = [], list(bufs)
    for chunk in CHUNKS:
        count = 12 if chunk[2][1] else 8
        groups.append(bufs[:count])
        bufs = bufs[count:]
    return Scatter(
        wires,
        g,
        [b[0] for b in groups],
        [b[1] for b in groups],
        [b[2] for b in groups],
        [b[3] for b in groups],
        [(b[4], b[6]) for b in groups],
        [(b[5], b[7]) for b in groups],
        [b[8:] for b in groups],
        last,
        out,
    )


def nn(a, b):
    return jnp.dot(a, b, preferred_element_type=F32)


def nt(a, b):
    return lax.dot_general(a, b, (((1,), (1,)), ((), ())), preferred_element_type=F32)


def tn(a, b):
    return lax.dot_general(a, b, (((0,), (0,)), ((), ())), preferred_element_type=F32)


class Spread:
    def __init__(self, wires, buf):
        self.wires, self.buf = wires, buf
        self.xl, self.c = (lax.axis_index(a) for a in SP)
        self.far, self.near, self.relays = {}, {}, {}

    def block(self, xl, c, start=0, count=128):
        return self.buf.at[rows_of(256 * xl + 128 * c + start, count), :]

    def start(self, i):
        part = self.block(self.xl, self.c, 64 * i, 64)
        self.far[i] = self.wires.go(part, part, turn("xl", 1, 2))
        self.near[i] = self.wires.go(part, part, turn("c", 1, 2))

    def relay(self, i):
        self.far[i].wait_recv()
        part = self.block(1 - self.xl, self.c, 64 * i, 64)
        self.relays[i] = self.wires.go(part, part, turn("c", 1, 2))

    def own_half(self):
        for copy in self.near.values():
            copy.wait_recv()

    def done(self):
        for copy in self.relays.values():
            copy.wait_recv()

    def release(self):
        for group in (self.far, self.near, self.relays):
            for copy in group.values():
                self.wires.sent(copy)


class Collect:
    def __init__(self, wires, part, pair, cross):
        self.wires, self.part, self.pair, self.cross = wires, part, pair, cross
        self.xl, self.c = (lax.axis_index(a) for a in SP)

    def block(self, xl, c):
        return self.part.at[rows_of(256 * xl + 128 * c, 128), :]

    def other(self):
        self.first = self.wires.go(self.block(1 - self.xl, 1 - self.c), self.pair.at[0], turn("c", 1, 2))

    def send(self):
        self.first.wait_recv()
        self.third = []
        for i in range(2):
            rows = pl.ds(64 * i, 64)
            mine = self.block(1 - self.xl, self.c).at[rows, :]
            add2(mine, self.pair.at[0, rows, :])
            self.third.append(self.wires.go(mine, self.cross.at[rows, :], turn("xl", 1, 2)))

    def own(self):
        self.second = self.wires.go(self.block(self.xl, 1 - self.c), self.pair.at[1], turn("c", 1, 2))

    def wait(self, i):
        if i == 0:
            self.second.wait_recv()
        self.third[i].wait_recv()

    def release(self):
        for copy in (self.first, self.second, *self.third):
            self.wires.sent(copy)

    def rows(self, start, count):
        at = rows_of(256 * self.xl + 128 * self.c + start, count)
        total = self.part[at, :].astype(F32) + self.pair[1, pl.ds(start, count), :].astype(F32)
        return total + self.cross[pl.ds(start, count), :].astype(F32)


def add2(dst, src):
    rows = dst.shape[0]

    @pl.loop(0, rows // 16)
    def _(i):
        at = (pl.ds(pl.multiple_of(i * 16, 16), 16), slice(None))
        dst[at] = (dst[at].astype(F32) + src[at].astype(F32)).astype(dst.dtype)


def normalize(stream):
    mean_part = jnp.mean(stream, axis=-1, keepdims=True)
    centred = stream - mean_part
    rstd = lax.rsqrt(jnp.mean(centred * centred, axis=-1, keepdims=True) + ln_eps)
    return (centred * rstd, rstd)


def norm_back(normed, rstd, incoming):
    first = jnp.mean(incoming, axis=-1, keepdims=True)
    second = jnp.mean(incoming * normed, axis=-1, keepdims=True)
    return rstd * (incoming - first - normed * second)


BLOCK = 16
ROOT = math.sqrt(2.0 / math.pi)


def by_rows(fn, start=0, count=128):
    @pl.loop(start // BLOCK, (start + count) // BLOCK)
    def _(i):
        fn(pl.multiple_of(i * BLOCK, BLOCK))


def block_kernel(
    x_in, m_in, og_in, wq_ref, wo_ref, wi_ref, wb_ref,
    final_out, ig_out, sums_out,
    x_ref, m_ref, og_ref, final_ref, ig_ref, sums_ref,
    w, g, last, a1, dm, a2, da, qkv, o, do, gp, act, part, probs, dv, pair0, cross0, pair1, cross1,
    mid, dmid, send, recv, local_sem, *bufs,
):
    z, y, xh, xl, c = (lax.axis_index(a) for a in FSDP + SP)
    shard_rows = rows_of(96 * y + 48 * xh, 48)
    pieces = [
        (wq_ref.at[which, :, pl.ds(128 * h, 128)], 384 * h + 128 * which, 128)
        for h in range(3)
        for which in range(3)
    ]
    pieces += [(wo_ref, 1152, 384), (wi_ref, 1536, 1536), (wb_ref, 3072, 1536)]
    loads = [
        pltpu.make_async_copy(part, w.at[z, shard_rows, pl.ds(at, count)], local_sem.at[i])
        for i, (part, at, count) in enumerate(pieces)
    ]
    inputs = [
        pltpu.make_async_copy(a, b, local_sem.at[12 + i])
        for i, (a, b) in enumerate(((x_in, x_ref), (m_in, m_ref), (og_in, og_ref)))
    ]
    outputs = {
        name: pltpu.make_async_copy(a, b, local_sem.at[15 + i])
        for i, (name, a, b) in enumerate(
            (("final", final_ref, final_out), ("ig", ig_ref, ig_out), ("sums", sums_ref, sums_out))
        )
    }
    greet()
    for load in loads[:3] + inputs[:2] + loads[3:] + inputs[2:]:
        load.start()
    wires = Wires(send, recv)
    ag = Gather(wires, w)
    rs = make_scatter(wires, g, bufs, last, sums_ref)
    own_row = 256 * xl + 128 * c
    own_start, other_start = 256 * xl, 256 * (1 - xl)
    scale = 1.0 / math.sqrt(32 * 512)
    factor = temper / math.sqrt(HEAD_DIM)
    steps = {}

    def step(fn):
        steps[fn.__name__] = fn
        return fn

    def mod(i):
        return m_ref[i]

    def own(start):
        return (rows_of(own_row + start, BLOCK), slice(None))

    def weights(start, count):
        return w[:, :, pl.ds(start, count)].reshape(1536, count)

    for k in range(len(CHUNKS)):
        third = ("c1", "c2", "c2b", "c3") if CHUNKS[k][2][1] else ()
        for name in ("s1", "s2", "s2b", "s3", "s3b", "done", *third):
            steps[f"ag_{name}_{k}"] = functools.partial(getattr(ag, name), k)
        for name in ("r1", "r1b", "r2", "r2b", "r3", "done", *third, *(("c4",) if third else ())):
            steps[f"rs_{name}_{k}"] = functools.partial(getattr(rs, name), k)
    for key, buf in (("a1", a1), ("dm", dm), ("a2", a2), ("da", da)):
        spread = Spread(wires, buf)
        for i in range(2):
            steps[f"{key}_start_{i}"] = functools.partial(spread.start, i)
            steps[f"{key}_relay_{i}"] = functools.partial(spread.relay, i)
        steps[f"{key}_own_half"] = spread.own_half
        steps[f"{key}_done"] = spread.done
        steps[f"{key}_release"] = spread.release
    reds = {
        "att": Collect(wires, part, pair0, cross0),
        "da2": Collect(wires, part, pair0, cross0),
        "da1": Collect(wires, part, pair0, cross0),
        "ffn": Collect(wires, dm, pair1, cross1),
    }
    for key, red in reds.items():
        for name in ("other", "own", "send", "release"):
            steps[f"{key}_{name}"] = getattr(red, name)
        for i in range(2):
            steps[f"{key}_wait_{i}"] = functools.partial(red.wait, i)

    @step
    def load_first():
        for load in loads[:3]:
            load.wait()

    steps["met"] = met

    @step
    def load_inputs():
        inputs[0].wait()
        inputs[1].wait()

    @step
    def load_rest():
        for load in loads[3:]:
            load.wait()
        inputs[2].wait()

    def first_norm(r):
        n1, _ = normalize(x_ref[pl.ds(r, BLOCK), :].astype(F32))
        a1[own(r)] = (n1 * (1.0 + mod(1)) + mod(0)).astype(BF)

    def second_norm(r):
        rows = pl.ds(r, BLOCK)
        value = x_ref[rows, :].astype(F32) + mod(2) * reds["att"].rows(r, BLOCK)
        mid[rows, :] = value
        n2, _ = normalize(value)
        a2[own(r)] = (n2 * (1.0 + mod(4)) + mod(3)).astype(BF)

    def mid_grad(r):
        rows = pl.ds(r, BLOCK)
        n2, r2 = normalize(mid[rows, :])
        inner = norm_back(n2, r2, reds["da2"].rows(r, BLOCK) * (1.0 + mod(4)))
        value = og_ref[rows, :].astype(F32) + inner
        dmid[rows, :] = value
        da[own(r)] = (mod(2) * value).astype(BF)

    for i in range(2):
        for fn in (first_norm, second_norm, mid_grad):
            steps[f"{fn.__name__}_{i}"] = functools.partial(by_rows, fn, 64 * i, 64)

    @step
    def gate_grad():
        def rows(r):
            dm[own(r)] = (mod(5) * og_ref[pl.ds(r, BLOCK), :].astype(F32)).astype(BF)

        by_rows(rows)

    def lanes(h, which):
        return pl.ds(384 * h + 128 * which, 128)

    def project(start, count):
        qkv[:, pl.ds(start, count)] = nn(a1[...], weights(start, count)).astype(BF)

    @step
    def project_0():
        project(0, 256)
        project(256, 128)

    @step
    def project_1():
        @pl.loop(0, 3)
        def _(j):
            project(pl.multiple_of(384 + j * 256, 128), 256)

    def attend(heads, start, blocks):
        @pl.loop(0, blocks)
        def _(i):
            rows = rows_of(start + i * 128, 128)
            for h in heads:
                s = nt(qkv[rows, lanes(h, 0)], qkv[:, lanes(h, 1)]) * factor
                e = jnp.exp(s - jnp.max(s, axis=-1, keepdims=True))
                p = (e * (1.0 / jnp.sum(e, axis=-1, keepdims=True))).astype(BF)
                probs[h, rows, :] = p
                o[rows, pl.ds(128 * h, 128)] = nn(p, qkv[:, lanes(h, 2)]).astype(BF)

    steps["attend_0"] = functools.partial(attend, (0,), 0, 4)
    steps["attend_other"] = functools.partial(attend, (1, 2), other_start, 2)
    steps["attend_own"] = functools.partial(attend, (1, 2), own_start, 2)

    def back_half(dst, lhs, start, at, count):
        rows = rows_of(start, 256)

        @pl.loop(0, 2)
        def _(j):
            rhs = w[pl.ds(2 * j, 2), :, pl.ds(at, count)].reshape(768, count)
            dst[rows, pl.ds(pl.multiple_of(768 * j, 128), 768)] = nt(lhs[rows, :], rhs).astype(BF)

    for key, dst, lhs, at, count in (
        ("att", part, o, 1152, 384),
        ("da2", part, gp, 1536, 1536),
        ("da1", part, qkv, 0, 1152),
        ("ffn", dm, act, 3072, 1536),
    ):
        steps[f"{key}_mm_other"] = functools.partial(back_half, dst, lhs, other_start, at, count)
        steps[f"{key}_mm_own"] = functools.partial(back_half, dst, lhs, own_start, at, count)

    def hidden(start, half):
        rows = rows_of(start, 256)

        @pl.loop(3 * half, 3 * half + 3)
        def _(j):
            at = pl.multiple_of(j * 256, 256)
            u = nn(a2[rows, :], weights(pl.multiple_of(1536 + at, 256), 256))
            sq = u * u
            t = jnp.tanh(ROOT * u * (1.0 + 0.044715 * sq))
            half = 0.5 * (1.0 + t)
            act[rows, pl.ds(at, 256)] = (u * half).astype(BF)
            slope = half + (0.5 * ROOT) * u * (1.0 - t * t) * (1.0 + (3 * 0.044715) * sq)
            gp[rows, pl.ds(at, 256)] = slope.astype(BF)

    def hidden_grad(half):
        @pl.loop(3 * half, 3 * half + 3)
        def _(j):
            at = pl.multiple_of(j * 256, 256)
            cols = pl.ds(at, 256)
            dg = nn(dm[...], weights(pl.multiple_of(3072 + at, 256), 256))
            gp[:, cols] = (gp[:, cols].astype(F32) * dg).astype(BF)

    def grad(left, right, right_at, at, count):
        @pl.loop(0, 4)
        def _(j):
            lhs = left[:, pl.ds(pl.multiple_of(384 * j, 128), 384)]
            value = tn(lhs, right[:, pl.ds(right_at, count)]) * scale
            g[j, :, pl.ds(at, count)] = value.astype(BF)

    for i in range(2):
        steps[f"hidden_own_{i}"] = functools.partial(hidden, own_start, i)
        steps[f"hidden_other_{i}"] = functools.partial(hidden, other_start, i)
        steps[f"hidden_grad_{i}"] = functools.partial(hidden_grad, i)
        steps[f"grad_in_{i}"] = functools.partial(grad, a2, gp, 768 * i, 1536 + 768 * i, 768)
        steps[f"grad_back_{i}"] = functools.partial(grad, dm, act, 768 * i, 3072 + 768 * i, 768)
    steps["grad_out"] = functools.partial(grad, da, o, 0, 1152, 384)
    steps["grad_q_0"] = functools.partial(grad, a1, qkv, 0, 0, 384)
    steps["grad_q_1"] = functools.partial(grad, a1, qkv, 384, 384, 768)

    def head_grads(start):
        rows = rows_of(start, 256)
        do[rows, :] = nn(da[rows, :], weights(1152, 384)).astype(BF)

    steps["heads_own"] = functools.partial(head_grads, own_start)
    steps["heads_other"] = functools.partial(head_grads, other_start)

    def attend_back(heads):
        for n, h in enumerate(heads):
            dv[n] = tn(probs[h], do[:, pl.ds(128 * h, 128)]).astype(BF)

        @pl.loop(0, 4)
        def _(i):
            rows = pl.ds(pl.multiple_of(i * 128, 128), 128)
            for h in heads:
                dp = nt(do[rows, pl.ds(128 * h, 128)], qkv[:, lanes(h, 2)])
                p = probs[h, rows, :].astype(F32)
                ds = factor * p * (dp - jnp.sum(p * dp, axis=-1, keepdims=True))
                probs[h, rows, :] = ds.astype(BF)

        for n, h in enumerate(heads):
            dk = tn(probs[h], qkv[:, lanes(h, 0)]).astype(BF)
            qkv[:, lanes(h, 0)] = nn(probs[h], qkv[:, lanes(h, 1)]).astype(BF)
            qkv[:, lanes(h, 1)] = dk
            qkv[:, lanes(h, 2)] = dv[n]

    steps["attend_back_0"] = functools.partial(attend_back, (0,))
    steps["attend_back_1"] = functools.partial(attend_back, (1, 2))

    @step
    def last_out():
        def each(r):
            rows = pl.ds(r, BLOCK)
            final_ref[rows, :] = (mid[rows, :] + mod(5) * reds["ffn"].rows(r, BLOCK)).astype(BF)

        by_rows(each)
        outputs["final"].start()

    @step
    def first_grad():
        def each(r):
            rows = pl.ds(r, BLOCK)
            n1, r1 = normalize(x_ref[rows, :].astype(F32))
            inner = norm_back(n1, r1, reds["da1"].rows(r, BLOCK) * (1.0 + mod(1)))
            ig_ref[rows, :] = dmid[rows, :] + inner

        by_rows(each)
        outputs["ig"].start()

    @step
    def finish():
        outputs["sums"].start()
        wires.drain()
        for copy in outputs.values():
            copy.wait()

    for name in ORDER:
        with jax.named_scope(name):
            steps[name]()


def finish_kernel(
    final_in, ig_in, sums_in, final_out, ig_out, gq_out, go_out, gi_out, gb_out, final, ig, sums, sem
):
    cuts = [(384 * which, 384, gq_out.at[which]) for which in range(3)]
    cuts += [(1152, 384, go_out), (1536, 1536, gi_out), (3072, 1536, gb_out)]
    pairs = [(sums_in.at[:, pl.ds(at, n)], sums.at[:, pl.ds(at, n)], out) for at, n, out in cuts]
    pairs += [(ig_in, ig, ig_out), (final_in, final, final_out)]
    loads, stores = [], []
    for i, (source, held, out) in enumerate(pairs):
        loads.append(pltpu.make_async_copy(source, held, sem.at[0, i]))
        stores.append(pltpu.make_async_copy(held, out, sem.at[1, i]))
    for load in loads:
        load.start()
    for load, store in zip(loads, stores):
        load.wait()
        store.start()
    for store in stores:
        store.wait()


def body(tokens, modulation, w_qkv, w_out, w_in, w_back, out_grad):
    own = w_qkv.shape[3]
    far = pl.BlockSpec(memory_space=pl.ANY)
    copies = 54 * len(CHUNKS) + 40
    rows = lambda n, dtype=BF: pltpu.VMEM((512, n), dtype)
    final, grad_in_rows, sums = pl.pallas_call(
        block_kernel,
        out_shape=(
            jax.ShapeDtypeStruct((128, 1536), BF),
            jax.ShapeDtypeStruct((128, 1536), F32),
            jax.ShapeDtypeStruct((48, WIDTH), F32),
        ),
        in_specs=[far] * 7,
        out_specs=(far, far, far),
        scratch_shapes=[
            pltpu.VMEM((128, 1536), BF),
            pltpu.VMEM((6, 1, 1536), F32),
            pltpu.VMEM((128, 1536), BF),
            pltpu.VMEM((128, 1536), BF),
            pltpu.VMEM((128, 1536), F32),
            pltpu.VMEM((48, WIDTH), F32),
            pltpu.VMEM((4, 384, WIDTH), BF),
            pltpu.VMEM((4, 384, WIDTH), BF),
            pltpu.VMEM((48, WIDTH), BF),
            rows(1536), rows(1536), rows(1536), rows(1536),
            rows(1152), rows(384), rows(384),
            rows(1536), rows(1536), rows(1536),
            pltpu.VMEM((3, 512, 512), BF),
            pltpu.VMEM((2, 512, 128), BF),
            pltpu.VMEM((2, 128, 1536), BF),
            pltpu.VMEM((128, 1536), BF),
            pltpu.VMEM((2, 128, 1536), BF),
            pltpu.VMEM((128, 1536), BF),
            pltpu.VMEM((128, 1536), F32),
            pltpu.VMEM((128, 1536), F32),
            pltpu.SemaphoreType.DMA((copies,)),
            pltpu.SemaphoreType.DMA((copies,)),
            pltpu.SemaphoreType.DMA((18,)),
            *scatter_buffers(),
        ],
        compiler_params=pltpu.CompilerParams(
            collective_id=0, has_side_effects=True, vmem_limit_bytes=VMEM_LIMIT
        ),
        name="block",
    )(
        tokens[0],
        modulation[0].transpose(1, 0, 2),
        out_grad[0],
        w_qkv[0].transpose(1, 0, 2),
        w_out[0].T,
        w_in[0],
        w_back[0].T,
    )
    outs = pl.pallas_call(
        finish_kernel,
        out_shape=(
            jax.ShapeDtypeStruct((128, 1536), BF),
            jax.ShapeDtypeStruct((128, 1536), F32),
            jax.ShapeDtypeStruct((3, 48, own), F32),
            jax.ShapeDtypeStruct((48, own), F32),
            jax.ShapeDtypeStruct((48, 4 * own), F32),
            jax.ShapeDtypeStruct((48, 4 * own), F32),
        ),
        in_specs=[far] * 3,
        out_specs=(far,) * 6,
        scratch_shapes=[
            pltpu.VMEM((128, 1536), BF),
            pltpu.VMEM((128, 1536), F32),
            pltpu.VMEM((48, WIDTH), F32),
            pltpu.SemaphoreType.DMA((2, 8)),
        ],
        name="finish",
    )(final, grad_in_rows, sums)
    final, grad_in_rows, gq, go, gi, gb = outs
    return (final[None], grad_in_rows[None], gq.transpose(1, 0, 2)[None], go.T[None], gi[None], gb.T[None])


def solution(mesh):
    torus = Mesh(mesh.devices.reshape(4, 4, 2, 2, 2), FSDP + SP)
    return jax.shard_map(
        body,
        mesh=torus,
        in_specs=(
            P(FSDP, SP, None),
            P(FSDP, None, None, None),
            P(None, FSDP, None, SP),
            P(None, SP, FSDP),
            P(None, FSDP, SP),
            P(None, SP, FSDP),
            P(FSDP, SP, None),
        ),
        out_specs=(
            P(FSDP, SP, None),
            P(FSDP, SP, None),
            P(None, FSDP, None, SP),
            P(None, SP, FSDP),
            P(None, FSDP, SP),
            P(None, SP, FSDP),
        ),
        check_vma=False,
    )
```

```python
import functools
import math

import jax
import jax.numpy as jnp
from jax import lax
from jax.experimental import pallas as pl
from jax.experimental.pallas import tpu as pltpu
from jax.sharding import Mesh
from jax.sharding import PartitionSpec as P

HEAD_DIM = 128
MESH = pl.DeviceIdType.MESH
FSDP = ("z", "y", "xh")
SP = ("xl", "c")
BF = jnp.bfloat16
F32 = jnp.float32

ln_eps = 1e-06
temper = 2.5
VMEM_LIMIT = 67_000_000

TILES = ((2, 1), (3, 3), (1, 2), (3, 3), (3, 3))


def split_chunks():
    chunks, at = [], 0
    for tiles in TILES:
        parts = []
        for count in tiles:
            parts.append((at, 128 * count))
            at += 128 * count
        chunks.append(tuple(parts))
    return tuple(chunks)


CHUNKS = split_chunks()
HELD = 3072
STEPS = {"own": 0, "next": 1, "prev": -1, "far": 2}
WIDTH = 4608
ORDER = (
    "load_first",
    "load_inputs",
    "met",
    "ag_s1_0",
    "first_norm_0",
    "load_rest",
    "gate_grad",
    "ag_s1_2",
    "ag_s1_1",
    "ag_s2_0",
    "first_norm_1",
    "a1_start_0",
    "ag_s2_2",
    "ag_s2b_0",
    "ag_s2_1",
    "ag_s2b_2",
    "a1_start_1",
    "ag_s3_0",
    "ag_s2b_1",
    "ag_s1_4",
    "dm_start_0",
    "ag_s3_2",
    "a1_relay_0",
    "ag_s1_3",
    "ag_s3_1",
    "a1_own_half",
    "ag_s3b_0",
    "dm_start_1",
    "a1_relay_1",
    "ag_s3b_1",
    "a1_done",
    "ag_s3b_2",
    "dm_relay_0",
    "ag_s2_3",
    "ag_done_0",
    "project_0",
    "attend_0",
    "ag_done_1",
    "project_1",
    "ag_s2_4",
    "ag_done_2",
    "attend_other",
    "att_mm_other",
    "ag_s2b_3",
    "att_other",
    "ag_s2b_4",
    "att_send",
    "ag_s3_3",
    "attend_own",
    "dm_relay_far",
    "att_mm_own",
    "att_own",
    "dm_relay_1",
    "dm_own_half",
    "dm_done",
    "att_wait_0",
    "second_norm_0",
    "ag_s3_4",
    "a2_start_0",
    "att_wait_1",
    "second_norm_1",
    "ag_s3b_3",
    "a2_start_1",
    "a2_own_half",
    "ag_s3b_4",
    "a2_relay_0",
    "a2_relay_1",
    "ag_done_3",
    "hidden_own",
    "a2_done",
    "hidden_next",
    "dm_done_far",
    "ag_done_4",
    "hgrad_next",
    "a2_relay_far",
    "da2_mm_next",
    "a2_done_far",
    "da2_give_next",
    "hidden_far",
    "hgrad_far",
    "da2_mm_far",
    "da2_give_far",
    "hidden_prev",
    "da2_take_far",
    "hgrad_prev",
    "da2_mm_prev",
    "da2_take_next",
    "da2_give_prev",
    "grad_back_1",
    "da2_take_prev",
    "grad_back_0",
    "hgrad_own",
    "rs_r1_4",
    "da2_pass_on",
    "grad_in_0",
    "dm_release",
    "att_release",
    "grad_in_1",
    "rs_r1_3",
    "da2_mm_own",
    "da2_give_own",
    "rs_r1b_4",
    "ffn_mm_prev",
    "da2_take_own",
    "da2_wait",
    "mid_grad_0",
    "da_start_0",
    "mid_grad_1",
    "ffn_give_prev",
    "da_start_1",
    "ffn_mm_own",
    "ffn_mm_far",
    "ffn_give_far",
    "ffn_mm_next",
    "ffn_take_far",
    "da_own_half",
    "rs_r1b_3",
    "da_relay_0",
    "rs_r2_4",
    "heads_own",
    "ffn_give_next",
    "da_relay_1",
    "da_done",
    "grad_out",
    "rs_r1_2",
    "ffn_give_own",
    "heads_other",
    "rs_r2_3",
    "rs_r2b_4",
    "attend_back_1",
    "rs_r1b_2",
    "rs_r2b_3",
    "grad_q_1",
    "rs_r1_1",
    "attend_back_0",
    "ffn_take_next",
    "grad_q_0",
    "rs_r1_0",
    "da1_mm_other",
    "ffn_take_own",
    "ffn_take_prev",
    "rs_r3_3",
    "rs_r2_2",
    "rs_r3_4",
    "da1_other",
    "rs_r1b_1",
    "rs_r1b_0",
    "ffn_pass_on",
    "da1_send",
    "rs_done_3",
    "rs_r2_1",
    "da1_mm_own",
    "da1_own",
    "rs_r2b_2",
    "rs_r2_0",
    "rs_r2b_1",
    "rs_r2b_0",
    "rs_r3_2",
    "rs_r3_1",
    "rs_done_4",
    "da1_wait_0",
    "ffn_wait",
    "last_out",
    "rs_r3_0",
    "rs_done_2",
    "da1_wait_1",
    "first_grad",
    "rs_done_1",
    "rs_done_0",
    "finish",
)


def turn(axis, step, size):
    return {axis: lax.rem(lax.axis_index(axis) + step + size, size)}


def near(axis, step):
    return lax.rem(lax.axis_index(axis) + step + 4, 4)


class Wires:
    def __init__(self, send, recv):
        self.send, self.recv, self.used, self.open = send, recv, 0, []

    def go(self, src, dst, device):
        at = self.used
        self.used += 1
        copy = pltpu.make_async_remote_copy(
            src_ref=src,
            dst_ref=dst,
            send_sem=self.send.at[at],
            recv_sem=self.recv.at[at],
            device_id=device,
            device_id_type=MESH,
        )
        copy.start()
        self.open.append(copy)
        return copy

    def sent(self, copy):
        copy.wait_send()
        self.open = [other for other in self.open if other is not copy]

    def drain(self):
        for copy in self.open:
            copy.wait_send()
        self.open = []


def chip(step):
    xh, xl = lax.axis_index("xh"), lax.axis_index("xl")
    if step == 0:
        return xh, xl
    if step == 2:
        return 1 - xh, xl
    return lax.rem(xh + xl + (0 if step == 1 else 1), 2), 1 - xl


def along(step):
    xh, xl = chip(step)
    return {"xh": xh, "xl": xl}


def partners():
    return [turn("z", 1, 4), turn("z", -1, 4), turn("y", 1, 4), turn("y", -1, 4)] + [
        turn("xh", 1, 2), turn("c", 1, 2), along(1), along(-1)
    ]


def greet():
    for device in partners():
        pl.semaphore_signal(
            pltpu.get_barrier_semaphore(), inc=1, device_id=device, device_id_type=MESH
        )


def met():
    pl.semaphore_wait(pltpu.get_barrier_semaphore(), len(partners()))


def rows_of(start, count):
    return pl.ds(pl.multiple_of(start, 16), count)


def cols_of(cols):
    return pl.ds(cols[0], cols[1])


class Gather:
    def __init__(self, wires, w, stage):
        self.wires, self.w, self.stage = wires, w, stage
        self.z, self.y, self.xh = (lax.axis_index(a) for a in FSDP)
        self.one, self.two, self.relay2, self.three, self.relay3 = {}, {}, {}, {}, {}

    def same(self, part, device):
        return self.wires.go(part, part, device)

    def s1(self, k):
        (a0, an), (b0, bn) = CHUNKS[k]
        part = self.w.at[self.z, rows_of(96 * self.y + 48 * self.xh, 48), pl.ds(a0, an + bn)]
        source = part if k < 3 else self.stage.at[:, pl.ds(a0 - 1536, an + bn)]
        self.one[k] = self.wires.go(source, part, turn("xh", 1, 2))

    def s2(self, k):
        self.one[k].wait_recv()
        ca, cb = map(cols_of, CHUNKS[k])
        pa = self.w.at[self.z, rows_of(96 * self.y, 96), ca]
        pb = self.w.at[self.z, rows_of(96 * self.y, 96), cb]
        self.two[k] = [
            self.same(pa, turn("y", 1, 4)),
            self.same(pa, turn("y", -1, 4)),
            self.same(pb, turn("z", 1, 4)),
            self.same(pb, turn("z", -1, 4)),
        ]

    def s2b(self, k):
        ca, cb = map(cols_of, CHUNKS[k])
        for copy in self.two[k]:
            copy.wait_recv()
        w, z, y = self.w, self.z, self.y
        self.relay2[k] = [
            self.same(w.at[z, rows_of(96 * near("y", -1), 48), ca], turn("y", 1, 4)),
            self.same(w.at[z, rows_of(96 * near("y", 1) + 48, 48), ca], turn("y", -1, 4)),
            self.same(w.at[near("z", -1), rows_of(96 * y, 48), cb], turn("z", 1, 4)),
            self.same(w.at[near("z", 1), rows_of(96 * y + 48, 48), cb], turn("z", -1, 4)),
        ]

    def s3(self, k):
        ca, cb = map(cols_of, CHUNKS[k])
        for copy in self.relay2[k]:
            copy.wait_recv()
        pa = self.w.at[self.z, :, ca]
        pb = self.w.at[:, rows_of(96 * self.y, 96), cb]
        self.three[k] = [
            self.same(pa, turn("z", 1, 4)),
            self.same(pa, turn("z", -1, 4)),
            self.same(pb, turn("y", 1, 4)),
            self.same(pb, turn("y", -1, 4)),
        ]

    def s3b(self, k):
        ca, cb = map(cols_of, CHUNKS[k])
        for copy in self.three[k]:
            copy.wait_recv()
        w = self.w
        self.relay3[k] = [
            self.same(w.at[near("z", -1), pl.ds(0, 192), ca], turn("z", 1, 4)),
            self.same(w.at[near("z", 1), pl.ds(192, 192), ca], turn("z", -1, 4)),
            self.same(w.at[:, rows_of(96 * near("y", -1), 48), cb], turn("y", 1, 4)),
            self.same(w.at[:, rows_of(96 * near("y", 1) + 48, 48), cb], turn("y", -1, 4)),
        ]

    def done(self, k):
        for copy in self.relay3[k]:
            copy.wait_recv()


def add_into(dst, *srcs):
    planes, rows, columns = dst.shape

    @pl.loop(0, planes * (rows // 48))
    def _(i):
        at = (i // (rows // 48), pl.ds(pl.multiple_of((i % (rows // 48)) * 48, 48), 48), slice(None))
        total = dst[at].astype(F32)
        for src in srcs:
            total = total + src[at].astype(F32)
        dst[at] = total.astype(dst.dtype)


class Scatter:
    def __init__(self, wires, g, half_a, full_a, half_b, full_b, half2, full2, last, out):
        self.wires, self.g, self.out = wires, g, out
        self.half_a, self.full_a, self.half_b, self.full_b = half_a, full_a, half_b, full_b
        self.half2, self.full2, self.last = half2, full2, last
        self.z, self.y, self.xh = (lax.axis_index(a) for a in FSDP)
        self.copies = {}

    def block_a(self, step, start, count, cols):
        return self.g.at[pl.ds(near("z", step), 1), pl.ds(start, count), cols]

    def block_b(self, step, start, count, cols):
        return self.g.at[:, rows_of(96 * near("y", step) + start, count), cols]

    def sub_a(self, step, start, count, cols):
        return self.g.at[pl.ds(self.z, 1), rows_of(96 * near("y", step) + start, count), cols]

    def sub_b(self, step, start, count, cols):
        return self.g.at[pl.ds(near("z", step), 1), rows_of(96 * self.y + start, count), cols]

    def r1(self, k):
        ca, cb = map(cols_of, CHUNKS[k])
        go = self.wires.go
        self.copies[k, 1] = [
            go(self.block_a(2, 0, 192, ca), self.half_a[k].at[pl.ds(0, 1)], turn("z", 1, 4)),
            go(self.block_a(2, 192, 192, ca), self.half_a[k].at[pl.ds(1, 1)], turn("z", -1, 4)),
            go(self.block_b(2, 0, 48, cb), self.half_b[k].at[0], turn("y", 1, 4)),
            go(self.block_b(2, 48, 48, cb), self.half_b[k].at[1], turn("y", -1, 4)),
        ]

    def r1b(self, k):
        ca, cb = map(cols_of, CHUNKS[k])
        go, copies = self.wires.go, self.copies[k, 1]
        sent = []
        copies[0].wait_recv()
        add_into(self.block_a(1, 0, 192, ca), self.half_a[k].at[pl.ds(0, 1)])
        sent.append(go(self.block_a(1, 0, 384, ca), self.full_a[k].at[pl.ds(0, 1)], turn("z", 1, 4)))
        copies[1].wait_recv()
        add_into(self.block_a(-1, 192, 192, ca), self.half_a[k].at[pl.ds(1, 1)])
        sent.append(go(self.block_a(-1, 0, 384, ca), self.full_a[k].at[pl.ds(1, 1)], turn("z", -1, 4)))
        copies[2].wait_recv()
        add_into(self.block_b(1, 0, 48, cb), self.half_b[k].at[0])
        sent.append(go(self.block_b(1, 0, 96, cb), self.full_b[k].at[0], turn("y", 1, 4)))
        copies[3].wait_recv()
        add_into(self.block_b(-1, 48, 48, cb), self.half_b[k].at[1])
        sent.append(go(self.block_b(-1, 0, 96, cb), self.full_b[k].at[1], turn("y", -1, 4)))
        self.copies[k, 2] = sent

    def r2(self, k):
        ca, cb = map(cols_of, CHUNKS[k])
        go, copies = self.wires.go, self.copies[k, 2]
        copies[0].wait_recv()
        copies[1].wait_recv()
        add_into(
            self.block_a(0, 0, 384, ca), self.full_a[k].at[pl.ds(0, 1)], self.full_a[k].at[pl.ds(1, 1)]
        )
        sent = [
            go(self.sub_a(2, 0, 48, ca), self.half2[k][0].at[pl.ds(0, 1)], turn("y", 1, 4)),
            go(self.sub_a(2, 48, 48, ca), self.half2[k][0].at[pl.ds(1, 1)], turn("y", -1, 4)),
        ]
        copies[2].wait_recv()
        copies[3].wait_recv()
        add_into(self.block_b(0, 0, 96, cb), self.full_b[k].at[0], self.full_b[k].at[1])
        sent += [
            go(self.sub_b(2, 0, 48, cb), self.half2[k][1].at[pl.ds(0, 1)], turn("z", 1, 4)),
            go(self.sub_b(2, 48, 48, cb), self.half2[k][1].at[pl.ds(1, 1)], turn("z", -1, 4)),
        ]
        self.copies[k, 3] = sent

    def r2b(self, k):
        go, copies = self.wires.go, self.copies[k, 3]
        sent = []
        for colour, (sub, axis) in enumerate(((self.sub_a, "y"), (self.sub_b, "z"))):
            cols = cols_of(CHUNKS[k][colour])
            half, full = self.half2[k][colour], self.full2[k][colour]
            copies[2 * colour].wait_recv()
            add_into(sub(1, 0, 48, cols), half.at[pl.ds(0, 1)])
            sent.append(go(sub(1, 0, 96, cols), full.at[pl.ds(0, 1)], turn(axis, 1, 4)))
            copies[2 * colour + 1].wait_recv()
            add_into(sub(-1, 48, 48, cols), half.at[pl.ds(1, 1)])
            sent.append(go(sub(-1, 0, 96, cols), full.at[pl.ds(1, 1)], turn(axis, -1, 4)))
        self.copies[k, 4] = sent

    def r3(self, k):
        go, copies = self.wires.go, self.copies[k, 4]
        (a0, an), (b0, bn) = CHUNKS[k]
        for colour, sub in enumerate((self.sub_a, self.sub_b)):
            cols, full = cols_of(CHUNKS[k][colour]), self.full2[k][colour]
            copies[2 * colour].wait_recv()
            copies[2 * colour + 1].wait_recv()
            add_into(sub(0, 0, 96, cols), full.at[pl.ds(0, 1)], full.at[pl.ds(1, 1)])
        part = self.g.at[self.z, rows_of(96 * self.y + 48 * (1 - self.xh), 48), pl.ds(a0, an + bn)]
        self.copies[k, 5] = [go(part, self.last.at[:, pl.ds(a0, an + bn)], turn("xh", 1, 2))]

    def done(self, k):
        (a0, an), (b0, bn) = CHUNKS[k]
        self.copies[k, 5][0].wait_recv()
        cols = pl.ds(a0, an + bn)
        own = self.g[self.z, rows_of(96 * self.y + 48 * self.xh, 48), cols].astype(F32)
        came = self.last[:, cols].astype(F32)
        if k >= 3:
            base = 1536 * (k - 2)
            self.out[:, pl.ds(pl.multiple_of(base + 768 * self.xh, 128), 768)] = own
            self.out[:, pl.ds(pl.multiple_of(base + 768 * (1 - self.xh), 128), 768)] = came
            return
        total = own + came
        if k == 2:
            self.out[:, cols] = total
            return
        for at in range(0, an + bn, 128):
            head, which = (a0 + at) // 384, (a0 + at) % 384 // 128
            self.out[:, pl.ds(384 * which + 128 * head, 128)] = total[:, at : at + 128]


def scatter_buffers():
    shapes = []
    for (_, an), (_, bn) in CHUNKS:
        shapes += [
            pltpu.VMEM((2, 192, an), BF),
            pltpu.VMEM((2, 384, an), BF),
            pltpu.VMEM((2, 4, 48, bn), BF),
            pltpu.VMEM((2, 4, 96, bn), BF),
            pltpu.VMEM((2, 48, an), BF),
            pltpu.VMEM((2, 96, an), BF),
            pltpu.VMEM((2, 48, bn), BF),
            pltpu.VMEM((2, 96, bn), BF),
        ]
    return shapes


def make_scatter(wires, g, bufs, last, out):
    groups = [bufs[8 * k : 8 * k + 8] for k in range(len(CHUNKS))]
    return Scatter(
        wires,
        g,
        [b[0] for b in groups],
        [b[1] for b in groups],
        [b[2] for b in groups],
        [b[3] for b in groups],
        [(b[4], b[6]) for b in groups],
        [(b[5], b[7]) for b in groups],
        last,
        out,
    )


def nn(a, b):
    return jnp.dot(a, b, preferred_element_type=F32)


def nt(a, b):
    return lax.dot_general(a, b, (((1,), (1,)), ((), ())), preferred_element_type=F32)


def tn(a, b):
    return lax.dot_general(a, b, (((0,), (0,)), ((), ())), preferred_element_type=F32)


class Spread:
    def __init__(self, wires, buf):
        self.wires, self.buf = wires, buf
        self.xl, self.c = (lax.axis_index(a) for a in SP)
        self.far, self.near, self.relays = {}, {}, {}

    def block(self, xl, c, start=0, count=128):
        return self.buf.at[rows_of(256 * xl + 128 * c + start, count), :]

    def start(self, i):
        part = self.block(self.xl, self.c, 64 * i, 64)
        self.far[i] = self.wires.go(part, part, turn("xl", 1, 2))
        self.near[i] = self.wires.go(part, part, turn("c", 1, 2))

    def relay(self, i):
        self.far[i].wait_recv()
        part = self.block(1 - self.xl, self.c, 64 * i, 64)
        self.relays[i] = self.wires.go(part, part, turn("c", 1, 2))

    def own_half(self):
        for copy in self.near.values():
            copy.wait_recv()

    def done(self):
        for copy in self.relays.values():
            copy.wait_recv()

    def release(self):
        for group in (self.far, self.near, self.relays):
            for copy in group.values():
                self.wires.sent(copy)


class Collect:
    def __init__(self, wires, part, pair, cross):
        self.wires, self.part, self.pair, self.cross = wires, part, pair, cross
        self.xl, self.c = (lax.axis_index(a) for a in SP)

    def block(self, xl, c):
        return self.part.at[rows_of(256 * xl + 128 * c, 128), :]

    def other(self):
        self.first = self.wires.go(self.block(1 - self.xl, 1 - self.c), self.pair.at[0], turn("c", 1, 2))

    def send(self):
        self.first.wait_recv()
        self.third = []
        for i in range(2):
            rows = pl.ds(64 * i, 64)
            mine = self.block(1 - self.xl, self.c).at[rows, :]
            add2(mine, self.pair.at[0, rows, :])
            self.third.append(self.wires.go(mine, self.cross.at[rows, :], turn("xl", 1, 2)))

    def own(self):
        self.second = self.wires.go(self.block(self.xl, 1 - self.c), self.pair.at[1], turn("c", 1, 2))

    def wait(self, i):
        if i == 0:
            self.second.wait_recv()
        self.third[i].wait_recv()

    def release(self):
        for copy in (self.first, self.second, *self.third):
            self.wires.sent(copy)

    def rows(self, start, count):
        at = rows_of(256 * self.xl + 128 * self.c + start, count)
        total = self.part[at, :].astype(F32) + self.pair[1, pl.ds(start, count), :].astype(F32)
        return total + self.cross[pl.ds(start, count), :].astype(F32)


class RingSpread:
    def __init__(self, wires, buf):
        self.wires, self.buf, self.c = wires, buf, lax.axis_index("c")
        self.sent = {}

    def part(self, step, i):
        xh, xl = chip(step)
        return self.buf.at[rows_of(512 * xh + 256 * xl + 128 * self.c + 64 * i, 64), :]

    def go(self, key, step, i, device):
        self.sent[key] = self.wires.go(self.part(step, i), self.part(step, i), device)

    def start(self, i):
        self.go(("next", i), 0, i, along(1))
        self.go(("prev", i), 0, i, along(-1))
        self.go(("own", i), 0, i, turn("c", 1, 2))

    def side(self, name, step, i):
        self.sent[name, i].wait_recv()
        if (name, i) in (("next", 0), ("prev", 1)):
            self.go(("far", i), step, i, along(-step))
        self.go(("core", step, i), step, i, turn("c", 1, 2))

    def relay(self, i):
        if i == 0:
            self.side("next", -1, 0)
            self.side("prev", 1, 1)
        else:
            self.side("next", -1, 1)
            self.side("prev", 1, 0)

    def relay_far(self):
        for i in range(2):
            self.sent["far", i].wait_recv()
            self.go(("core", 2, i), 2, i, turn("c", 1, 2))

    def own_half(self):
        for i in range(2):
            self.sent["own", i].wait_recv()

    def done(self):
        for step in (1, -1):
            for i in range(2):
                self.sent["core", step, i].wait_recv()

    def done_far(self):
        for i in range(2):
            self.sent["core", 2, i].wait_recv()

    def release(self):
        for copy in self.sent.values():
            self.wires.sent(copy)


class RingCollect:
    def __init__(self, wires, part, pair, half, full):
        self.wires, self.part, self.pair, self.half, self.full = wires, part, pair, half, full
        self.c = lax.axis_index("c")
        self.sent = {}

    def block(self, step, c, start=0, count=128):
        xh, xl = chip(step)
        return self.part.at[rows_of(512 * xh + 256 * xl + 128 * c + start, count), :]

    def give(self, name):
        step = STEPS[name]
        self.sent[name] = self.wires.go(self.block(step, 1 - self.c), self.pair.at[step % 4], turn("c", 1, 2))

    def take(self, name):
        step = STEPS[name]
        self.sent[name].wait_recv()
        if step == 0:
            return
        add2(self.block(step, self.c), self.pair.at[step % 4])
        if step == 2:
            for i, way in enumerate((1, -1)):
                self.sent["half", way] = self.wires.go(
                    self.block(2, self.c, 64 * i, 64), self.half.at[i], along(way)
                )
            return
        i = 1 if step == 1 else 0
        self.sent["early", step] = self.wires.go(
            self.block(step, self.c, 64 * i, 64), self.full.at[1 - i, pl.ds(64 * i, 64), :], along(step)
        )

    def pass_on(self):
        for i, step in enumerate((1, -1)):
            self.sent["half", step].wait_recv()
            block = self.block(step, self.c, 64 * i, 64)
            add2(block, self.half.at[i])
            self.sent["late", step] = self.wires.go(
                block, self.full.at[i, pl.ds(64 * i, 64), :], along(step)
            )

    def wait(self):
        for step in (1, -1):
            self.sent["early", step].wait_recv()
            self.sent["late", step].wait_recv()

    def rows(self, start, count):
        xh, xl = chip(0)
        total = self.part[rows_of(512 * xh + 256 * xl + 128 * self.c + start, count), :].astype(F32)
        for ref in (self.pair.at[0], self.full.at[0], self.full.at[1]):
            total = total + ref[pl.ds(start, count), :].astype(F32)
        return total


def add2(dst, src):
    rows = dst.shape[0]

    @pl.loop(0, rows // 16)
    def _(i):
        at = (pl.ds(pl.multiple_of(i * 16, 16), 16), slice(None))
        dst[at] = (dst[at].astype(F32) + src[at].astype(F32)).astype(dst.dtype)


def normalize(stream):
    mean_part = jnp.mean(stream, axis=-1, keepdims=True)
    centred = stream - mean_part
    rstd = lax.rsqrt(jnp.mean(centred * centred, axis=-1, keepdims=True) + ln_eps)
    return (centred * rstd, rstd)


def norm_back(normed, rstd, incoming):
    first = jnp.mean(incoming, axis=-1, keepdims=True)
    second = jnp.mean(incoming * normed, axis=-1, keepdims=True)
    return rstd * (incoming - first - normed * second)


BLOCK = 16
ROOT = math.sqrt(2.0 / math.pi)


def by_rows(fn, start=0, count=128):
    @pl.loop(start // BLOCK, (start + count) // BLOCK)
    def _(i):
        fn(pl.multiple_of(i * BLOCK, BLOCK))


def block_kernel(
    x_in, m_in, og_in, wq_ref, wo_ref, wi_ref, wb_ref,
    final_out, ig_out, sums_out,
    x_ref, m_ref, og_ref, final_ref, ig_ref, sums_ref,
    w, g, last, stage, a1, dm, a2, da, qkv, o, do, gp, act, part, ring_part, probs, dv, pair, cross,
    pair0, half0, full0, pair1, half1, full1, mid, dmid, send, recv, local_sem, *bufs,
):
    z, y, xh, xl, c = (lax.axis_index(a) for a in FSDP + SP)
    shard_rows = rows_of(96 * y + 48 * xh, 48)
    pieces = [
        (wq_ref.at[which, :, pl.ds(128 * h, 128)], 384 * h + 128 * which, 128)
        for h in range(3)
        for which in range(3)
    ]
    mine = pl.ds(pl.multiple_of(768 * xh, 128), 768)
    theirs = pl.ds(pl.multiple_of(768 * (1 - xh), 128), 768)
    pieces += [(wo_ref, 1152, 384), (wi_ref.at[:, mine], 1536, 768), (wb_ref.at[:, mine], 2304, 768)]
    loads = [
        pltpu.make_async_copy(source, w.at[z, shard_rows, pl.ds(at, count)], local_sem.at[i])
        for i, (source, at, count) in enumerate(pieces)
    ]
    loads += [
        pltpu.make_async_copy(ref.at[:, theirs], stage.at[:, pl.ds(768 * i, 768)], local_sem.at[18 + i])
        for i, ref in enumerate((wi_ref, wb_ref))
    ]
    inputs = [
        pltpu.make_async_copy(a, b, local_sem.at[12 + i])
        for i, (a, b) in enumerate(((x_in, x_ref), (m_in, m_ref), (og_in, og_ref)))
    ]
    outputs = {
        name: pltpu.make_async_copy(a, b, local_sem.at[15 + i])
        for i, (name, a, b) in enumerate(
            (("final", final_ref, final_out), ("ig", ig_ref, ig_out), ("sums", sums_ref, sums_out))
        )
    }
    greet()
    for load in loads[:3] + inputs[:2] + loads[3:] + inputs[2:]:
        load.start()
    wires = Wires(send, recv)
    ag = Gather(wires, w, stage)
    rs = make_scatter(wires, g, bufs, last, sums_ref)
    own_row = 256 * xl + 128 * c
    own_start, other_start = 256 * xl, 256 * (1 - xl)
    scale = 1.0 / math.sqrt(32 * 512)
    factor = temper / math.sqrt(HEAD_DIM)
    steps = {}

    def step(fn):
        steps[fn.__name__] = fn
        return fn

    def mod(i):
        return m_ref[i]

    def own(start):
        return (rows_of(own_row + start, BLOCK), slice(None))

    def ring_own(start):
        return (rows_of(512 * xh + own_row + start, BLOCK), slice(None))

    def weights(start, count):
        return w[:, :, pl.ds(start, count)].reshape(1536, count)

    for k in range(len(CHUNKS)):
        for name in ("s1", "s2", "s2b", "s3", "s3b", "done"):
            steps[f"ag_{name}_{k}"] = functools.partial(getattr(ag, name), k)
        for name in ("r1", "r1b", "r2", "r2b", "r3", "done"):
            steps[f"rs_{name}_{k}"] = functools.partial(getattr(rs, name), k)
    for key, buf in (("a1", a1), ("da", da)):
        spread = Spread(wires, buf)
        for i in range(2):
            steps[f"{key}_start_{i}"] = functools.partial(spread.start, i)
            steps[f"{key}_relay_{i}"] = functools.partial(spread.relay, i)
        steps[f"{key}_own_half"] = spread.own_half
        steps[f"{key}_done"] = spread.done
    for key, buf in (("dm", dm), ("a2", a2)):
        spread = RingSpread(wires, buf)
        for i in range(2):
            steps[f"{key}_start_{i}"] = functools.partial(spread.start, i)
            steps[f"{key}_relay_{i}"] = functools.partial(spread.relay, i)
        for name in ("relay_far", "own_half", "done", "done_far", "release"):
            steps[f"{key}_{name}"] = getattr(spread, name)
    reds = {"att": Collect(wires, part, pair, cross), "da1": Collect(wires, part, pair, cross)}
    for key, red in reds.items():
        for name in ("other", "own", "send", "release"):
            steps[f"{key}_{name}"] = getattr(red, name)
        for i in range(2):
            steps[f"{key}_wait_{i}"] = functools.partial(red.wait, i)
    reds["da2"] = RingCollect(wires, ring_part, pair0, half0, full0)
    reds["ffn"] = RingCollect(wires, dm, pair1, half1, full1)
    for key in ("da2", "ffn"):
        red = reds[key]
        for name in STEPS:
            steps[f"{key}_give_{name}"] = functools.partial(red.give, name)
            steps[f"{key}_take_{name}"] = functools.partial(red.take, name)
        steps[f"{key}_pass_on"] = red.pass_on
        steps[f"{key}_wait"] = red.wait

    @step
    def load_first():
        for load in loads[:3]:
            load.wait()

    steps["met"] = met

    @step
    def load_inputs():
        inputs[0].wait()
        inputs[1].wait()

    @step
    def load_rest():
        for load in loads[3:]:
            load.wait()
        inputs[2].wait()

    def first_norm(r):
        n1, _ = normalize(x_ref[pl.ds(r, BLOCK), :].astype(F32))
        a1[own(r)] = (n1 * (1.0 + mod(1)) + mod(0)).astype(BF)

    def second_norm(r):
        rows = pl.ds(r, BLOCK)
        value = x_ref[rows, :].astype(F32) + mod(2) * reds["att"].rows(r, BLOCK)
        mid[rows, :] = value
        n2, _ = normalize(value)
        a2[ring_own(r)] = (n2 * (1.0 + mod(4)) + mod(3)).astype(BF)

    def mid_grad(r):
        rows = pl.ds(r, BLOCK)
        n2, r2 = normalize(mid[rows, :])
        inner = norm_back(n2, r2, reds["da2"].rows(r, BLOCK) * (1.0 + mod(4)))
        value = og_ref[rows, :].astype(F32) + inner
        dmid[rows, :] = value
        da[own(r)] = (mod(2) * value).astype(BF)

    for i in range(2):
        for fn in (first_norm, second_norm, mid_grad):
            steps[f"{fn.__name__}_{i}"] = functools.partial(by_rows, fn, 64 * i, 64)

    @step
    def gate_grad():
        def rows(r):
            dm[ring_own(r)] = (mod(5) * og_ref[pl.ds(r, BLOCK), :].astype(F32)).astype(BF)

        by_rows(rows)

    def lanes(h, which):
        return pl.ds(384 * h + 128 * which, 128)

    def project(start, count):
        qkv[:, pl.ds(start, count)] = nn(a1[...], weights(start, count)).astype(BF)

    @step
    def project_0():
        project(0, 256)
        project(256, 128)

    @step
    def project_1():
        @pl.loop(0, 3)
        def _(j):
            project(pl.multiple_of(384 + j * 256, 128), 256)

    def attend(heads, start, blocks):
        @pl.loop(0, blocks)
        def _(i):
            rows = rows_of(start + i * 128, 128)
            for h in heads:
                s = nt(qkv[rows, lanes(h, 0)], qkv[:, lanes(h, 1)]) * factor
                e = jnp.exp(s - jnp.max(s, axis=-1, keepdims=True))
                p = (e * (1.0 / jnp.sum(e, axis=-1, keepdims=True))).astype(BF)
                probs[h, rows, :] = p
                o[rows, pl.ds(128 * h, 128)] = nn(p, qkv[:, lanes(h, 2)]).astype(BF)

    steps["attend_0"] = functools.partial(attend, (0,), 0, 4)
    steps["attend_other"] = functools.partial(attend, (1, 2), other_start, 2)
    steps["attend_own"] = functools.partial(attend, (1, 2), own_start, 2)

    def back_half(dst, lhs, start, at, count):
        rows = rows_of(start, 256)

        @pl.loop(0, 2)
        def _(j):
            rhs = w[pl.ds(2 * j, 2), :, pl.ds(at, count)].reshape(768, count)
            dst[rows, pl.ds(pl.multiple_of(768 * j, 128), 768)] = nt(lhs[rows, :], rhs).astype(BF)

    for key, dst, lhs, at, count in (("att", part, o, 1152, 384), ("da1", part, qkv, 0, 1152)):
        steps[f"{key}_mm_other"] = functools.partial(back_half, dst, lhs, other_start, at, count)
        steps[f"{key}_mm_own"] = functools.partial(back_half, dst, lhs, own_start, at, count)

    def quarter(name):
        at_xh, at_xl = chip(STEPS[name])
        return 512 * at_xh + 256 * at_xl

    def hidden(name):
        rows = rows_of(quarter(name), 256)

        @pl.loop(0, 3)
        def _(j):
            at = pl.multiple_of(j * 256, 256)
            u = nn(a2[rows, :], weights(pl.multiple_of(1536 + at, 256), 256))
            sq = u * u
            t = jnp.tanh(ROOT * u * (1.0 + 0.044715 * sq))
            half = 0.5 * (1.0 + t)
            act[rows, pl.ds(at, 256)] = (u * half).astype(BF)
            slope = half + (0.5 * ROOT) * u * (1.0 - t * t) * (1.0 + (3 * 0.044715) * sq)
            gp[rows, pl.ds(at, 256)] = slope.astype(BF)

    def hidden_grad(name):
        rows = rows_of(quarter(name), 256)

        @pl.loop(0, 3)
        def _(j):
            at = pl.multiple_of(j * 256, 256)
            cols = pl.ds(at, 256)
            dg = nn(dm[rows, :], weights(pl.multiple_of(2304 + at, 256), 256))
            gp[rows, cols] = (gp[rows, cols].astype(F32) * dg).astype(BF)

    for name in STEPS:
        steps[f"hidden_{name}"] = functools.partial(hidden, name)
        steps[f"hgrad_{name}"] = functools.partial(hidden_grad, name)
        steps[f"da2_mm_{name}"] = functools.partial(back_half, ring_part, gp, quarter(name), 1536, 768)
        steps[f"ffn_mm_{name}"] = functools.partial(back_half, dm, act, quarter(name), 2304, 768)

    def grad(left, right, right_at, at, count, planes=(0, 4)):
        @pl.loop(*planes)
        def _(j):
            lhs = left[:, pl.ds(pl.multiple_of(384 * j, 128), 384)]
            value = tn(lhs, right[:, pl.ds(right_at, count)]) * scale
            g[j, :, pl.ds(at, count)] = value.astype(BF)

    for i in range(2):
        steps[f"grad_in_{i}"] = functools.partial(grad, a2, gp, 0, 1536, 768, (2 * i, 2 * i + 2))
        steps[f"grad_back_{i}"] = functools.partial(grad, dm, act, 0, 2304, 768, (2 * i, 2 * i + 2))
    steps["grad_out"] = functools.partial(grad, da, o, 0, 1152, 384)
    steps["grad_q_0"] = functools.partial(grad, a1, qkv, 0, 0, 384)
    steps["grad_q_1"] = functools.partial(grad, a1, qkv, 384, 384, 768)

    def head_grads(start):
        rows = rows_of(start, 256)
        do[rows, :] = nn(da[rows, :], weights(1152, 384)).astype(BF)

    steps["heads_own"] = functools.partial(head_grads, own_start)
    steps["heads_other"] = functools.partial(head_grads, other_start)

    def attend_back(heads):
        for n, h in enumerate(heads):
            dv[n] = tn(probs[h], do[:, pl.ds(128 * h, 128)]).astype(BF)

        @pl.loop(0, 4)
        def _(i):
            rows = pl.ds(pl.multiple_of(i * 128, 128), 128)
            for h in heads:
                dp = nt(do[rows, pl.ds(128 * h, 128)], qkv[:, lanes(h, 2)])
                p = probs[h, rows, :].astype(F32)
                ds = factor * p * (dp - jnp.sum(p * dp, axis=-1, keepdims=True))
                probs[h, rows, :] = ds.astype(BF)

        for n, h in enumerate(heads):
            dk = tn(probs[h], qkv[:, lanes(h, 0)]).astype(BF)
            qkv[:, lanes(h, 0)] = nn(probs[h], qkv[:, lanes(h, 1)]).astype(BF)
            qkv[:, lanes(h, 1)] = dk
            qkv[:, lanes(h, 2)] = dv[n]

    steps["attend_back_0"] = functools.partial(attend_back, (0,))
    steps["attend_back_1"] = functools.partial(attend_back, (1, 2))

    @step
    def last_out():
        def each(r):
            rows = pl.ds(r, BLOCK)
            final_ref[rows, :] = (mid[rows, :] + mod(5) * reds["ffn"].rows(r, BLOCK)).astype(BF)

        by_rows(each)
        outputs["final"].start()

    @step
    def first_grad():
        def each(r):
            rows = pl.ds(r, BLOCK)
            n1, r1 = normalize(x_ref[rows, :].astype(F32))
            inner = norm_back(n1, r1, reds["da1"].rows(r, BLOCK) * (1.0 + mod(1)))
            ig_ref[rows, :] = dmid[rows, :] + inner

        by_rows(each)
        outputs["ig"].start()

    @step
    def finish():
        outputs["sums"].start()
        wires.drain()
        for copy in outputs.values():
            copy.wait()

    for name in ORDER:
        with jax.named_scope(name):
            steps[name]()


def finish_kernel(
    final_in, ig_in, sums_in, final_out, ig_out, gq_out, go_out, gi_out, gb_out, final, ig, sums, sem
):
    cuts = [(384 * which, 384, gq_out.at[which]) for which in range(3)]
    cuts += [(1152, 384, go_out), (1536, 1536, gi_out), (3072, 1536, gb_out)]
    pairs = [(sums_in.at[:, pl.ds(at, n)], sums.at[:, pl.ds(at, n)], out) for at, n, out in cuts]
    pairs += [(ig_in, ig, ig_out), (final_in, final, final_out)]
    loads, stores = [], []
    for i, (source, held, out) in enumerate(pairs):
        loads.append(pltpu.make_async_copy(source, held, sem.at[0, i]))
        stores.append(pltpu.make_async_copy(held, out, sem.at[1, i]))
    for load in loads:
        load.start()
    for load, store in zip(loads, stores):
        load.wait()
        store.start()
    for store in stores:
        store.wait()


def body(tokens, modulation, w_qkv, w_out, w_in, w_back, out_grad):
    own = w_qkv.shape[3]
    far = pl.BlockSpec(memory_space=pl.ANY)
    copies = 34 * len(CHUNKS) + 2 * 6 + 2 * 4 + 2 * 14 + 2 * 10
    rows = lambda n, count=512: pltpu.VMEM((count, n), BF)
    final, grad_in_rows, sums = pl.pallas_call(
        block_kernel,
        out_shape=(
            jax.ShapeDtypeStruct((128, 1536), BF),
            jax.ShapeDtypeStruct((128, 1536), F32),
            jax.ShapeDtypeStruct((48, WIDTH), F32),
        ),
        in_specs=[far] * 7,
        out_specs=(far, far, far),
        scratch_shapes=[
            pltpu.VMEM((128, 1536), BF),
            pltpu.VMEM((6, 1, 1536), F32),
            pltpu.VMEM((128, 1536), BF),
            pltpu.VMEM((128, 1536), BF),
            pltpu.VMEM((128, 1536), F32),
            pltpu.VMEM((48, WIDTH), F32),
            pltpu.VMEM((4, 384, HELD), BF),
            pltpu.VMEM((4, 384, HELD), BF),
            pltpu.VMEM((48, HELD), BF),
            pltpu.VMEM((48, 1536), BF),
            rows(1536), rows(1536, 1024), rows(1536, 1024), rows(1536),
            rows(1152), rows(384), rows(384),
            rows(768, 1024), rows(768, 1024), rows(1536), rows(1536, 1024),
            pltpu.VMEM((3, 512, 512), BF),
            pltpu.VMEM((2, 512, 128), BF),
            pltpu.VMEM((2, 128, 1536), BF),
            pltpu.VMEM((128, 1536), BF),
            pltpu.VMEM((4, 128, 1536), BF),
            pltpu.VMEM((2, 64, 1536), BF),
            pltpu.VMEM((2, 128, 1536), BF),
            pltpu.VMEM((4, 128, 1536), BF),
            pltpu.VMEM((2, 64, 1536), BF),
            pltpu.VMEM((2, 128, 1536), BF),
            pltpu.VMEM((128, 1536), F32),
            pltpu.VMEM((128, 1536), F32),
            pltpu.SemaphoreType.DMA((copies,)),
            pltpu.SemaphoreType.DMA((copies,)),
            pltpu.SemaphoreType.DMA((20,)),
            *scatter_buffers(),
        ],
        compiler_params=pltpu.CompilerParams(
            collective_id=0, has_side_effects=True, vmem_limit_bytes=VMEM_LIMIT
        ),
        name="block",
    )(
        tokens[0],
        modulation[0].transpose(1, 0, 2),
        out_grad[0],
        w_qkv[0].transpose(1, 0, 2),
        w_out[0].T,
        w_in[0],
        w_back[0].T,
    )
    outs = pl.pallas_call(
        finish_kernel,
        out_shape=(
            jax.ShapeDtypeStruct((128, 1536), BF),
            jax.ShapeDtypeStruct((128, 1536), F32),
            jax.ShapeDtypeStruct((3, 48, own), F32),
            jax.ShapeDtypeStruct((48, own), F32),
            jax.ShapeDtypeStruct((48, 4 * own), F32),
            jax.ShapeDtypeStruct((48, 4 * own), F32),
        ),
        in_specs=[far] * 3,
        out_specs=(far,) * 6,
        scratch_shapes=[
            pltpu.VMEM((128, 1536), BF),
            pltpu.VMEM((128, 1536), F32),
            pltpu.VMEM((48, WIDTH), F32),
            pltpu.SemaphoreType.DMA((2, 8)),
        ],
        name="finish",
    )(final, grad_in_rows, sums)
    final, grad_in_rows, gq, go, gi, gb = outs
    return (final[None], grad_in_rows[None], gq.transpose(1, 0, 2)[None], go.T[None], gi[None], gb.T[None])


def solution(mesh):
    torus = Mesh(mesh.devices.reshape(4, 4, 2, 2, 2), FSDP + SP)
    return jax.shard_map(
        body,
        mesh=torus,
        in_specs=(
            P(FSDP, SP, None),
            P(FSDP, None, None, None),
            P(None, FSDP, None, SP),
            P(None, SP, FSDP),
            P(None, FSDP, SP),
            P(None, SP, FSDP),
            P(FSDP, SP, None),
        ),
        out_specs=(
            P(FSDP, SP, None),
            P(FSDP, SP, None),
            P(None, FSDP, None, SP),
            P(None, SP, FSDP),
            P(None, FSDP, SP),
            P(None, SP, FSDP),
        ),
        check_vma=False,
    )
```

```python
import functools
import math

import jax
import jax.numpy as jnp
from jax import lax
from jax.experimental import pallas as pl
from jax.experimental.pallas import tpu as pltpu
from jax.sharding import Mesh
from jax.sharding import PartitionSpec as P

HEAD_DIM = 128
MESH = pl.DeviceIdType.MESH
FSDP = ("z", "y", "xh")
SP = ("xl", "c")
BF = jnp.bfloat16
F32 = jnp.float32

ln_eps = 1e-06
temper = 2.5
VMEM_LIMIT = 67_000_000

TILES = ((2, 1), (1, 2), (2, 1), (1, 2), (3, 3), (3, 3))
OUT, IN, BACK = 3, 4, 5


def split_chunks():
    chunks, at = [], 0
    for tiles in TILES:
        parts = []
        for count in tiles:
            parts.append((at, 128 * count))
            at += 128 * count
        chunks.append(tuple(parts))
    return tuple(chunks)


CHUNKS = split_chunks()
HELD = 3072
STEPS = {"own": 0, "next": 1, "prev": -1, "far": 2}
WIDTH = 4608
ORDER = (
    "load_first",
    "load_rest",
    "load_inputs",
    "first_norm_0",
    "gate_grad",
    "met",
    "ag_s1_1",
    "ag_s1_2",
    "ag_s1_0",
    "ag_s1_3",
    "a1_start_0",
    "first_norm_1",
    "ag_s1_5",
    "ag_s2_1",
    "a1_start_1",
    "ag_s2_2",
    "ag_s2_0",
    "ag_s2_3",
    "ag_s2b_1",
    "ag_s2b_2",
    "ag_s2b_0",
    "ag_s2b_3",
    "ag_s3_1",
    "ag_s3_0",
    "ag_s3_2",
    "dm_start_1",
    "a1_relay_0",
    "dm_start_0",
    "a1_relay_1",
    "ag_s1_4",
    "ag_s3b_1",
    "a1_done",
    "ag_s3_3",
    "ag_s3b_0",
    "dm_own_half",
    "a1_own_half",
    "dm_relay_0",
    "ag_s3b_2",
    "ag_done_1",
    "project_1",
    "ag_s3b_3",
    "attend_1_other",
    "ag_s2_4",
    "ag_s2_5",
    "ag_done_0",
    "project_0",
    "attend_0_other",
    "attend_0_own",
    "ag_done_2",
    "project_2",
    "attend_2_other",
    "ag_done_3",
    "att_mm_other",
    "att_other",
    "dm_relay_far",
    "ag_s2b_4",
    "attend_1_own",
    "attend_2_own",
    "att_send",
    "ag_s2b_5",
    "att_mm_own",
    "ag_s3_4",
    "dm_relay_1",
    "att_own",
    "ag_s3_5",
    "att_release",
    "att_wait_0",
    "second_norm_0",
    "a2_start_0",
    "att_wait_1",
    "second_norm_1",
    "ag_s3b_4",
    "a2_start_1",
    "dm_done",
    "dm_release",
    "a2_relay_0",
    "ag_s3b_5",
    "a2_own_half",
    "dm_done_far",
    "a2_relay_1",
    "ag_done_4",
    "hidden_own",
    "a2_done",
    "hidden_next",
    "hidden_prev",
    "a2_relay_far",
    "ag_done_5",
    "hgrad_own",
    "hgrad_next",
    "a2_done_far",
    "hidden_far",
    "hgrad_far",
    "da2_mm_far",
    "da2_give_far",
    "hgrad_prev",
    "da2_mm_prev",
    "da2_give_prev",
    "da2_take_far",
    "grad_back_0",
    "da2_mm_next",
    "da2_give_next",
    "grad_back_1",
    "rs_r1_5",
    "da2_take_prev",
    "da2_take_next",
    "grad_in_0",
    "grad_in_1",
    "rs_r1_4",
    "da2_pass_on",
    "da2_mm_own",
    "ffn_mm_own",
    "ffn_mm_prev",
    "ffn_give_prev",
    "rs_r1b_5",
    "ffn_mm_far",
    "ffn_mm_next",
    "da2_give_own",
    "rs_r1b_4",
    "da2_take_own",
    "da2_wait",
    "mid_grad_0",
    "da_start_0",
    "mid_grad_1",
    "da_start_1",
    "ffn_take_prev",
    "ffn_give_next",
    "ffn_give_far",
    "rs_r2_5",
    "da_own_half",
    "da_relay_0",
    "ffn_give_own",
    "rs_r2_4",
    "da_relay_1",
    "ffn_take_next",
    "heads_own",
    "rs_r2b_5",
    "da_done",
    "grad_out",
    "rs_r1_3",
    "heads_other",
    "rs_r2b_4",
    "attend_back_0",
    "grad_q_0",
    "rs_r1_0",
    "ffn_take_far",
    "attend_back_2",
    "ffn_take_own",
    "rs_r1b_3",
    "grad_q_2",
    "rs_r1_2",
    "rs_r3_5",
    "attend_back_1",
    "grad_q_1",
    "da1_mm_other",
    "da1_other",
    "rs_r3_4",
    "rs_r1_1",
    "rs_r1b_0",
    "da1_mm_own",
    "da1_send",
    "rs_r1b_2",
    "rs_done_5",
    "ffn_pass_on",
    "rs_r1b_1",
    "rs_r2_0",
    "da1_own",
    "rs_r2_2",
    "da1_wait_0",
    "rs_r2_3",
    "rs_r2_1",
    "rs_r2b_0",
    "rs_r2b_3",
    "rs_r2b_2",
    "rs_done_4",
    "rs_r2b_1",
    "rs_r3_0",
    "da1_wait_1",
    "rs_r3_3",
    "first_grad",
    "rs_r3_2",
    "ffn_wait",
    "last_out",
    "rs_r3_1",
    "rs_done_2",
    "rs_done_3",
    "rs_done_0",
    "rs_done_1",
    "finish",
)


def turn(axis, step, size):
    return {axis: lax.rem(lax.axis_index(axis) + step + size, size)}


def near(axis, step):
    return lax.rem(lax.axis_index(axis) + step + 4, 4)


class Wires:
    def __init__(self, send, recv):
        self.send, self.recv, self.used, self.open = send, recv, 0, []

    def go(self, src, dst, device):
        at = self.used
        self.used += 1
        copy = pltpu.make_async_remote_copy(
            src_ref=src,
            dst_ref=dst,
            send_sem=self.send.at[at],
            recv_sem=self.recv.at[at],
            device_id=device,
            device_id_type=MESH,
        )
        copy.start()
        self.open.append(copy)
        return copy

    def sent(self, copy):
        copy.wait_send()
        self.open = [other for other in self.open if other is not copy]

    def drain(self):
        for copy in self.open:
            copy.wait_send()
        self.open = []


def chip(step):
    xh, xl = lax.axis_index("xh"), lax.axis_index("xl")
    if step == 0:
        return xh, xl
    if step == 2:
        return 1 - xh, xl
    return lax.rem(xh + xl + (0 if step == 1 else 1), 2), 1 - xl


def along(step):
    xh, xl = chip(step)
    return {"xh": xh, "xl": xl}


def partners():
    return [turn("z", 1, 4), turn("z", -1, 4), turn("y", 1, 4), turn("y", -1, 4)] + [
        turn("xh", 1, 2), turn("c", 1, 2), along(1), along(-1)
    ]


def greet():
    for device in partners():
        pl.semaphore_signal(
            pltpu.get_barrier_semaphore(), inc=1, device_id=device, device_id_type=MESH
        )


def met():
    pl.semaphore_wait(pltpu.get_barrier_semaphore(), len(partners()))


def rows_of(start, count):
    return pl.ds(pl.multiple_of(start, 16), count)


def cols_of(cols):
    return pl.ds(cols[0], cols[1])


class Gather:
    def __init__(self, wires, w, stage):
        self.wires, self.w, self.stage = wires, w, stage
        self.z, self.y, self.xh = (lax.axis_index(a) for a in FSDP)
        self.one, self.two, self.relay2, self.three, self.relay3 = {}, {}, {}, {}, {}

    def same(self, part, device):
        return self.wires.go(part, part, device)

    def s1(self, k):
        (a0, an), (b0, bn) = CHUNKS[k]
        part = self.w.at[self.z, rows_of(96 * self.y + 48 * self.xh, 48), pl.ds(a0, an + bn)]
        source = part if k < IN else self.stage.at[:, pl.ds(a0 - 1536, an + bn)]
        self.one[k] = self.wires.go(source, part, turn("xh", 1, 2))

    def s2(self, k):
        self.one[k].wait_recv()
        ca, cb = map(cols_of, CHUNKS[k])
        pa = self.w.at[self.z, rows_of(96 * self.y, 96), ca]
        pb = self.w.at[self.z, rows_of(96 * self.y, 96), cb]
        self.two[k] = [
            self.same(pa, turn("y", 1, 4)),
            self.same(pa, turn("y", -1, 4)),
            self.same(pb, turn("z", 1, 4)),
            self.same(pb, turn("z", -1, 4)),
        ]

    def s2b(self, k):
        ca, cb = map(cols_of, CHUNKS[k])
        for copy in self.two[k]:
            copy.wait_recv()
        w, z, y = self.w, self.z, self.y
        self.relay2[k] = [
            self.same(w.at[z, rows_of(96 * near("y", -1), 48), ca], turn("y", 1, 4)),
            self.same(w.at[z, rows_of(96 * near("y", 1) + 48, 48), ca], turn("y", -1, 4)),
            self.same(w.at[near("z", -1), rows_of(96 * y, 48), cb], turn("z", 1, 4)),
            self.same(w.at[near("z", 1), rows_of(96 * y + 48, 48), cb], turn("z", -1, 4)),
        ]

    def s3(self, k):
        ca, cb = map(cols_of, CHUNKS[k])
        for copy in self.relay2[k]:
            copy.wait_recv()
        pa = self.w.at[self.z, :, ca]
        pb = self.w.at[:, rows_of(96 * self.y, 96), cb]
        self.three[k] = [
            self.same(pa, turn("z", 1, 4)),
            self.same(pa, turn("z", -1, 4)),
            self.same(pb, turn("y", 1, 4)),
            self.same(pb, turn("y", -1, 4)),
        ]

    def s3b(self, k):
        ca, cb = map(cols_of, CHUNKS[k])
        for copy in self.three[k]:
            copy.wait_recv()
        w = self.w
        self.relay3[k] = [
            self.same(w.at[near("z", -1), pl.ds(0, 192), ca], turn("z", 1, 4)),
            self.same(w.at[near("z", 1), pl.ds(192, 192), ca], turn("z", -1, 4)),
            self.same(w.at[:, rows_of(96 * near("y", -1), 48), cb], turn("y", 1, 4)),
            self.same(w.at[:, rows_of(96 * near("y", 1) + 48, 48), cb], turn("y", -1, 4)),
        ]

    def done(self, k):
        for copy in self.relay3[k]:
            copy.wait_recv()


def add_into(dst, *srcs):
    planes, rows, columns = dst.shape

    @pl.loop(0, planes * (rows // 48))
    def _(i):
        at = (i // (rows // 48), pl.ds(pl.multiple_of((i % (rows // 48)) * 48, 48), 48), slice(None))
        total = dst[at].astype(F32)
        for src in srcs:
            total = total + src[at].astype(F32)
        dst[at] = total.astype(dst.dtype)


class Scatter:
    def __init__(self, wires, g, half_a, full_a, half_b, full_b, half2, full2, last, out):
        self.wires, self.g, self.out = wires, g, out
        self.half_a, self.full_a, self.half_b, self.full_b = half_a, full_a, half_b, full_b
        self.half2, self.full2, self.last = half2, full2, last
        self.z, self.y, self.xh = (lax.axis_index(a) for a in FSDP)
        self.copies = {}

    def block_a(self, step, start, count, cols):
        return self.g.at[pl.ds(near("z", step), 1), pl.ds(start, count), cols]

    def block_b(self, step, start, count, cols):
        return self.g.at[:, rows_of(96 * near("y", step) + start, count), cols]

    def sub_a(self, step, start, count, cols):
        return self.g.at[pl.ds(self.z, 1), rows_of(96 * near("y", step) + start, count), cols]

    def sub_b(self, step, start, count, cols):
        return self.g.at[pl.ds(near("z", step), 1), rows_of(96 * self.y + start, count), cols]

    def r1(self, k):
        ca, cb = map(cols_of, CHUNKS[k])
        go = self.wires.go
        self.copies[k, 1] = [
            go(self.block_a(2, 0, 192, ca), self.half_a[k].at[pl.ds(0, 1)], turn("z", 1, 4)),
            go(self.block_a(2, 192, 192, ca), self.half_a[k].at[pl.ds(1, 1)], turn("z", -1, 4)),
            go(self.block_b(2, 0, 48, cb), self.half_b[k].at[0], turn("y", 1, 4)),
            go(self.block_b(2, 48, 48, cb), self.half_b[k].at[1], turn("y", -1, 4)),
        ]

    def r1b(self, k):
        ca, cb = map(cols_of, CHUNKS[k])
        go, copies = self.wires.go, self.copies[k, 1]
        sent = []
        copies[0].wait_recv()
        add_into(self.block_a(1, 0, 192, ca), self.half_a[k].at[pl.ds(0, 1)])
        sent.append(go(self.block_a(1, 0, 384, ca), self.full_a[k].at[pl.ds(0, 1)], turn("z", 1, 4)))
        copies[1].wait_recv()
        add_into(self.block_a(-1, 192, 192, ca), self.half_a[k].at[pl.ds(1, 1)])
        sent.append(go(self.block_a(-1, 0, 384, ca), self.full_a[k].at[pl.ds(1, 1)], turn("z", -1, 4)))
        copies[2].wait_recv()
        add_into(self.block_b(1, 0, 48, cb), self.half_b[k].at[0])
        sent.append(go(self.block_b(1, 0, 96, cb), self.full_b[k].at[0], turn("y", 1, 4)))
        copies[3].wait_recv()
        add_into(self.block_b(-1, 48, 48, cb), self.half_b[k].at[1])
        sent.append(go(self.block_b(-1, 0, 96, cb), self.full_b[k].at[1], turn("y", -1, 4)))
        self.copies[k, 2] = sent

    def r2(self, k):
        ca, cb = map(cols_of, CHUNKS[k])
        go, copies = self.wires.go, self.copies[k, 2]
        copies[0].wait_recv()
        copies[1].wait_recv()
        add_into(
            self.block_a(0, 0, 384, ca), self.full_a[k].at[pl.ds(0, 1)], self.full_a[k].at[pl.ds(1, 1)]
        )
        sent = [
            go(self.sub_a(2, 0, 48, ca), self.half2[k][0].at[pl.ds(0, 1)], turn("y", 1, 4)),
            go(self.sub_a(2, 48, 48, ca), self.half2[k][0].at[pl.ds(1, 1)], turn("y", -1, 4)),
        ]
        copies[2].wait_recv()
        copies[3].wait_recv()
        add_into(self.block_b(0, 0, 96, cb), self.full_b[k].at[0], self.full_b[k].at[1])
        sent += [
            go(self.sub_b(2, 0, 48, cb), self.half2[k][1].at[pl.ds(0, 1)], turn("z", 1, 4)),
            go(self.sub_b(2, 48, 48, cb), self.half2[k][1].at[pl.ds(1, 1)], turn("z", -1, 4)),
        ]
        self.copies[k, 3] = sent

    def r2b(self, k):
        go, copies = self.wires.go, self.copies[k, 3]
        sent = []
        for colour, (sub, axis) in enumerate(((self.sub_a, "y"), (self.sub_b, "z"))):
            cols = cols_of(CHUNKS[k][colour])
            half, full = self.half2[k][colour], self.full2[k][colour]
            copies[2 * colour].wait_recv()
            add_into(sub(1, 0, 48, cols), half.at[pl.ds(0, 1)])
            sent.append(go(sub(1, 0, 96, cols), full.at[pl.ds(0, 1)], turn(axis, 1, 4)))
            copies[2 * colour + 1].wait_recv()
            add_into(sub(-1, 48, 48, cols), half.at[pl.ds(1, 1)])
            sent.append(go(sub(-1, 0, 96, cols), full.at[pl.ds(1, 1)], turn(axis, -1, 4)))
        self.copies[k, 4] = sent

    def r3(self, k):
        go, copies = self.wires.go, self.copies[k, 4]
        (a0, an), (b0, bn) = CHUNKS[k]
        for colour, sub in enumerate((self.sub_a, self.sub_b)):
            cols, full = cols_of(CHUNKS[k][colour]), self.full2[k][colour]
            copies[2 * colour].wait_recv()
            copies[2 * colour + 1].wait_recv()
            add_into(sub(0, 0, 96, cols), full.at[pl.ds(0, 1)], full.at[pl.ds(1, 1)])
        part = self.g.at[self.z, rows_of(96 * self.y + 48 * (1 - self.xh), 48), pl.ds(a0, an + bn)]
        self.copies[k, 5] = [go(part, self.last.at[:, pl.ds(a0, an + bn)], turn("xh", 1, 2))]

    def done(self, k):
        (a0, an), (b0, bn) = CHUNKS[k]
        self.copies[k, 5][0].wait_recv()
        cols = pl.ds(a0, an + bn)
        own = self.g[self.z, rows_of(96 * self.y + 48 * self.xh, 48), cols].astype(F32)
        came = self.last[:, cols].astype(F32)
        if k >= IN:
            base = 1536 * (k - OUT)
            self.out[:, pl.ds(pl.multiple_of(base + 768 * self.xh, 128), 768)] = own
            self.out[:, pl.ds(pl.multiple_of(base + 768 * (1 - self.xh), 128), 768)] = came
            return
        total = own + came
        if k == OUT:
            self.out[:, cols] = total
            return
        for at in range(0, an + bn, 128):
            head, which = (a0 + at) // 384, (a0 + at) % 384 // 128
            self.out[:, pl.ds(384 * which + 128 * head, 128)] = total[:, at : at + 128]


def scatter_buffers():
    shapes = []
    for (_, an), (_, bn) in CHUNKS:
        shapes += [
            pltpu.VMEM((2, 192, an), BF),
            pltpu.VMEM((2, 384, an), BF),
            pltpu.VMEM((2, 4, 48, bn), BF),
            pltpu.VMEM((2, 4, 96, bn), BF),
            pltpu.VMEM((2, 48, an), BF),
            pltpu.VMEM((2, 96, an), BF),
            pltpu.VMEM((2, 48, bn), BF),
            pltpu.VMEM((2, 96, bn), BF),
        ]
    return shapes


def make_scatter(wires, g, bufs, last, out):
    groups = [bufs[8 * k : 8 * k + 8] for k in range(len(CHUNKS))]
    return Scatter(
        wires,
        g,
        [b[0] for b in groups],
        [b[1] for b in groups],
        [b[2] for b in groups],
        [b[3] for b in groups],
        [(b[4], b[6]) for b in groups],
        [(b[5], b[7]) for b in groups],
        last,
        out,
    )


def nn(a, b):
    return jnp.dot(a, b, preferred_element_type=F32)


def nt(a, b):
    return lax.dot_general(a, b, (((1,), (1,)), ((), ())), preferred_element_type=F32)


def tn(a, b):
    return lax.dot_general(a, b, (((0,), (0,)), ((), ())), preferred_element_type=F32)


class Spread:
    def __init__(self, wires, buf):
        self.wires, self.buf = wires, buf
        self.xl, self.c = (lax.axis_index(a) for a in SP)
        self.far, self.near, self.relays = {}, {}, {}

    def block(self, xl, c, start=0, count=128):
        return self.buf.at[rows_of(256 * xl + 128 * c + start, count), :]

    def start(self, i):
        part = self.block(self.xl, self.c, 64 * i, 64)
        self.far[i] = self.wires.go(part, part, turn("xl", 1, 2))
        self.near[i] = self.wires.go(part, part, turn("c", 1, 2))

    def relay(self, i):
        self.far[i].wait_recv()
        part = self.block(1 - self.xl, self.c, 64 * i, 64)
        self.relays[i] = self.wires.go(part, part, turn("c", 1, 2))

    def own_half(self):
        for copy in self.near.values():
            copy.wait_recv()

    def done(self):
        for copy in self.relays.values():
            copy.wait_recv()

    def release(self):
        for group in (self.far, self.near, self.relays):
            for copy in group.values():
                self.wires.sent(copy)


class Collect:
    def __init__(self, wires, part, pair, cross):
        self.wires, self.part, self.pair, self.cross = wires, part, pair, cross
        self.xl, self.c = (lax.axis_index(a) for a in SP)

    def block(self, xl, c):
        return self.part.at[rows_of(256 * xl + 128 * c, 128), :]

    def other(self):
        self.first = self.wires.go(self.block(1 - self.xl, 1 - self.c), self.pair.at[0], turn("c", 1, 2))

    def send(self):
        self.first.wait_recv()
        self.third = []
        for i in range(2):
            rows = pl.ds(64 * i, 64)
            mine = self.block(1 - self.xl, self.c).at[rows, :]
            add2(mine, self.pair.at[0, rows, :])
            self.third.append(self.wires.go(mine, self.cross.at[rows, :], turn("xl", 1, 2)))

    def own(self):
        self.second = self.wires.go(self.block(self.xl, 1 - self.c), self.pair.at[1], turn("c", 1, 2))

    def wait(self, i):
        if i == 0:
            self.second.wait_recv()
        self.third[i].wait_recv()

    def release(self):
        for copy in (self.first, self.second, *self.third):
            self.wires.sent(copy)

    def rows(self, start, count):
        at = rows_of(256 * self.xl + 128 * self.c + start, count)
        total = self.part[at, :].astype(F32) + self.pair[1, pl.ds(start, count), :].astype(F32)
        return total + self.cross[pl.ds(start, count), :].astype(F32)


class RingSpread:
    def __init__(self, wires, buf):
        self.wires, self.buf, self.c = wires, buf, lax.axis_index("c")
        self.sent = {}

    def part(self, step, i):
        xh, xl = chip(step)
        return self.buf.at[rows_of(512 * xh + 256 * xl + 128 * self.c + 64 * i, 64), :]

    def go(self, key, step, i, device):
        self.sent[key] = self.wires.go(self.part(step, i), self.part(step, i), device)

    def start(self, i):
        self.go(("next", i), 0, i, along(1))
        self.go(("prev", i), 0, i, along(-1))
        self.go(("own", i), 0, i, turn("c", 1, 2))

    def side(self, name, step, i):
        self.sent[name, i].wait_recv()
        if (name, i) in (("next", 0), ("prev", 1)):
            self.go(("far", i), step, i, along(-step))
        self.go(("core", step, i), step, i, turn("c", 1, 2))

    def relay(self, i):
        if i == 0:
            self.side("next", -1, 0)
            self.side("prev", 1, 1)
        else:
            self.side("next", -1, 1)
            self.side("prev", 1, 0)

    def relay_far(self):
        for i in range(2):
            self.sent["far", i].wait_recv()
            self.go(("core", 2, i), 2, i, turn("c", 1, 2))

    def own_half(self):
        for i in range(2):
            self.sent["own", i].wait_recv()

    def done(self):
        for step in (1, -1):
            for i in range(2):
                self.sent["core", step, i].wait_recv()

    def done_far(self):
        for i in range(2):
            self.sent["core", 2, i].wait_recv()

    def release(self):
        for copy in self.sent.values():
            self.wires.sent(copy)


class RingCollect:
    def __init__(self, wires, part, pair, half, full):
        self.wires, self.part, self.pair, self.half, self.full = wires, part, pair, half, full
        self.c = lax.axis_index("c")
        self.sent = {}

    def block(self, step, c, start=0, count=128):
        xh, xl = chip(step)
        return self.part.at[rows_of(512 * xh + 256 * xl + 128 * c + start, count), :]

    def give(self, name):
        step = STEPS[name]
        self.sent[name] = self.wires.go(self.block(step, 1 - self.c), self.pair.at[step % 4], turn("c", 1, 2))

    def take(self, name):
        step = STEPS[name]
        self.sent[name].wait_recv()
        if step == 0:
            return
        add2(self.block(step, self.c), self.pair.at[step % 4])
        if step == 2:
            for i, way in enumerate((1, -1)):
                self.sent["half", way] = self.wires.go(
                    self.block(2, self.c, 64 * i, 64), self.half.at[i], along(way)
                )
            return
        i = 1 if step == 1 else 0
        self.sent["early", step] = self.wires.go(
            self.block(step, self.c, 64 * i, 64), self.full.at[1 - i, pl.ds(64 * i, 64), :], along(step)
        )

    def pass_on(self):
        for i, step in enumerate((1, -1)):
            self.sent["half", step].wait_recv()
            block = self.block(step, self.c, 64 * i, 64)
            add2(block, self.half.at[i])
            self.sent["late", step] = self.wires.go(
                block, self.full.at[i, pl.ds(64 * i, 64), :], along(step)
            )

    def wait(self):
        for step in (1, -1):
            self.sent["early", step].wait_recv()
            self.sent["late", step].wait_recv()

    def rows(self, start, count):
        xh, xl = chip(0)
        total = self.part[rows_of(512 * xh + 256 * xl + 128 * self.c + start, count), :].astype(F32)
        for ref in (self.pair.at[0], self.full.at[0], self.full.at[1]):
            total = total + ref[pl.ds(start, count), :].astype(F32)
        return total


def add2(dst, src):
    rows = dst.shape[0]

    @pl.loop(0, rows // 16)
    def _(i):
        at = (pl.ds(pl.multiple_of(i * 16, 16), 16), slice(None))
        dst[at] = (dst[at].astype(F32) + src[at].astype(F32)).astype(dst.dtype)


def normalize(stream):
    mean_part = jnp.mean(stream, axis=-1, keepdims=True)
    centred = stream - mean_part
    rstd = lax.rsqrt(jnp.mean(centred * centred, axis=-1, keepdims=True) + ln_eps)
    return (centred * rstd, rstd)


def norm_back(normed, rstd, incoming):
    first = jnp.mean(incoming, axis=-1, keepdims=True)
    second = jnp.mean(incoming * normed, axis=-1, keepdims=True)
    return rstd * (incoming - first - normed * second)


BLOCK = 16
ROOT = math.sqrt(2.0 / math.pi)


def by_rows(fn, start=0, count=128):
    for r in range(start, start + count, BLOCK):
        fn(r)


def block_kernel(
    x_in, m_in, og_in, wq_ref, wo_ref, wi_ref, wb_ref,
    final_out, ig_out, sums_out,
    x_ref, m_ref, og_ref, final_ref, ig_ref, sums_ref,
    w, g, last, stage, a1, dm, a2, da, qkv, o, do, gp, act, part, ring_part, probs, dv, pair, cross,
    pair0, half0, full0, pair1, half1, full1, mid, dmid, send, recv, local_sem, *bufs,
):
    z, y, xh, xl, c = (lax.axis_index(a) for a in FSDP + SP)
    shard_rows = rows_of(96 * y + 48 * xh, 48)
    pieces = [
        (wq_ref.at[which, :, pl.ds(128 * h, 128)], 384 * h + 128 * which, 128)
        for h in range(3)
        for which in range(3)
    ]
    mine = pl.ds(pl.multiple_of(768 * xh, 128), 768)
    theirs = pl.ds(pl.multiple_of(768 * (1 - xh), 128), 768)
    pieces += [(wo_ref, 1152, 384), (wi_ref.at[:, mine], 1536, 768), (wb_ref.at[:, mine], 2304, 768)]
    loads = [
        pltpu.make_async_copy(source, w.at[z, shard_rows, pl.ds(at, count)], local_sem.at[i])
        for i, (source, at, count) in enumerate(pieces)
    ]
    loads += [
        pltpu.make_async_copy(ref.at[:, theirs], stage.at[:, pl.ds(768 * i, 768)], local_sem.at[18 + i])
        for i, ref in enumerate((wi_ref, wb_ref))
    ]
    inputs = [
        pltpu.make_async_copy(a, b, local_sem.at[12 + i])
        for i, (a, b) in enumerate(((x_in, x_ref), (m_in, m_ref), (og_in, og_ref)))
    ]
    outputs = {
        name: pltpu.make_async_copy(a, b, local_sem.at[15 + i])
        for i, (name, a, b) in enumerate(
            (("final", final_ref, final_out), ("ig", ig_ref, ig_out), ("sums", sums_ref, sums_out))
        )
    }
    greet()
    for load in loads[:3] + inputs[:2] + loads[3:] + inputs[2:]:
        load.start()
    wires = Wires(send, recv)
    ag = Gather(wires, w, stage)
    rs = make_scatter(wires, g, bufs, last, sums_ref)
    own_row = 256 * xl + 128 * c
    own_start, other_start = 256 * xl, 256 * (1 - xl)
    scale = 1.0 / math.sqrt(32 * 512)
    factor = temper / math.sqrt(HEAD_DIM)
    steps = {}

    def step(fn):
        steps[fn.__name__] = fn
        return fn

    def mod(i):
        return m_ref[i]

    def own(start):
        return (rows_of(own_row + start, BLOCK), slice(None))

    def ring_own(start):
        return (rows_of(512 * xh + own_row + start, BLOCK), slice(None))

    def weights(start, count):
        return w[:, :, pl.ds(start, count)].reshape(1536, count)

    for k in range(len(CHUNKS)):
        for name in ("s1", "s2", "s2b", "s3", "s3b", "done"):
            steps[f"ag_{name}_{k}"] = functools.partial(getattr(ag, name), k)
        for name in ("r1", "r1b", "r2", "r2b", "r3", "done"):
            steps[f"rs_{name}_{k}"] = functools.partial(getattr(rs, name), k)
    for key, buf in (("a1", a1), ("da", da)):
        spread = Spread(wires, buf)
        for i in range(2):
            steps[f"{key}_start_{i}"] = functools.partial(spread.start, i)
            steps[f"{key}_relay_{i}"] = functools.partial(spread.relay, i)
        steps[f"{key}_own_half"] = spread.own_half
        steps[f"{key}_done"] = spread.done
    for key, buf in (("dm", dm), ("a2", a2)):
        spread = RingSpread(wires, buf)
        for i in range(2):
            steps[f"{key}_start_{i}"] = functools.partial(spread.start, i)
            steps[f"{key}_relay_{i}"] = functools.partial(spread.relay, i)
        for name in ("relay_far", "own_half", "done", "done_far", "release"):
            steps[f"{key}_{name}"] = getattr(spread, name)
    reds = {"att": Collect(wires, part, pair, cross), "da1": Collect(wires, part, pair, cross)}
    for key, red in reds.items():
        for name in ("other", "own", "send", "release"):
            steps[f"{key}_{name}"] = getattr(red, name)
        for i in range(2):
            steps[f"{key}_wait_{i}"] = functools.partial(red.wait, i)
    reds["da2"] = RingCollect(wires, ring_part, pair0, half0, full0)
    reds["ffn"] = RingCollect(wires, dm, pair1, half1, full1)
    for key in ("da2", "ffn"):
        red = reds[key]
        for name in STEPS:
            steps[f"{key}_give_{name}"] = functools.partial(red.give, name)
            steps[f"{key}_take_{name}"] = functools.partial(red.take, name)
        steps[f"{key}_pass_on"] = red.pass_on
        steps[f"{key}_wait"] = red.wait

    @step
    def load_first():
        for load in loads[:3]:
            load.wait()

    steps["met"] = met

    @step
    def load_inputs():
        inputs[0].wait()
        inputs[1].wait()

    @step
    def load_rest():
        for load in loads[3:]:
            load.wait()
        inputs[2].wait()

    def first_norm(r):
        n1, _ = normalize(x_ref[pl.ds(r, BLOCK), :].astype(F32))
        a1[own(r)] = (n1 * (1.0 + mod(1)) + mod(0)).astype(BF)

    def second_norm(r):
        rows = pl.ds(r, BLOCK)
        value = x_ref[rows, :].astype(F32) + mod(2) * reds["att"].rows(r, BLOCK)
        mid[rows, :] = value
        n2, _ = normalize(value)
        a2[ring_own(r)] = (n2 * (1.0 + mod(4)) + mod(3)).astype(BF)

    def mid_grad(r):
        rows = pl.ds(r, BLOCK)
        n2, r2 = normalize(mid[rows, :])
        inner = norm_back(n2, r2, reds["da2"].rows(r, BLOCK) * (1.0 + mod(4)))
        value = og_ref[rows, :].astype(F32) + inner
        dmid[rows, :] = value
        da[own(r)] = (mod(2) * value).astype(BF)

    for i in range(2):
        for fn in (first_norm, second_norm, mid_grad):
            steps[f"{fn.__name__}_{i}"] = functools.partial(by_rows, fn, 64 * i, 64)

    @step
    def gate_grad():
        def rows(r):
            dm[ring_own(r)] = (mod(5) * og_ref[pl.ds(r, BLOCK), :].astype(F32)).astype(BF)

        by_rows(rows)

    def lanes(h, which):
        return pl.ds(384 * h + 128 * which, 128)

    def project(start, count):
        qkv[:, pl.ds(start, count)] = nn(a1[...], weights(start, count)).astype(BF)

    for h in range(3):

        def project_head(h=h):
            project(384 * h, 384)

        steps[f"project_{h}"] = project_head

    def attend(h, start):
        rows = rows_of(start, 256)
        s = nt(qkv[rows, lanes(h, 0)], qkv[:, lanes(h, 1)])
        e = jnp.exp(factor * (s - jnp.max(s, axis=-1, keepdims=True)))
        p = (e * (1.0 / jnp.sum(e, axis=-1, keepdims=True))).astype(BF)
        probs[h, rows, :] = p
        o[rows, pl.ds(128 * h, 128)] = nn(p, qkv[:, lanes(h, 2)]).astype(BF)

    for h in range(3):
        steps[f"attend_{h}_other"] = functools.partial(attend, h, other_start)
        steps[f"attend_{h}_own"] = functools.partial(attend, h, own_start)

    def back_half(dst, lhs, start, at, count):
        rows = rows_of(start, 256)

        for j in range(2):
            rhs = w[2 * j : 2 * j + 2, :, pl.ds(at, count)].reshape(768, count)
            dst[rows, pl.ds(768 * j, 768)] = nt(lhs[rows, :], rhs).astype(BF)

    for key, dst, lhs, at, count in (("att", part, o, 1152, 384), ("da1", part, qkv, 0, 1152)):
        steps[f"{key}_mm_other"] = functools.partial(back_half, dst, lhs, other_start, at, count)
        steps[f"{key}_mm_own"] = functools.partial(back_half, dst, lhs, own_start, at, count)

    def quarter(name):
        at_xh, at_xl = chip(STEPS[name])
        return 512 * at_xh + 256 * at_xl

    def hidden(name):
        rows = rows_of(quarter(name), 256)

        for at in range(0, 768, 256):
            u = nn(a2[rows, :], weights(1536 + at, 256))
            sq = u * u
            t = jnp.tanh(u * (ROOT + (ROOT * 0.044715) * sq))
            half = 0.5 + 0.5 * t
            act[rows, pl.ds(at, 256)] = (u * half).astype(BF)
            inner = (0.5 * ROOT) + (1.5 * ROOT * 0.044715) * sq
            gp[rows, pl.ds(at, 256)] = (half + u * inner * (1.0 - t * t)).astype(BF)

    def hidden_grad(name):
        rows = rows_of(quarter(name), 256)

        for at in range(0, 768, 256):
            cols = pl.ds(at, 256)
            dg = nn(dm[rows, :], weights(2304 + at, 256))
            gp[rows, cols] = (gp[rows, cols].astype(F32) * dg).astype(BF)

    for name in STEPS:
        steps[f"hidden_{name}"] = functools.partial(hidden, name)
        steps[f"hgrad_{name}"] = functools.partial(hidden_grad, name)
        steps[f"da2_mm_{name}"] = functools.partial(back_half, ring_part, gp, quarter(name), 1536, 768)
        steps[f"ffn_mm_{name}"] = functools.partial(back_half, dm, act, quarter(name), 2304, 768)

    def grad(left, right, right_at, at, count, planes=(0, 4)):
        for j in range(*planes):
            lhs = left[:, pl.ds(384 * j, 384)]
            value = tn(lhs, right[:, pl.ds(right_at, count)]) * scale
            g[j, :, pl.ds(at, count)] = value.astype(BF)

    for i in range(2):
        steps[f"grad_in_{i}"] = functools.partial(grad, a2, gp, 0, 1536, 768, (2 * i, 2 * i + 2))
        steps[f"grad_back_{i}"] = functools.partial(grad, dm, act, 0, 2304, 768, (2 * i, 2 * i + 2))
    steps["grad_out"] = functools.partial(grad, da, o, 0, 1152, 384)
    for h in range(3):
        steps[f"grad_q_{h}"] = functools.partial(grad, a1, qkv, 384 * h, 384 * h, 384)

    def head_grads(start):
        rows = rows_of(start, 256)
        do[rows, :] = nn(da[rows, :], weights(1152, 384)).astype(BF)

    steps["heads_own"] = functools.partial(head_grads, own_start)
    steps["heads_other"] = functools.partial(head_grads, other_start)

    def attend_back(h):
        dv[...] = tn(probs[h], do[:, pl.ds(128 * h, 128)]).astype(BF)
        for i in range(4):
            rows = pl.ds(i * 128, 128)
            dp = nt(do[rows, pl.ds(128 * h, 128)], qkv[:, lanes(h, 2)])
            p = probs[h, rows, :].astype(F32)
            ds = factor * p * (dp - jnp.sum(p * dp, axis=-1, keepdims=True))
            probs[h, rows, :] = ds.astype(BF)
        dk = tn(probs[h], qkv[:, lanes(h, 0)]).astype(BF)
        qkv[:, lanes(h, 0)] = nn(probs[h], qkv[:, lanes(h, 1)]).astype(BF)
        qkv[:, lanes(h, 1)] = dk
        qkv[:, lanes(h, 2)] = dv[...]

    for h in range(3):
        steps[f"attend_back_{h}"] = functools.partial(attend_back, h)

    @step
    def last_out():
        def each(r):
            rows = pl.ds(r, BLOCK)
            final_ref[rows, :] = (mid[rows, :] + mod(5) * reds["ffn"].rows(r, BLOCK)).astype(BF)

        by_rows(each)
        outputs["final"].start()

    @step
    def first_grad():
        def each(r):
            rows = pl.ds(r, BLOCK)
            n1, r1 = normalize(x_ref[rows, :].astype(F32))
            inner = norm_back(n1, r1, reds["da1"].rows(r, BLOCK) * (1.0 + mod(1)))
            ig_ref[rows, :] = dmid[rows, :] + inner

        by_rows(each)
        outputs["ig"].start()

    @step
    def finish():
        outputs["sums"].start()
        wires.drain()
        for copy in outputs.values():
            copy.wait()

    for name in ORDER:
        with jax.named_scope(name):
            steps[name]()


def finish_kernel(
    final_in, ig_in, sums_in, final_out, ig_out, gq_out, go_out, gi_out, gb_out, final, ig, sums, sem
):
    cuts = [(384 * which, 384, gq_out.at[which]) for which in range(3)]
    cuts += [(1152, 384, go_out), (1536, 1536, gi_out), (3072, 1536, gb_out)]
    pairs = [(sums_in.at[:, pl.ds(at, n)], sums.at[:, pl.ds(at, n)], out) for at, n, out in cuts]
    pairs += [(ig_in, ig, ig_out), (final_in, final, final_out)]
    loads, stores = [], []
    for i, (source, held, out) in enumerate(pairs):
        loads.append(pltpu.make_async_copy(source, held, sem.at[0, i]))
        stores.append(pltpu.make_async_copy(held, out, sem.at[1, i]))
    for load in loads:
        load.start()
    for load, store in zip(loads, stores):
        load.wait()
        store.start()
    for store in stores:
        store.wait()


def body(tokens, modulation, w_qkv, w_out, w_in, w_back, out_grad):
    own = w_qkv.shape[3]
    far = pl.BlockSpec(memory_space=pl.ANY)
    copies = 34 * len(CHUNKS) + 2 * 6 + 2 * 4 + 2 * 14 + 2 * 10
    rows = lambda n, count=512: pltpu.VMEM((count, n), BF)
    final, grad_in_rows, sums = pl.pallas_call(
        block_kernel,
        out_shape=(
            jax.ShapeDtypeStruct((128, 1536), BF),
            jax.ShapeDtypeStruct((128, 1536), F32),
            jax.ShapeDtypeStruct((48, WIDTH), F32),
        ),
        in_specs=[far] * 7,
        out_specs=(far, far, far),
        scratch_shapes=[
            pltpu.VMEM((128, 1536), BF),
            pltpu.VMEM((6, 1, 1536), F32),
            pltpu.VMEM((128, 1536), BF),
            pltpu.VMEM((128, 1536), BF),
            pltpu.VMEM((128, 1536), F32),
            pltpu.VMEM((48, WIDTH), F32),
            pltpu.VMEM((4, 384, HELD), BF),
            pltpu.VMEM((4, 384, HELD), BF),
            pltpu.VMEM((48, HELD), BF),
            pltpu.VMEM((48, 1536), BF),
            rows(1536), rows(1536, 1024), rows(1536, 1024), rows(1536),
            rows(1152), rows(384), rows(384),
            rows(768, 1024), rows(768, 1024), rows(1536), rows(1536, 1024),
            pltpu.VMEM((3, 512, 512), BF),
            pltpu.VMEM((512, 128), BF),
            pltpu.VMEM((2, 128, 1536), BF),
            pltpu.VMEM((128, 1536), BF),
            pltpu.VMEM((4, 128, 1536), BF),
            pltpu.VMEM((2, 64, 1536), BF),
            pltpu.VMEM((2, 128, 1536), BF),
            pltpu.VMEM((4, 128, 1536), BF),
            pltpu.VMEM((2, 64, 1536), BF),
            pltpu.VMEM((2, 128, 1536), BF),
            pltpu.VMEM((128, 1536), F32),
            pltpu.VMEM((128, 1536), F32),
            pltpu.SemaphoreType.DMA((copies,)),
            pltpu.SemaphoreType.DMA((copies,)),
            pltpu.SemaphoreType.DMA((20,)),
            *scatter_buffers(),
        ],
        compiler_params=pltpu.CompilerParams(
            collective_id=0, has_side_effects=True, vmem_limit_bytes=VMEM_LIMIT
        ),
        name="block",
    )(
        tokens[0],
        modulation[0].transpose(1, 0, 2),
        out_grad[0],
        w_qkv[0].transpose(1, 0, 2),
        w_out[0].T,
        w_in[0],
        w_back[0].T,
    )
    outs = pl.pallas_call(
        finish_kernel,
        out_shape=(
            jax.ShapeDtypeStruct((128, 1536), BF),
            jax.ShapeDtypeStruct((128, 1536), F32),
            jax.ShapeDtypeStruct((3, 48, own), F32),
            jax.ShapeDtypeStruct((48, own), F32),
            jax.ShapeDtypeStruct((48, 4 * own), F32),
            jax.ShapeDtypeStruct((48, 4 * own), F32),
        ),
        in_specs=[far] * 3,
        out_specs=(far,) * 6,
        scratch_shapes=[
            pltpu.VMEM((128, 1536), BF),
            pltpu.VMEM((128, 1536), F32),
            pltpu.VMEM((48, WIDTH), F32),
            pltpu.SemaphoreType.DMA((2, 8)),
        ],
        name="finish",
    )(final, grad_in_rows, sums)
    final, grad_in_rows, gq, go, gi, gb = outs
    return (final[None], grad_in_rows[None], gq.transpose(1, 0, 2)[None], go.T[None], gi[None], gb.T[None])


def solution(mesh):
    torus = Mesh(mesh.devices.reshape(4, 4, 2, 2, 2), FSDP + SP)
    return jax.shard_map(
        body,
        mesh=torus,
        in_specs=(
            P(FSDP, SP, None),
            P(FSDP, None, None, None),
            P(None, FSDP, None, SP),
            P(None, SP, FSDP),
            P(None, FSDP, SP),
            P(None, SP, FSDP),
            P(FSDP, SP, None),
        ),
        out_specs=(
            P(FSDP, SP, None),
            P(FSDP, SP, None),
            P(None, FSDP, None, SP),
            P(None, SP, FSDP),
            P(None, FSDP, SP),
            P(None, SP, FSDP),
        ),
        check_vma=False,
    )
```

```python
import functools
import math

import jax
import jax.numpy as jnp
from jax import lax
from jax.experimental import pallas as pl
from jax.experimental.pallas import tpu as pltpu
from jax.sharding import Mesh
from jax.sharding import PartitionSpec as P

HEAD_DIM = 128
MESH = pl.DeviceIdType.MESH
FSDP = ("z", "y", "xh")
SP = ("xl", "c")
BF = jnp.bfloat16
F32 = jnp.float32

ln_eps = 1e-06
temper = 2.5
VMEM_LIMIT = 64_500_000

TILES = ((2, 1), (1, 2), (2, 1), (1, 2), (3, 3), (3, 3))
OUT, IN, BACK = 3, 4, 5


def split_chunks():
    chunks, at = [], 0
    for tiles in TILES:
        parts = []
        for count in tiles:
            parts.append((at, 128 * count))
            at += 128 * count
        chunks.append(tuple(parts))
    return tuple(chunks)


CHUNKS = split_chunks()
HELD = 3072
STEPS = {"own": 0, "next": 1, "prev": -1, "far": 2}
WIDTH = 4608
ORDER = (
    134, 137, 136, 135, 36, 24,
    144, 12, 0, 86, 37, 141,
    25, 13, 1, 138, 72, 74,
    38, 26, 48, 76, 14, 2,
    39, 15, 73, 3, 84, 75,
    77, 60, 27, 16, 4, 28,
    40, 49, 61, 85, 17, 146,
    150, 5, 145, 148, 29, 147,
    41, 152, 154, 102, 50, 89,
    153, 149, 62, 104, 51, 151,
    87, 63, 155, 88, 103, 106,
    139, 93, 91, 107, 142, 95,
    52, 90, 105, 94, 98, 64,
    96, 53, 158, 99, 162, 166,
    97, 65, 167, 100, 170, 171,
    172, 120, 163, 164, 121, 168,
    118, 116, 175, 177, 117, 66,
    119, 159, 174, 176, 54, 122,
    160, 114, 92, 169, 128, 67,
    115, 161, 165, 124, 129, 126,
    123, 140, 78, 55, 143, 80,
    125, 127, 68, 173, 82, 130,
    131, 79, 182, 81, 56, 83,
    178, 42, 183, 69, 186, 181,
    30, 184, 179, 6, 43, 185,
    180, 18, 70, 156, 132, 31,
    157, 7, 19, 44, 108, 32,
    110, 8, 57, 20, 45, 109,
    9, 112, 33, 58, 21, 46,
    113, 10, 133, 187, 34, 22,
    188, 59, 11, 35, 71, 47,
    23, 189,
)


def turn(axis, step, size):
    return {axis: lax.rem(lax.axis_index(axis) + step + size, size)}


def near(axis, step):
    return lax.rem(lax.axis_index(axis) + step + 4, 4)


class Wires:
    def __init__(self, send, recv):
        self.send, self.recv, self.used, self.open = send, recv, 0, []

    def go(self, src, dst, device):
        at = self.used
        self.used += 1
        copy = pltpu.make_async_remote_copy(
            src_ref=src,
            dst_ref=dst,
            send_sem=self.send.at[at],
            recv_sem=self.recv.at[at],
            device_id=device,
            device_id_type=MESH,
        )
        copy.start()
        self.open.append(copy)
        return copy

    def sent(self, copy):
        copy.wait_send()
        self.open = [other for other in self.open if other is not copy]

    def drain(self):
        for copy in self.open:
            copy.wait_send()
        self.open = []


def chip(step):
    xh, xl = lax.axis_index("xh"), lax.axis_index("xl")
    if step == 0:
        return xh, xl
    if step == 2:
        return 1 - xh, xl
    return lax.rem(xh + xl + (0 if step == 1 else 1), 2), 1 - xl


def along(step):
    xh, xl = chip(step)
    return {"xh": xh, "xl": xl}


def partners():
    return [turn("z", 1, 4), turn("z", -1, 4), turn("y", 1, 4), turn("y", -1, 4)] + [
        turn("xh", 1, 2), turn("c", 1, 2), along(1), along(-1)
    ]


def greet():
    for device in partners():
        pl.semaphore_signal(
            pltpu.get_barrier_semaphore(), inc=1, device_id=device, device_id_type=MESH
        )


def met():
    pl.semaphore_wait(pltpu.get_barrier_semaphore(), len(partners()))


def rows_of(start, count):
    return pl.ds(pl.multiple_of(start, 16), count)


def cols_of(cols):
    return pl.ds(cols[0], cols[1])


class Gather:
    def __init__(self, wires, w, stage):
        self.wires, self.w, self.stage = wires, w, stage
        self.z, self.y, self.xh = (lax.axis_index(a) for a in FSDP)
        self.one, self.two, self.relay2, self.three, self.relay3 = {}, {}, {}, {}, {}

    def same(self, part, device):
        return self.wires.go(part, part, device)

    def s1(self, k):
        (a0, an), (b0, bn) = CHUNKS[k]
        part = self.w.at[self.z, rows_of(96 * self.y + 48 * self.xh, 48), pl.ds(a0, an + bn)]
        source = part if k < IN else self.stage.at[:, pl.ds(a0 - 1536, an + bn)]
        self.one[k] = self.wires.go(source, part, turn("xh", 1, 2))

    def s2(self, k):
        self.one[k].wait_recv()
        ca, cb = map(cols_of, CHUNKS[k])
        pa = self.w.at[self.z, rows_of(96 * self.y, 96), ca]
        pb = self.w.at[self.z, rows_of(96 * self.y, 96), cb]
        self.two[k] = [
            self.same(pa, turn("y", 1, 4)),
            self.same(pa, turn("y", -1, 4)),
            self.same(pb, turn("z", 1, 4)),
            self.same(pb, turn("z", -1, 4)),
        ]

    def s2b(self, k):
        ca, cb = map(cols_of, CHUNKS[k])
        for copy in self.two[k]:
            copy.wait_recv()
        w, z, y = self.w, self.z, self.y
        self.relay2[k] = [
            self.same(w.at[z, rows_of(96 * near("y", -1), 48), ca], turn("y", 1, 4)),
            self.same(w.at[z, rows_of(96 * near("y", 1) + 48, 48), ca], turn("y", -1, 4)),
            self.same(w.at[near("z", -1), rows_of(96 * y, 48), cb], turn("z", 1, 4)),
            self.same(w.at[near("z", 1), rows_of(96 * y + 48, 48), cb], turn("z", -1, 4)),
        ]

    def s3(self, k):
        ca, cb = map(cols_of, CHUNKS[k])
        for copy in self.relay2[k]:
            copy.wait_recv()
        pa = self.w.at[self.z, :, ca]
        pb = self.w.at[:, rows_of(96 * self.y, 96), cb]
        self.three[k] = [
            self.same(pa, turn("z", 1, 4)),
            self.same(pa, turn("z", -1, 4)),
            self.same(pb, turn("y", 1, 4)),
            self.same(pb, turn("y", -1, 4)),
        ]

    def s3b(self, k):
        ca, cb = map(cols_of, CHUNKS[k])
        for copy in self.three[k]:
            copy.wait_recv()
        w = self.w
        self.relay3[k] = [
            self.same(w.at[near("z", -1), pl.ds(0, 192), ca], turn("z", 1, 4)),
            self.same(w.at[near("z", 1), pl.ds(192, 192), ca], turn("z", -1, 4)),
            self.same(w.at[:, rows_of(96 * near("y", -1), 48), cb], turn("y", 1, 4)),
            self.same(w.at[:, rows_of(96 * near("y", 1) + 48, 48), cb], turn("y", -1, 4)),
        ]

    def done(self, k):
        for copy in self.relay3[k]:
            copy.wait_recv()


def add_into(dst, *srcs):
    planes, rows, columns = dst.shape

    @pl.loop(0, planes * (rows // 48))
    def _(i):
        at = (i // (rows // 48), pl.ds(pl.multiple_of((i % (rows // 48)) * 48, 48), 48), slice(None))
        total = dst[at].astype(F32)
        for src in srcs:
            total = total + src[at].astype(F32)
        dst[at] = total.astype(dst.dtype)


class Scatter:
    def __init__(self, wires, g, half_a, full_a, half_b, full_b, half2, full2, last, out):
        self.wires, self.g, self.out = wires, g, out
        self.half_a, self.full_a, self.half_b, self.full_b = half_a, full_a, half_b, full_b
        self.half2, self.full2, self.last = half2, full2, last
        self.z, self.y, self.xh = (lax.axis_index(a) for a in FSDP)
        self.copies = {}

    def block_a(self, step, start, count, cols):
        return self.g.at[pl.ds(near("z", step), 1), pl.ds(start, count), cols]

    def block_b(self, step, start, count, cols):
        return self.g.at[:, rows_of(96 * near("y", step) + start, count), cols]

    def sub_a(self, step, start, count, cols):
        return self.g.at[pl.ds(self.z, 1), rows_of(96 * near("y", step) + start, count), cols]

    def sub_b(self, step, start, count, cols):
        return self.g.at[pl.ds(near("z", step), 1), rows_of(96 * self.y + start, count), cols]

    def r1(self, k):
        ca, cb = map(cols_of, CHUNKS[k])
        go = self.wires.go
        self.copies[k, 1] = [
            go(self.block_a(2, 0, 192, ca), self.half_a[k].at[pl.ds(0, 1)], turn("z", 1, 4)),
            go(self.block_a(2, 192, 192, ca), self.half_a[k].at[pl.ds(1, 1)], turn("z", -1, 4)),
            go(self.block_b(2, 0, 48, cb), self.half_b[k].at[0], turn("y", 1, 4)),
            go(self.block_b(2, 48, 48, cb), self.half_b[k].at[1], turn("y", -1, 4)),
        ]

    def r1b(self, k):
        ca, cb = map(cols_of, CHUNKS[k])
        go, copies = self.wires.go, self.copies[k, 1]
        sent = []
        copies[0].wait_recv()
        add_into(self.block_a(1, 0, 192, ca), self.half_a[k].at[pl.ds(0, 1)])
        sent.append(go(self.block_a(1, 0, 384, ca), self.full_a[k].at[pl.ds(0, 1)], turn("z", 1, 4)))
        copies[1].wait_recv()
        add_into(self.block_a(-1, 192, 192, ca), self.half_a[k].at[pl.ds(1, 1)])
        sent.append(go(self.block_a(-1, 0, 384, ca), self.full_a[k].at[pl.ds(1, 1)], turn("z", -1, 4)))
        copies[2].wait_recv()
        add_into(self.block_b(1, 0, 48, cb), self.half_b[k].at[0])
        sent.append(go(self.block_b(1, 0, 96, cb), self.full_b[k].at[0], turn("y", 1, 4)))
        copies[3].wait_recv()
        add_into(self.block_b(-1, 48, 48, cb), self.half_b[k].at[1])
        sent.append(go(self.block_b(-1, 0, 96, cb), self.full_b[k].at[1], turn("y", -1, 4)))
        self.copies[k, 2] = sent

    def r2(self, k):
        ca, cb = map(cols_of, CHUNKS[k])
        go, copies = self.wires.go, self.copies[k, 2]
        copies[0].wait_recv()
        copies[1].wait_recv()
        add_into(
            self.block_a(0, 0, 384, ca), self.full_a[k].at[pl.ds(0, 1)], self.full_a[k].at[pl.ds(1, 1)]
        )
        sent = [
            go(self.sub_a(2, 0, 48, ca), self.half2[k][0].at[pl.ds(0, 1)], turn("y", 1, 4)),
            go(self.sub_a(2, 48, 48, ca), self.half2[k][0].at[pl.ds(1, 1)], turn("y", -1, 4)),
        ]
        copies[2].wait_recv()
        copies[3].wait_recv()
        add_into(self.block_b(0, 0, 96, cb), self.full_b[k].at[0], self.full_b[k].at[1])
        sent += [
            go(self.sub_b(2, 0, 48, cb), self.half2[k][1].at[pl.ds(0, 1)], turn("z", 1, 4)),
            go(self.sub_b(2, 48, 48, cb), self.half2[k][1].at[pl.ds(1, 1)], turn("z", -1, 4)),
        ]
        self.copies[k, 3] = sent

    def r2b(self, k):
        go, copies = self.wires.go, self.copies[k, 3]
        sent = []
        for colour, (sub, axis) in enumerate(((self.sub_a, "y"), (self.sub_b, "z"))):
            cols = cols_of(CHUNKS[k][colour])
            half, full = self.half2[k][colour], self.full2[k][colour]
            copies[2 * colour].wait_recv()
            add_into(sub(1, 0, 48, cols), half.at[pl.ds(0, 1)])
            sent.append(go(sub(1, 0, 96, cols), full.at[pl.ds(0, 1)], turn(axis, 1, 4)))
            copies[2 * colour + 1].wait_recv()
            add_into(sub(-1, 48, 48, cols), half.at[pl.ds(1, 1)])
            sent.append(go(sub(-1, 0, 96, cols), full.at[pl.ds(1, 1)], turn(axis, -1, 4)))
        self.copies[k, 4] = sent

    def r3(self, k):
        go, copies = self.wires.go, self.copies[k, 4]
        (a0, an), (b0, bn) = CHUNKS[k]
        for colour, sub in enumerate((self.sub_a, self.sub_b)):
            cols, full = cols_of(CHUNKS[k][colour]), self.full2[k][colour]
            copies[2 * colour].wait_recv()
            copies[2 * colour + 1].wait_recv()
            add_into(sub(0, 0, 96, cols), full.at[pl.ds(0, 1)], full.at[pl.ds(1, 1)])
        part = self.g.at[self.z, rows_of(96 * self.y + 48 * (1 - self.xh), 48), pl.ds(a0, an + bn)]
        self.copies[k, 5] = [go(part, self.last.at[:, pl.ds(a0, an + bn)], turn("xh", 1, 2))]

    def done(self, k):
        (a0, an), (b0, bn) = CHUNKS[k]
        self.copies[k, 5][0].wait_recv()
        cols = pl.ds(a0, an + bn)
        own = self.g[self.z, rows_of(96 * self.y + 48 * self.xh, 48), cols].astype(F32)
        came = self.last[:, cols].astype(F32)
        if k >= IN:
            base = 1536 * (k - OUT)
            self.out[:, pl.ds(pl.multiple_of(base + 768 * self.xh, 128), 768)] = own
            self.out[:, pl.ds(pl.multiple_of(base + 768 * (1 - self.xh), 128), 768)] = came
            return
        total = own + came
        if k == OUT:
            self.out[:, cols] = total
            return
        for at in range(0, an + bn, 128):
            head, which = (a0 + at) // 384, (a0 + at) % 384 // 128
            self.out[:, pl.ds(384 * which + 128 * head, 128)] = total[:, at : at + 128]


def scatter_buffers():
    shapes = []
    for (_, an), (_, bn) in CHUNKS:
        shapes += [
            pltpu.VMEM((2, 192, an), BF),
            pltpu.VMEM((2, 384, an), BF),
            pltpu.VMEM((2, 4, 48, bn), BF),
            pltpu.VMEM((2, 4, 96, bn), BF),
            pltpu.VMEM((2, 48, an), BF),
            pltpu.VMEM((2, 96, an), BF),
            pltpu.VMEM((2, 48, bn), BF),
            pltpu.VMEM((2, 96, bn), BF),
        ]
    return shapes


def make_scatter(wires, g, bufs, last, out):
    groups = [bufs[8 * k : 8 * k + 8] for k in range(len(CHUNKS))]
    return Scatter(
        wires,
        g,
        [b[0] for b in groups],
        [b[1] for b in groups],
        [b[2] for b in groups],
        [b[3] for b in groups],
        [(b[4], b[6]) for b in groups],
        [(b[5], b[7]) for b in groups],
        last,
        out,
    )


def nn(a, b):
    return jnp.dot(a, b, preferred_element_type=F32)


def nt(a, b):
    return lax.dot_general(a, b, (((1,), (1,)), ((), ())), preferred_element_type=F32)


def tn(a, b):
    return lax.dot_general(a, b, (((0,), (0,)), ((), ())), preferred_element_type=F32)


class Spread:
    def __init__(self, wires, buf):
        self.wires, self.buf = wires, buf
        self.xl, self.c = (lax.axis_index(a) for a in SP)
        self.far, self.near, self.relays = {}, {}, {}

    def block(self, xl, c, start=0, count=128):
        return self.buf.at[rows_of(256 * xl + 128 * c + start, count), :]

    def start(self, i):
        part = self.block(self.xl, self.c, 64 * i, 64)
        self.far[i] = self.wires.go(part, part, turn("xl", 1, 2))
        self.near[i] = self.wires.go(part, part, turn("c", 1, 2))

    def relay(self, i):
        self.far[i].wait_recv()
        part = self.block(1 - self.xl, self.c, 64 * i, 64)
        self.relays[i] = self.wires.go(part, part, turn("c", 1, 2))

    def own_half(self):
        for copy in self.near.values():
            copy.wait_recv()

    def done(self):
        for copy in self.relays.values():
            copy.wait_recv()

    def release(self):
        for group in (self.far, self.near, self.relays):
            for copy in group.values():
                self.wires.sent(copy)


class Collect:
    def __init__(self, wires, part, pair, cross):
        self.wires, self.part, self.pair, self.cross = wires, part, pair, cross
        self.xl, self.c = (lax.axis_index(a) for a in SP)

    def block(self, xl, c):
        return self.part.at[rows_of(256 * xl + 128 * c, 128), :]

    def other(self):
        self.first = self.wires.go(self.block(1 - self.xl, 1 - self.c), self.pair.at[0], turn("c", 1, 2))

    def send(self):
        self.first.wait_recv()
        self.third = []
        for i in range(2):
            rows = pl.ds(64 * i, 64)
            mine = self.block(1 - self.xl, self.c).at[rows, :]
            add2(mine, self.pair.at[0, rows, :])
            self.third.append(self.wires.go(mine, self.cross.at[rows, :], turn("xl", 1, 2)))

    def own(self):
        self.second = self.wires.go(self.block(self.xl, 1 - self.c), self.pair.at[1], turn("c", 1, 2))

    def wait(self, i):
        if i == 0:
            self.second.wait_recv()
        self.third[i].wait_recv()

    def release(self):
        for copy in (self.first, self.second, *self.third):
            self.wires.sent(copy)

    def rows(self, start, count):
        at = rows_of(256 * self.xl + 128 * self.c + start, count)
        total = self.part[at, :].astype(F32) + self.pair[1, pl.ds(start, count), :].astype(F32)
        return total + self.cross[pl.ds(start, count), :].astype(F32)


class RingSpread:
    def __init__(self, wires, buf):
        self.wires, self.buf, self.c = wires, buf, lax.axis_index("c")
        self.sent = {}

    def part(self, step, i):
        xh, xl = chip(step)
        return self.buf.at[rows_of(512 * xh + 256 * xl + 128 * self.c + 64 * i, 64), :]

    def go(self, key, step, i, device):
        self.sent[key] = self.wires.go(self.part(step, i), self.part(step, i), device)

    def start(self, i):
        self.go(("next", i), 0, i, along(1))
        self.go(("prev", i), 0, i, along(-1))
        self.go(("own", i), 0, i, turn("c", 1, 2))

    def side(self, name, step, i):
        self.sent[name, i].wait_recv()
        if (name, i) in (("next", 0), ("prev", 1)):
            self.go(("far", i), step, i, along(-step))
        self.go(("core", step, i), step, i, turn("c", 1, 2))

    def relay(self, i):
        if i == 0:
            self.side("next", -1, 0)
            self.side("prev", 1, 1)
        else:
            self.side("next", -1, 1)
            self.side("prev", 1, 0)

    def relay_far(self):
        for i in range(2):
            self.sent["far", i].wait_recv()
            self.go(("core", 2, i), 2, i, turn("c", 1, 2))

    def own_half(self):
        for i in range(2):
            self.sent["own", i].wait_recv()

    def done(self):
        for step in (1, -1):
            for i in range(2):
                self.sent["core", step, i].wait_recv()

    def done_far(self):
        for i in range(2):
            self.sent["core", 2, i].wait_recv()

    def release(self):
        for copy in self.sent.values():
            self.wires.sent(copy)


class RingCollect:
    def __init__(self, wires, part, pair, half, full):
        self.wires, self.part, self.pair, self.half, self.full = wires, part, pair, half, full
        self.c = lax.axis_index("c")
        self.sent = {}

    def block(self, step, c, start=0, count=128):
        xh, xl = chip(step)
        return self.part.at[rows_of(512 * xh + 256 * xl + 128 * c + start, count), :]

    def give(self, name):
        step = STEPS[name]
        self.sent[name] = self.wires.go(self.block(step, 1 - self.c), self.pair.at[step % 4], turn("c", 1, 2))

    def take(self, name):
        step = STEPS[name]
        self.sent[name].wait_recv()
        if step == 0:
            return
        add2(self.block(step, self.c), self.pair.at[step % 4])
        if step == 2:
            for i, way in enumerate((1, -1)):
                self.sent["half", way] = self.wires.go(
                    self.block(2, self.c, 64 * i, 64), self.half.at[i], along(way)
                )
            return
        i = 1 if step == 1 else 0
        self.sent["early", step] = self.wires.go(
            self.block(step, self.c, 64 * i, 64), self.full.at[1 - i, pl.ds(64 * i, 64), :], along(step)
        )

    def pass_on(self):
        for i, step in enumerate((1, -1)):
            self.sent["half", step].wait_recv()
            block = self.block(step, self.c, 64 * i, 64)
            add2(block, self.half.at[i])
            self.sent["late", step] = self.wires.go(
                block, self.full.at[i, pl.ds(64 * i, 64), :], along(step)
            )

    def wait(self):
        for step in (1, -1):
            self.sent["early", step].wait_recv()
            self.sent["late", step].wait_recv()

    def rows(self, start, count):
        xh, xl = chip(0)
        total = self.part[rows_of(512 * xh + 256 * xl + 128 * self.c + start, count), :].astype(F32)
        for ref in (self.pair.at[0], self.full.at[0], self.full.at[1]):
            total = total + ref[pl.ds(start, count), :].astype(F32)
        return total


def add2(dst, src):
    rows = dst.shape[0]

    @pl.loop(0, rows // 16)
    def _(i):
        at = (pl.ds(pl.multiple_of(i * 16, 16), 16), slice(None))
        dst[at] = (dst[at].astype(F32) + src[at].astype(F32)).astype(dst.dtype)


def normalize(stream):
    mean_part = jnp.mean(stream, axis=-1, keepdims=True)
    centred = stream - mean_part
    rstd = lax.rsqrt(jnp.mean(centred * centred, axis=-1, keepdims=True) + ln_eps)
    return (centred * rstd, rstd)


def norm_back(normed, rstd, incoming):
    first = jnp.mean(incoming, axis=-1, keepdims=True)
    second = jnp.mean(incoming * normed, axis=-1, keepdims=True)
    return rstd * (incoming - first - normed * second)


BLOCK = 16
ROOT = math.sqrt(2.0 / math.pi)


def by_rows(fn, start=0, count=128):
    for r in range(start, start + count, BLOCK):
        fn(r)


def block_kernel(
    x_in, m_in, og_in, wq_ref, wo_ref, wi_ref, wb_ref,
    final_ref, ig_ref, sums_ref,
    x_ref, m_ref, og_ref,
    w, g, last, stage, a1, dm, a2, da, qkv, o, do, gp, act, part, ring_part, probs, dv, pair, cross,
    pair0, half0, full0, pair1, half1, full1, mid, dmid, send, recv, local_sem, *bufs,
):
    z, y, xh, xl, c = (lax.axis_index(a) for a in FSDP + SP)
    shard_rows = rows_of(96 * y + 48 * xh, 48)
    pieces = [
        (wq_ref.at[which, :, pl.ds(128 * h, 128)], 384 * h + 128 * which, 128)
        for h in range(3)
        for which in range(3)
    ]
    mine = pl.ds(pl.multiple_of(768 * xh, 128), 768)
    theirs = pl.ds(pl.multiple_of(768 * (1 - xh), 128), 768)
    pieces += [(wo_ref, 1152, 384), (wi_ref.at[:, mine], 1536, 768), (wb_ref.at[:, mine], 2304, 768)]
    loads = [
        pltpu.make_async_copy(source, w.at[z, shard_rows, pl.ds(at, count)], local_sem.at[i])
        for i, (source, at, count) in enumerate(pieces)
    ]
    loads += [
        pltpu.make_async_copy(ref.at[:, theirs], stage.at[:, pl.ds(768 * i, 768)], local_sem.at[18 + i])
        for i, ref in enumerate((wi_ref, wb_ref))
    ]
    inputs = [
        pltpu.make_async_copy(a, b, local_sem.at[12 + i])
        for i, (a, b) in enumerate(((x_in, x_ref), (m_in, m_ref), (og_in, og_ref)))
    ]
    greet()
    for load in loads[:3] + inputs[:2] + loads[3:] + inputs[2:]:
        load.start()
    wires = Wires(send, recv)
    ag = Gather(wires, w, stage)
    rs = make_scatter(wires, g, bufs, last, sums_ref)
    own_row = 256 * xl + 128 * c
    own_start, other_start = 256 * xl, 256 * (1 - xl)
    scale = 1.0 / math.sqrt(32 * 512)
    factor = temper / math.sqrt(HEAD_DIM)
    steps = {}

    def step(fn):
        steps[fn.__name__] = fn
        return fn

    def mod(i):
        return m_ref[i]

    def own(start):
        return (rows_of(own_row + start, BLOCK), slice(None))

    def ring_own(start):
        return (rows_of(512 * xh + own_row + start, BLOCK), slice(None))

    def weights(start, count):
        return w[:, :, pl.ds(start, count)].reshape(1536, count)

    for k in range(len(CHUNKS)):
        for name in ("s1", "s2", "s2b", "s3", "s3b", "done"):
            steps[f"ag_{name}_{k}"] = functools.partial(getattr(ag, name), k)
        for name in ("r1", "r1b", "r2", "r2b", "r3", "done"):
            steps[f"rs_{name}_{k}"] = functools.partial(getattr(rs, name), k)
    for key, buf in (("a1", a1), ("da", da)):
        spread = Spread(wires, buf)
        for i in range(2):
            steps[f"{key}_start_{i}"] = functools.partial(spread.start, i)
            steps[f"{key}_relay_{i}"] = functools.partial(spread.relay, i)
        steps[f"{key}_own_half"] = spread.own_half
        steps[f"{key}_done"] = spread.done
    for key, buf in (("dm", dm), ("a2", a2)):
        spread = RingSpread(wires, buf)
        for i in range(2):
            steps[f"{key}_start_{i}"] = functools.partial(spread.start, i)
            steps[f"{key}_relay_{i}"] = functools.partial(spread.relay, i)
        for name in ("relay_far", "own_half", "done", "done_far", "release"):
            steps[f"{key}_{name}"] = getattr(spread, name)
    reds = {"att": Collect(wires, part, pair, cross), "da1": Collect(wires, part, pair, cross)}
    for key, red in reds.items():
        for name in ("other", "own", "send", "release"):
            steps[f"{key}_{name}"] = getattr(red, name)
        for i in range(2):
            steps[f"{key}_wait_{i}"] = functools.partial(red.wait, i)
    reds["da2"] = RingCollect(wires, ring_part, pair0, half0, full0)
    reds["ffn"] = RingCollect(wires, dm, pair1, half1, full1)
    for key in ("da2", "ffn"):
        red = reds[key]
        for name in STEPS:
            steps[f"{key}_give_{name}"] = functools.partial(red.give, name)
            steps[f"{key}_take_{name}"] = functools.partial(red.take, name)
        steps[f"{key}_pass_on"] = red.pass_on
        steps[f"{key}_wait"] = red.wait

    @step
    def load_first():
        for load in loads[:3]:
            load.wait()

    steps["met"] = met

    @step
    def load_inputs():
        inputs[0].wait()
        inputs[1].wait()

    @step
    def load_rest():
        for load in loads[3:]:
            load.wait()
        inputs[2].wait()

    def first_norm(r):
        n1, _ = normalize(x_ref[pl.ds(r, BLOCK), :].astype(F32))
        a1[own(r)] = (n1 * (1.0 + mod(1)) + mod(0)).astype(BF)

    def second_norm(r):
        rows = pl.ds(r, BLOCK)
        value = x_ref[rows, :].astype(F32) + mod(2) * reds["att"].rows(r, BLOCK)
        mid[rows, :] = value
        n2, _ = normalize(value)
        a2[ring_own(r)] = (n2 * (1.0 + mod(4)) + mod(3)).astype(BF)

    def mid_grad(r):
        rows = pl.ds(r, BLOCK)
        n2, r2 = normalize(mid[rows, :])
        inner = norm_back(n2, r2, reds["da2"].rows(r, BLOCK) * (1.0 + mod(4)))
        value = og_ref[rows, :].astype(F32) + inner
        dmid[rows, :] = value
        da[own(r)] = (mod(2) * value).astype(BF)

    for i in range(2):
        for fn in (first_norm, second_norm, mid_grad):
            steps[f"{fn.__name__}_{i}"] = functools.partial(by_rows, fn, 64 * i, 64)

    @step
    def gate_grad():
        def rows(r):
            dm[ring_own(r)] = (mod(5) * og_ref[pl.ds(r, BLOCK), :].astype(F32)).astype(BF)

        by_rows(rows)

    def lanes(h, which):
        return pl.ds(384 * h + 128 * which, 128)

    def project(start, count):
        qkv[:, pl.ds(start, count)] = nn(a1[...], weights(start, count)).astype(BF)

    for h in range(3):

        def project_head(h=h):
            project(384 * h, 384)

        steps[f"project_{h}"] = project_head

    def attend(h, start):
        rows = rows_of(start, 256)
        s = nt(qkv[rows, lanes(h, 0)], qkv[:, lanes(h, 1)])
        e = jnp.exp(factor * (s - jnp.max(s, axis=-1, keepdims=True)))
        p = (e * (1.0 / jnp.sum(e, axis=-1, keepdims=True))).astype(BF)
        probs[h, rows, :] = p
        o[rows, pl.ds(128 * h, 128)] = nn(p, qkv[:, lanes(h, 2)]).astype(BF)

    for h in range(3):
        steps[f"attend_{h}_other"] = functools.partial(attend, h, other_start)
        steps[f"attend_{h}_own"] = functools.partial(attend, h, own_start)

    def back_half(dst, lhs, start, at, count):
        rows = rows_of(start, 256)

        for j in range(2):
            rhs = w[2 * j : 2 * j + 2, :, pl.ds(at, count)].reshape(768, count)
            dst[rows, pl.ds(768 * j, 768)] = nt(lhs[rows, :], rhs).astype(BF)

    for key, dst, lhs, at, count in (("att", part, o, 1152, 384), ("da1", part, qkv, 0, 1152)):
        steps[f"{key}_mm_other"] = functools.partial(back_half, dst, lhs, other_start, at, count)
        steps[f"{key}_mm_own"] = functools.partial(back_half, dst, lhs, own_start, at, count)

    def quarter(name):
        at_xh, at_xl = chip(STEPS[name])
        return 512 * at_xh + 256 * at_xl

    def hidden(name):
        rows = rows_of(quarter(name), 256)

        for at in range(0, 768, 256):
            u = nn(a2[rows, :], weights(1536 + at, 256))
            sq = u * u
            t = jnp.tanh(u * (ROOT + (ROOT * 0.044715) * sq))
            half = 0.5 + 0.5 * t
            act[rows, pl.ds(at, 256)] = (u * half).astype(BF)
            inner = (0.5 * ROOT) + (1.5 * ROOT * 0.044715) * sq
            gp[rows, pl.ds(at, 256)] = (half + u * inner * (1.0 - t * t)).astype(BF)

    def hidden_grad(name):
        rows = rows_of(quarter(name), 256)

        for at in range(0, 768, 256):
            cols = pl.ds(at, 256)
            dg = nn(dm[rows, :], weights(2304 + at, 256))
            gp[rows, cols] = (gp[rows, cols].astype(F32) * dg).astype(BF)

    for name in STEPS:
        steps[f"hidden_{name}"] = functools.partial(hidden, name)
        steps[f"hgrad_{name}"] = functools.partial(hidden_grad, name)
        steps[f"da2_mm_{name}"] = functools.partial(back_half, ring_part, gp, quarter(name), 1536, 768)
        steps[f"ffn_mm_{name}"] = functools.partial(back_half, dm, act, quarter(name), 2304, 768)

    def grad(left, right, right_at, at, count, planes=(0, 4)):
        for j in range(*planes):
            lhs = left[:, pl.ds(384 * j, 384)]
            value = tn(lhs, right[:, pl.ds(right_at, count)]) * scale
            g[j, :, pl.ds(at, count)] = value.astype(BF)

    for i in range(2):
        steps[f"grad_in_{i}"] = functools.partial(grad, a2, gp, 0, 1536, 768, (2 * i, 2 * i + 2))
        steps[f"grad_back_{i}"] = functools.partial(grad, dm, act, 0, 2304, 768, (2 * i, 2 * i + 2))
    steps["grad_out"] = functools.partial(grad, da, o, 0, 1152, 384)
    for h in range(3):
        steps[f"grad_q_{h}"] = functools.partial(grad, a1, qkv, 384 * h, 384 * h, 384)

    def head_grads(start):
        rows = rows_of(start, 256)
        do[rows, :] = nn(da[rows, :], weights(1152, 384)).astype(BF)

    steps["heads_own"] = functools.partial(head_grads, own_start)
    steps["heads_other"] = functools.partial(head_grads, other_start)

    def attend_back(h):
        dv[...] = tn(probs[h], do[:, pl.ds(128 * h, 128)]).astype(BF)
        for i in range(4):
            rows = pl.ds(i * 128, 128)
            dp = nt(do[rows, pl.ds(128 * h, 128)], qkv[:, lanes(h, 2)])
            p = probs[h, rows, :].astype(F32)
            ds = factor * p * (dp - jnp.sum(p * dp, axis=-1, keepdims=True))
            probs[h, rows, :] = ds.astype(BF)
        dk = tn(probs[h], qkv[:, lanes(h, 0)]).astype(BF)
        qkv[:, lanes(h, 0)] = nn(probs[h], qkv[:, lanes(h, 1)]).astype(BF)
        qkv[:, lanes(h, 1)] = dk
        qkv[:, lanes(h, 2)] = dv[...]

    for h in range(3):
        steps[f"attend_back_{h}"] = functools.partial(attend_back, h)

    @step
    def last_out():
        def each(r):
            rows = pl.ds(r, BLOCK)
            final_ref[rows, :] = (mid[rows, :] + mod(5) * reds["ffn"].rows(r, BLOCK)).astype(BF)

        by_rows(each)

    @step
    def first_grad():
        def each(r):
            rows = pl.ds(r, BLOCK)
            n1, r1 = normalize(x_ref[rows, :].astype(F32))
            inner = norm_back(n1, r1, reds["da1"].rows(r, BLOCK) * (1.0 + mod(1)))
            ig_ref[rows, :] = dmid[rows, :] + inner

        by_rows(each)

    @step
    def finish():
        wires.drain()

    names = list(steps)
    for at in ORDER:
        with jax.named_scope(names[at]):
            steps[names[at]]()


def finish_kernel(final, ig, sums, final_out, ig_out, gq_out, go_out, gi_out, gb_out, sem):
    cuts = [(384 * which, 384, gq_out.at[which]) for which in range(3)]
    cuts += [(1152, 384, go_out), (1536, 1536, gi_out), (3072, 1536, gb_out)]
    pairs = [(sums.at[:, pl.ds(at, n)], out) for at, n, out in cuts]
    pairs += [(ig, ig_out), (final, final_out)]
    stores = [pltpu.make_async_copy(held, out, sem.at[i]) for i, (held, out) in enumerate(pairs)]
    for store in stores:
        store.start()
    for store in stores:
        store.wait()


def body(tokens, modulation, w_qkv, w_out, w_in, w_back, out_grad):
    own = w_qkv.shape[3]
    far = pl.BlockSpec(memory_space=pl.ANY)
    near_memory = pl.BlockSpec(memory_space=pltpu.VMEM)
    copies = 34 * len(CHUNKS) + 2 * 6 + 2 * 4 + 2 * 14 + 2 * 10
    rows = lambda n, count=512: pltpu.VMEM((count, n), BF)
    final, grad_in_rows, sums = pl.pallas_call(
        block_kernel,
        out_shape=(
            pltpu.VMEM((128, 1536), BF),
            pltpu.VMEM((128, 1536), F32),
            pltpu.VMEM((48, WIDTH), F32),
        ),
        in_specs=[far] * 7,
        out_specs=(near_memory,) * 3,
        scratch_shapes=[
            pltpu.VMEM((128, 1536), BF),
            pltpu.VMEM((6, 1, 1536), F32),
            pltpu.VMEM((128, 1536), BF),
            pltpu.VMEM((4, 384, HELD), BF),
            pltpu.VMEM((4, 384, HELD), BF),
            pltpu.VMEM((48, HELD), BF),
            pltpu.VMEM((48, 1536), BF),
            rows(1536), rows(1536, 1024), rows(1536, 1024), rows(1536),
            rows(1152), rows(384), rows(384),
            rows(768, 1024), rows(768, 1024), rows(1536), rows(1536, 1024),
            pltpu.VMEM((3, 512, 512), BF),
            pltpu.VMEM((512, 128), BF),
            pltpu.VMEM((2, 128, 1536), BF),
            pltpu.VMEM((128, 1536), BF),
            pltpu.VMEM((4, 128, 1536), BF),
            pltpu.VMEM((2, 64, 1536), BF),
            pltpu.VMEM((2, 128, 1536), BF),
            pltpu.VMEM((4, 128, 1536), BF),
            pltpu.VMEM((2, 64, 1536), BF),
            pltpu.VMEM((2, 128, 1536), BF),
            pltpu.VMEM((128, 1536), F32),
            pltpu.VMEM((128, 1536), F32),
            pltpu.SemaphoreType.DMA((copies,)),
            pltpu.SemaphoreType.DMA((copies,)),
            pltpu.SemaphoreType.DMA((20,)),
            *scatter_buffers(),
        ],
        compiler_params=pltpu.CompilerParams(
            collective_id=0, has_side_effects=True, vmem_limit_bytes=VMEM_LIMIT
        ),
        name="block",
    )(
        tokens[0],
        modulation[0].transpose(1, 0, 2),
        out_grad[0],
        w_qkv[0].transpose(1, 0, 2),
        w_out[0].T,
        w_in[0],
        w_back[0].T,
    )
    outs = pl.pallas_call(
        finish_kernel,
        out_shape=(
            jax.ShapeDtypeStruct((128, 1536), BF),
            jax.ShapeDtypeStruct((128, 1536), F32),
            jax.ShapeDtypeStruct((3, 48, own), F32),
            jax.ShapeDtypeStruct((48, own), F32),
            jax.ShapeDtypeStruct((48, 4 * own), F32),
            jax.ShapeDtypeStruct((48, 4 * own), F32),
        ),
        in_specs=[near_memory] * 3,
        out_specs=(far,) * 6,
        scratch_shapes=[pltpu.SemaphoreType.DMA((8,))],
        name="finish",
    )(*(pltpu.with_memory_space_constraint(held, pltpu.VMEM) for held in (final, grad_in_rows, sums)))
    final, grad_in_rows, gq, go, gi, gb = outs
    return (final[None], grad_in_rows[None], gq.transpose(1, 0, 2)[None], go.T[None], gi[None], gb.T[None])


def solution(mesh):
    torus = Mesh(mesh.devices.reshape(4, 4, 2, 2, 2), FSDP + SP)
    return jax.shard_map(
        body,
        mesh=torus,
        in_specs=(
            P(FSDP, SP, None),
            P(FSDP, None, None, None),
            P(None, FSDP, None, SP),
            P(None, SP, FSDP),
            P(None, FSDP, SP),
            P(None, SP, FSDP),
            P(FSDP, SP, None),
        ),
        out_specs=(
            P(FSDP, SP, None),
            P(FSDP, SP, None),
            P(None, FSDP, None, SP),
            P(None, SP, FSDP),
            P(None, FSDP, SP),
            P(None, SP, FSDP),
        ),
        check_vma=False,
    )
```

```python
import functools
import math

import jax
import jax.numpy as jnp
from jax import lax
from jax.experimental import pallas as pl
from jax.experimental.pallas import tpu as pltpu
from jax.sharding import Mesh
from jax.sharding import PartitionSpec as P

HEAD_DIM = 128
MESH = pl.DeviceIdType.MESH
FSDP = ("z", "y", "xh")
SP = ("xl", "c")
BF = jnp.bfloat16
F32 = jnp.float32

ln_eps = 1e-06
temper = 2.5
VMEM_LIMIT = 64_500_000

TILES = ((2, 1), (1, 2), (2, 1), (1, 2), (3, 3), (3, 3))
OUT, IN, BACK = 3, 4, 5


def split_chunks():
    chunks, at = [], 0
    for tiles in TILES:
        parts = []
        for count in tiles:
            parts.append((at, 128 * count))
            at += 128 * count
        chunks.append(tuple(parts))
    return tuple(chunks)


CHUNKS = split_chunks()
HELD = 3072
STEPS = {"own": 0, "next": 1, "prev": -1, "far": 2}
WIDTH = 4608
ORDER = (
    134, 137, 135, 12, 0, 24,
    136, 36, 48, 138, 72, 141,
    144, 74, 13, 86, 84, 1,
    25, 37, 14, 76, 89, 49,
    60, 2, 26, 38, 15, 3,
    73, 75, 27, 39, 4, 16,
    28, 40, 85, 87, 50, 77,
    61, 5, 145, 148, 17, 146,
    150, 29, 147, 152, 41, 154,
    102, 90, 151, 88, 62, 149,
    104, 51, 153, 155, 91, 103,
    63, 92, 106, 139, 93, 52,
    107, 142, 95, 64, 94, 96,
    53, 98, 158, 99, 166, 162,
    97, 65, 167, 100, 170, 171,
    172, 120, 163, 164, 121, 116,
    168, 118, 175, 177, 66, 119,
    117, 159, 105, 176, 174, 54,
    122, 160, 114, 67, 173, 165,
    130, 169, 161, 124, 115, 123,
    140, 78, 143, 80, 128, 125,
    55, 68, 129, 82, 126, 131,
    182, 127, 79, 81, 56, 69,
    83, 178, 42, 183, 186, 181,
    30, 185, 180, 18, 184, 43,
    179, 6, 31, 156, 70, 132,
    157, 108, 110, 19, 7, 44,
    32, 109, 20, 133, 187, 57,
    112, 71, 8, 33, 45, 113,
    21, 58, 9, 188, 34, 46,
    22, 10, 23, 35, 47, 59,
    11, 189,
)


def turn(axis, step, size):
    return {axis: lax.rem(lax.axis_index(axis) + step + size, size)}


def near(axis, step):
    return lax.rem(lax.axis_index(axis) + step + 4, 4)


class Wires:
    def __init__(self, send, recv):
        self.send, self.recv, self.used, self.open = send, recv, 0, []

    def go(self, src, dst, device):
        at = self.used
        self.used += 1
        copy = pltpu.make_async_remote_copy(
            src_ref=src,
            dst_ref=dst,
            send_sem=self.send.at[at],
            recv_sem=self.recv.at[at],
            device_id=device,
            device_id_type=MESH,
        )
        copy.start()
        self.open.append(copy)
        return copy

    def sent(self, copy):
        copy.wait_send()
        self.open = [other for other in self.open if other is not copy]

    def drain(self):
        for copy in self.open:
            copy.wait_send()
        self.open = []


def chip(step):
    xh, xl = lax.axis_index("xh"), lax.axis_index("xl")
    if step == 0:
        return xh, xl
    if step == 2:
        return 1 - xh, xl
    return lax.rem(xh + xl + (0 if step == 1 else 1), 2), 1 - xl


def along(step):
    xh, xl = chip(step)
    return {"xh": xh, "xl": xl}


def partners():
    return [turn("z", 1, 4), turn("z", -1, 4), turn("y", 1, 4), turn("y", -1, 4)] + [
        turn("xh", 1, 2), turn("c", 1, 2), along(1), along(-1)
    ]


def greet():
    for device in partners():
        pl.semaphore_signal(
            pltpu.get_barrier_semaphore(), inc=1, device_id=device, device_id_type=MESH
        )


def met():
    pl.semaphore_wait(pltpu.get_barrier_semaphore(), len(partners()))


def rows_of(start, count):
    return pl.ds(pl.multiple_of(start, 16), count)


def cols_of(cols):
    return pl.ds(cols[0], cols[1])


class Gather:
    def __init__(self, wires, w, stage):
        self.wires, self.w, self.stage = wires, w, stage
        self.z, self.y, self.xh = (lax.axis_index(a) for a in FSDP)
        self.one, self.two, self.relay2, self.three, self.relay3 = {}, {}, {}, {}, {}

    def same(self, part, device):
        return self.wires.go(part, part, device)

    def s1(self, k):
        (a0, an), (b0, bn) = CHUNKS[k]
        part = self.w.at[self.z, rows_of(96 * self.y + 48 * self.xh, 48), pl.ds(a0, an + bn)]
        source = part if k < IN else self.stage.at[:, pl.ds(a0 - 1536, an + bn)]
        self.one[k] = self.wires.go(source, part, turn("xh", 1, 2))

    def s2(self, k):
        self.one[k].wait_recv()
        ca, cb = map(cols_of, CHUNKS[k])
        pa = self.w.at[self.z, rows_of(96 * self.y, 96), ca]
        pb = self.w.at[self.z, rows_of(96 * self.y, 96), cb]
        self.two[k] = [
            self.same(pa, turn("y", 1, 4)),
            self.same(pa, turn("y", -1, 4)),
            self.same(pb, turn("z", 1, 4)),
            self.same(pb, turn("z", -1, 4)),
        ]

    def s2b(self, k):
        ca, cb = map(cols_of, CHUNKS[k])
        for copy in self.two[k]:
            copy.wait_recv()
        w, z, y = self.w, self.z, self.y
        self.relay2[k] = [
            self.same(w.at[z, rows_of(96 * near("y", -1), 48), ca], turn("y", 1, 4)),
            self.same(w.at[z, rows_of(96 * near("y", 1) + 48, 48), ca], turn("y", -1, 4)),
            self.same(w.at[near("z", -1), rows_of(96 * y, 48), cb], turn("z", 1, 4)),
            self.same(w.at[near("z", 1), rows_of(96 * y + 48, 48), cb], turn("z", -1, 4)),
        ]

    def s3(self, k):
        ca, cb = map(cols_of, CHUNKS[k])
        for copy in self.relay2[k]:
            copy.wait_recv()
        pa = self.w.at[self.z, :, ca]
        pb = self.w.at[:, rows_of(96 * self.y, 96), cb]
        self.three[k] = [
            self.same(pa, turn("z", 1, 4)),
            self.same(pa, turn("z", -1, 4)),
            self.same(pb, turn("y", 1, 4)),
            self.same(pb, turn("y", -1, 4)),
        ]

    def s3b(self, k):
        ca, cb = map(cols_of, CHUNKS[k])
        for copy in self.three[k]:
            copy.wait_recv()
        w = self.w
        self.relay3[k] = [
            self.same(w.at[near("z", -1), pl.ds(0, 192), ca], turn("z", 1, 4)),
            self.same(w.at[near("z", 1), pl.ds(192, 192), ca], turn("z", -1, 4)),
            self.same(w.at[:, rows_of(96 * near("y", -1), 48), cb], turn("y", 1, 4)),
            self.same(w.at[:, rows_of(96 * near("y", 1) + 48, 48), cb], turn("y", -1, 4)),
        ]

    def done(self, k):
        for copy in self.relay3[k]:
            copy.wait_recv()


def add_into(dst, *srcs):
    planes, rows, columns = dst.shape

    @pl.loop(0, planes * (rows // 48))
    def _(i):
        at = (i // (rows // 48), pl.ds(pl.multiple_of((i % (rows // 48)) * 48, 48), 48), slice(None))
        total = dst[at].astype(F32)
        for src in srcs:
            total = total + src[at].astype(F32)
        dst[at] = total.astype(dst.dtype)


class Scatter:
    def __init__(self, wires, g, half_a, full_a, half_b, full_b, half2, full2, last, out):
        self.wires, self.g, self.out = wires, g, out
        self.half_a, self.full_a, self.half_b, self.full_b = half_a, full_a, half_b, full_b
        self.half2, self.full2, self.last = half2, full2, last
        self.z, self.y, self.xh = (lax.axis_index(a) for a in FSDP)
        self.copies = {}

    def block_a(self, step, start, count, cols):
        return self.g.at[pl.ds(near("z", step), 1), pl.ds(start, count), cols]

    def block_b(self, step, start, count, cols):
        return self.g.at[:, rows_of(96 * near("y", step) + start, count), cols]

    def sub_a(self, step, start, count, cols):
        return self.g.at[pl.ds(self.z, 1), rows_of(96 * near("y", step) + start, count), cols]

    def sub_b(self, step, start, count, cols):
        return self.g.at[pl.ds(near("z", step), 1), rows_of(96 * self.y + start, count), cols]

    def r1(self, k):
        ca, cb = map(cols_of, CHUNKS[k])
        go = self.wires.go
        self.copies[k, 1] = [
            go(self.block_a(2, 0, 192, ca), self.half_a[k].at[pl.ds(0, 1)], turn("z", 1, 4)),
            go(self.block_a(2, 192, 192, ca), self.half_a[k].at[pl.ds(1, 1)], turn("z", -1, 4)),
            go(self.block_b(2, 0, 48, cb), self.half_b[k].at[0], turn("y", 1, 4)),
            go(self.block_b(2, 48, 48, cb), self.half_b[k].at[1], turn("y", -1, 4)),
        ]

    def r1b(self, k):
        ca, cb = map(cols_of, CHUNKS[k])
        go, copies = self.wires.go, self.copies[k, 1]
        sent = []
        copies[0].wait_recv()
        add_into(self.block_a(1, 0, 192, ca), self.half_a[k].at[pl.ds(0, 1)])
        sent.append(go(self.block_a(1, 0, 384, ca), self.full_a[k].at[pl.ds(0, 1)], turn("z", 1, 4)))
        copies[1].wait_recv()
        add_into(self.block_a(-1, 192, 192, ca), self.half_a[k].at[pl.ds(1, 1)])
        sent.append(go(self.block_a(-1, 0, 384, ca), self.full_a[k].at[pl.ds(1, 1)], turn("z", -1, 4)))
        copies[2].wait_recv()
        add_into(self.block_b(1, 0, 48, cb), self.half_b[k].at[0])
        sent.append(go(self.block_b(1, 0, 96, cb), self.full_b[k].at[0], turn("y", 1, 4)))
        copies[3].wait_recv()
        add_into(self.block_b(-1, 48, 48, cb), self.half_b[k].at[1])
        sent.append(go(self.block_b(-1, 0, 96, cb), self.full_b[k].at[1], turn("y", -1, 4)))
        self.copies[k, 2] = sent

    def r2(self, k):
        ca, cb = map(cols_of, CHUNKS[k])
        go, copies = self.wires.go, self.copies[k, 2]
        copies[0].wait_recv()
        copies[1].wait_recv()
        add_into(
            self.block_a(0, 0, 384, ca), self.full_a[k].at[pl.ds(0, 1)], self.full_a[k].at[pl.ds(1, 1)]
        )
        sent = [
            go(self.sub_a(2, 0, 48, ca), self.half2[k][0].at[pl.ds(0, 1)], turn("y", 1, 4)),
            go(self.sub_a(2, 48, 48, ca), self.half2[k][0].at[pl.ds(1, 1)], turn("y", -1, 4)),
        ]
        copies[2].wait_recv()
        copies[3].wait_recv()
        add_into(self.block_b(0, 0, 96, cb), self.full_b[k].at[0], self.full_b[k].at[1])
        sent += [
            go(self.sub_b(2, 0, 48, cb), self.half2[k][1].at[pl.ds(0, 1)], turn("z", 1, 4)),
            go(self.sub_b(2, 48, 48, cb), self.half2[k][1].at[pl.ds(1, 1)], turn("z", -1, 4)),
        ]
        self.copies[k, 3] = sent

    def r2b(self, k):
        go, copies = self.wires.go, self.copies[k, 3]
        sent = []
        for colour, (sub, axis) in enumerate(((self.sub_a, "y"), (self.sub_b, "z"))):
            cols = cols_of(CHUNKS[k][colour])
            half, full = self.half2[k][colour], self.full2[k][colour]
            copies[2 * colour].wait_recv()
            add_into(sub(1, 0, 48, cols), half.at[pl.ds(0, 1)])
            sent.append(go(sub(1, 0, 96, cols), full.at[pl.ds(0, 1)], turn(axis, 1, 4)))
            copies[2 * colour + 1].wait_recv()
            add_into(sub(-1, 48, 48, cols), half.at[pl.ds(1, 1)])
            sent.append(go(sub(-1, 0, 96, cols), full.at[pl.ds(1, 1)], turn(axis, -1, 4)))
        self.copies[k, 4] = sent

    def r3(self, k):
        go, copies = self.wires.go, self.copies[k, 4]
        (a0, an), (b0, bn) = CHUNKS[k]
        for colour, sub in enumerate((self.sub_a, self.sub_b)):
            cols, full = cols_of(CHUNKS[k][colour]), self.full2[k][colour]
            copies[2 * colour].wait_recv()
            copies[2 * colour + 1].wait_recv()
            add_into(sub(0, 0, 96, cols), full.at[pl.ds(0, 1)], full.at[pl.ds(1, 1)])
        part = self.g.at[self.z, rows_of(96 * self.y + 48 * (1 - self.xh), 48), pl.ds(a0, an + bn)]
        self.copies[k, 5] = [go(part, self.last.at[:, pl.ds(a0, an + bn)], turn("xh", 1, 2))]

    def done(self, k):
        (a0, an), (b0, bn) = CHUNKS[k]
        self.copies[k, 5][0].wait_recv()
        cols = pl.ds(a0, an + bn)
        own = self.g[self.z, rows_of(96 * self.y + 48 * self.xh, 48), cols].astype(F32)
        came = self.last[:, cols].astype(F32)
        if k >= IN:
            base = 1536 * (k - OUT)
            self.out[:, pl.ds(pl.multiple_of(base + 768 * self.xh, 128), 768)] = own
            self.out[:, pl.ds(pl.multiple_of(base + 768 * (1 - self.xh), 128), 768)] = came
            return
        total = own + came
        if k == OUT:
            self.out[:, cols] = total
            return
        for at in range(0, an + bn, 128):
            head, which = (a0 + at) // 384, (a0 + at) % 384 // 128
            self.out[:, pl.ds(384 * which + 128 * head, 128)] = total[:, at : at + 128]


def scatter_buffers():
    shapes = []
    for (_, an), (_, bn) in CHUNKS:
        shapes += [
            pltpu.VMEM((2, 192, an), BF),
            pltpu.VMEM((2, 384, an), BF),
            pltpu.VMEM((2, 4, 48, bn), BF),
            pltpu.VMEM((2, 4, 96, bn), BF),
            pltpu.VMEM((2, 48, an), BF),
            pltpu.VMEM((2, 96, an), BF),
            pltpu.VMEM((2, 48, bn), BF),
            pltpu.VMEM((2, 96, bn), BF),
        ]
    return shapes


def make_scatter(wires, g, bufs, last, out):
    groups = [bufs[8 * k : 8 * k + 8] for k in range(len(CHUNKS))]
    return Scatter(
        wires,
        g,
        [b[0] for b in groups],
        [b[1] for b in groups],
        [b[2] for b in groups],
        [b[3] for b in groups],
        [(b[4], b[6]) for b in groups],
        [(b[5], b[7]) for b in groups],
        last,
        out,
    )


def nn(a, b):
    return jnp.dot(a, b, preferred_element_type=F32)


def nt(a, b):
    return lax.dot_general(a, b, (((1,), (1,)), ((), ())), preferred_element_type=F32)


def tn(a, b):
    return lax.dot_general(a, b, (((0,), (0,)), ((), ())), preferred_element_type=F32)


class Spread:
    def __init__(self, wires, buf):
        self.wires, self.buf = wires, buf
        self.xl, self.c = (lax.axis_index(a) for a in SP)
        self.far, self.near, self.relays = {}, {}, {}

    def block(self, xl, c, start=0, count=128):
        return self.buf.at[rows_of(256 * xl + 128 * c + start, count), :]

    def start(self, i):
        part = self.block(self.xl, self.c, 64 * i, 64)
        self.far[i] = self.wires.go(part, part, turn("xl", 1, 2))
        self.near[i] = self.wires.go(part, part, turn("c", 1, 2))

    def relay(self, i):
        self.far[i].wait_recv()
        part = self.block(1 - self.xl, self.c, 64 * i, 64)
        self.relays[i] = self.wires.go(part, part, turn("c", 1, 2))

    def own_half(self):
        for copy in self.near.values():
            copy.wait_recv()

    def done(self):
        for copy in self.relays.values():
            copy.wait_recv()

    def release(self):
        for group in (self.far, self.near, self.relays):
            for copy in group.values():
                self.wires.sent(copy)


class Collect:
    def __init__(self, wires, part, pair, cross):
        self.wires, self.part, self.pair, self.cross = wires, part, pair, cross
        self.xl, self.c = (lax.axis_index(a) for a in SP)

    def block(self, xl, c):
        return self.part.at[rows_of(256 * xl + 128 * c, 128), :]

    def other(self):
        self.first = self.wires.go(self.block(1 - self.xl, 1 - self.c), self.pair.at[0], turn("c", 1, 2))

    def send(self):
        self.first.wait_recv()
        self.third = []
        for i in range(2):
            rows = pl.ds(64 * i, 64)
            mine = self.block(1 - self.xl, self.c).at[rows, :]
            add2(mine, self.pair.at[0, rows, :])
            self.third.append(self.wires.go(mine, self.cross.at[rows, :], turn("xl", 1, 2)))

    def own(self):
        self.second = self.wires.go(self.block(self.xl, 1 - self.c), self.pair.at[1], turn("c", 1, 2))

    def wait(self, i):
        if i == 0:
            self.second.wait_recv()
        self.third[i].wait_recv()

    def release(self):
        for copy in (self.first, self.second, *self.third):
            self.wires.sent(copy)

    def rows(self, start, count):
        at = rows_of(256 * self.xl + 128 * self.c + start, count)
        total = self.part[at, :].astype(F32) + self.pair[1, pl.ds(start, count), :].astype(F32)
        return total + self.cross[pl.ds(start, count), :].astype(F32)


class RingSpread:
    def __init__(self, wires, buf):
        self.wires, self.buf, self.c = wires, buf, lax.axis_index("c")
        self.sent = {}

    def part(self, step, i):
        xh, xl = chip(step)
        return self.buf.at[rows_of(512 * xh + 256 * xl + 128 * self.c + 64 * i, 64), :]

    def go(self, key, step, i, device):
        self.sent[key] = self.wires.go(self.part(step, i), self.part(step, i), device)

    def start(self, i):
        self.go(("next", i), 0, i, along(1))
        self.go(("prev", i), 0, i, along(-1))
        self.go(("own", i), 0, i, turn("c", 1, 2))

    def side(self, name, step, i):
        self.sent[name, i].wait_recv()
        if (name, i) in (("next", 0), ("prev", 1)):
            self.go(("far", i), step, i, along(-step))
        self.go(("core", step, i), step, i, turn("c", 1, 2))

    def relay(self, i):
        if i == 0:
            self.side("next", -1, 0)
            self.side("prev", 1, 1)
        else:
            self.side("next", -1, 1)
            self.side("prev", 1, 0)

    def relay_far(self):
        for i in range(2):
            self.sent["far", i].wait_recv()
            self.go(("core", 2, i), 2, i, turn("c", 1, 2))

    def own_half(self):
        for i in range(2):
            self.sent["own", i].wait_recv()

    def done(self):
        for step in (1, -1):
            for i in range(2):
                self.sent["core", step, i].wait_recv()

    def done_far(self):
        for i in range(2):
            self.sent["core", 2, i].wait_recv()

    def release(self):
        for copy in self.sent.values():
            self.wires.sent(copy)


class RingCollect:
    def __init__(self, wires, part, pair, half, full):
        self.wires, self.part, self.pair, self.half, self.full = wires, part, pair, half, full
        self.c = lax.axis_index("c")
        self.sent = {}

    def block(self, step, c, start=0, count=128):
        xh, xl = chip(step)
        return self.part.at[rows_of(512 * xh + 256 * xl + 128 * c + start, count), :]

    def give(self, name):
        step = STEPS[name]
        self.sent[name] = self.wires.go(self.block(step, 1 - self.c), self.pair.at[step % 4], turn("c", 1, 2))

    def take(self, name):
        step = STEPS[name]
        self.sent[name].wait_recv()
        if step == 0:
            return
        add2(self.block(step, self.c), self.pair.at[step % 4])
        if step == 2:
            for i, way in enumerate((1, -1)):
                self.sent["half", way] = self.wires.go(
                    self.block(2, self.c, 64 * i, 64), self.half.at[i], along(way)
                )
            return
        i = 1 if step == 1 else 0
        self.sent["early", step] = self.wires.go(
            self.block(step, self.c, 64 * i, 64), self.full.at[1 - i, pl.ds(64 * i, 64), :], along(step)
        )

    def pass_on(self):
        for i, step in enumerate((1, -1)):
            self.sent["half", step].wait_recv()
            block = self.block(step, self.c, 64 * i, 64)
            add2(block, self.half.at[i])
            self.sent["late", step] = self.wires.go(
                block, self.full.at[i, pl.ds(64 * i, 64), :], along(step)
            )

    def wait(self):
        for step in (1, -1):
            self.sent["early", step].wait_recv()
            self.sent["late", step].wait_recv()

    def rows(self, start, count):
        xh, xl = chip(0)
        total = self.part[rows_of(512 * xh + 256 * xl + 128 * self.c + start, count), :].astype(F32)
        for ref in (self.pair.at[0], self.full.at[0], self.full.at[1]):
            total = total + ref[pl.ds(start, count), :].astype(F32)
        return total


def add2(dst, src):
    rows = dst.shape[0]

    @pl.loop(0, rows // 16)
    def _(i):
        at = (pl.ds(pl.multiple_of(i * 16, 16), 16), slice(None))
        dst[at] = (dst[at].astype(F32) + src[at].astype(F32)).astype(dst.dtype)


def normalize(stream):
    mean_part = jnp.mean(stream, axis=-1, keepdims=True)
    centred = stream - mean_part
    rstd = lax.rsqrt(jnp.mean(centred * centred, axis=-1, keepdims=True) + ln_eps)
    return (centred * rstd, rstd)


def norm_back(normed, rstd, incoming):
    first = jnp.mean(incoming, axis=-1, keepdims=True)
    second = jnp.mean(incoming * normed, axis=-1, keepdims=True)
    return rstd * (incoming - first - normed * second)


BLOCK = 16
ROOT = math.sqrt(2.0 / math.pi)


def by_rows(fn, start=0, count=128):
    for r in range(start, start + count, BLOCK):
        fn(r)


def block_kernel(
    x_in, m_in, og_in, wq_ref, wo_ref, wi_ref, wb_ref,
    final_ref, ig_ref, sums_ref,
    x_ref, m_ref, og_ref,
    w, g, last, stage, a1, dm, a2, da, qkv, o, do, gp, act, part, ring_part, probs, dv, pair, cross,
    pair0, half0, full0, pair1, half1, full1, mid, dmid, send, recv, local_sem, *bufs,
):
    z, y, xh, xl, c = (lax.axis_index(a) for a in FSDP + SP)
    shard_rows = rows_of(96 * y + 48 * xh, 48)
    pieces = [
        (wq_ref.at[which, :, pl.ds(128 * h, 128)], 384 * h + 128 * which, 128)
        for h in range(3)
        for which in range(3)
    ]
    mine = pl.ds(pl.multiple_of(768 * xh, 128), 768)
    theirs = pl.ds(pl.multiple_of(768 * (1 - xh), 128), 768)
    pieces += [(wo_ref, 1152, 384), (wi_ref.at[:, mine], 1536, 768), (wb_ref.at[:, mine], 2304, 768)]
    loads = [
        pltpu.make_async_copy(source, w.at[z, shard_rows, pl.ds(at, count)], local_sem.at[i])
        for i, (source, at, count) in enumerate(pieces)
    ]
    loads += [
        pltpu.make_async_copy(ref.at[:, theirs], stage.at[:, pl.ds(768 * i, 768)], local_sem.at[18 + i])
        for i, ref in enumerate((wi_ref, wb_ref))
    ]
    inputs = [
        pltpu.make_async_copy(a, b, local_sem.at[12 + i])
        for i, (a, b) in enumerate(((x_in, x_ref), (m_in, m_ref), (og_in, og_ref)))
    ]
    greet()
    for load in loads[:3] + inputs[:2] + loads[3:] + inputs[2:]:
        load.start()
    wires = Wires(send, recv)
    ag = Gather(wires, w, stage)
    rs = make_scatter(wires, g, bufs, last, sums_ref)
    own_row = 256 * xl + 128 * c
    own_start, other_start = 256 * xl, 256 * (1 - xl)
    scale = 1.0 / math.sqrt(32 * 512)
    factor = temper / math.sqrt(HEAD_DIM)
    steps = {}

    def step(fn):
        steps[fn.__name__] = fn
        return fn

    def mod(i):
        return m_ref[i]

    def own(start):
        return (rows_of(own_row + start, BLOCK), slice(None))

    def ring_own(start):
        return (rows_of(512 * xh + own_row + start, BLOCK), slice(None))

    def weights(start, count):
        return w[:, :, pl.ds(start, count)].reshape(1536, count)

    for k in range(len(CHUNKS)):
        for name in ("s1", "s2", "s2b", "s3", "s3b", "done"):
            steps[f"ag_{name}_{k}"] = functools.partial(getattr(ag, name), k)
        for name in ("r1", "r1b", "r2", "r2b", "r3", "done"):
            steps[f"rs_{name}_{k}"] = functools.partial(getattr(rs, name), k)
    for key, buf in (("a1", a1), ("da", da)):
        spread = Spread(wires, buf)
        for i in range(2):
            steps[f"{key}_start_{i}"] = functools.partial(spread.start, i)
            steps[f"{key}_relay_{i}"] = functools.partial(spread.relay, i)
        steps[f"{key}_own_half"] = spread.own_half
        steps[f"{key}_done"] = spread.done
    for key, buf in (("dm", dm), ("a2", a2)):
        spread = RingSpread(wires, buf)
        for i in range(2):
            steps[f"{key}_start_{i}"] = functools.partial(spread.start, i)
            steps[f"{key}_relay_{i}"] = functools.partial(spread.relay, i)
        for name in ("relay_far", "own_half", "done", "done_far", "release"):
            steps[f"{key}_{name}"] = getattr(spread, name)
    reds = {"att": Collect(wires, part, pair, cross), "da1": Collect(wires, part, pair, cross)}
    for key, red in reds.items():
        for name in ("other", "own", "send", "release"):
            steps[f"{key}_{name}"] = getattr(red, name)
        for i in range(2):
            steps[f"{key}_wait_{i}"] = functools.partial(red.wait, i)
    reds["da2"] = RingCollect(wires, ring_part, pair0, half0, full0)
    reds["ffn"] = RingCollect(wires, dm, pair1, half1, full1)
    for key in ("da2", "ffn"):
        red = reds[key]
        for name in STEPS:
            steps[f"{key}_give_{name}"] = functools.partial(red.give, name)
            steps[f"{key}_take_{name}"] = functools.partial(red.take, name)
        steps[f"{key}_pass_on"] = red.pass_on
        steps[f"{key}_wait"] = red.wait

    @step
    def load_first():
        for load in loads[:3]:
            load.wait()

    steps["met"] = met

    @step
    def load_inputs():
        inputs[0].wait()
        inputs[1].wait()

    @step
    def load_rest():
        for load in loads[3:]:
            load.wait()
        inputs[2].wait()

    def first_norm(r):
        n1, _ = normalize(x_ref[pl.ds(r, BLOCK), :].astype(F32))
        a1[own(r)] = (n1 * (1.0 + mod(1)) + mod(0)).astype(BF)

    def second_norm(r):
        rows = pl.ds(r, BLOCK)
        value = x_ref[rows, :].astype(F32) + mod(2) * reds["att"].rows(r, BLOCK)
        mid[rows, :] = value
        n2, _ = normalize(value)
        a2[ring_own(r)] = (n2 * (1.0 + mod(4)) + mod(3)).astype(BF)

    def mid_grad(r):
        rows = pl.ds(r, BLOCK)
        n2, r2 = normalize(mid[rows, :])
        inner = norm_back(n2, r2, reds["da2"].rows(r, BLOCK) * (1.0 + mod(4)))
        value = og_ref[rows, :].astype(F32) + inner
        dmid[rows, :] = value
        da[own(r)] = (mod(2) * value).astype(BF)

    for i in range(2):
        for fn in (first_norm, second_norm, mid_grad):
            steps[f"{fn.__name__}_{i}"] = functools.partial(by_rows, fn, 64 * i, 64)

    @step
    def gate_grad():
        def rows(r):
            dm[ring_own(r)] = (mod(5) * og_ref[pl.ds(r, BLOCK), :].astype(F32)).astype(BF)

        by_rows(rows)

    def lanes(h, which):
        return pl.ds(384 * h + 128 * which, 128)

    def project(start, count):
        qkv[:, pl.ds(start, count)] = nn(a1[...], weights(start, count)).astype(BF)

    for h in range(3):

        def project_head(h=h):
            project(384 * h, 384)

        steps[f"project_{h}"] = project_head

    def attend(h, start):
        rows = rows_of(start, 256)
        s = nt(qkv[rows, lanes(h, 0)], qkv[:, lanes(h, 1)])
        e = jnp.exp(factor * (s - jnp.max(s, axis=-1, keepdims=True)))
        p = (e * (1.0 / jnp.sum(e, axis=-1, keepdims=True))).astype(BF)
        probs[h, rows, :] = p
        o[rows, pl.ds(128 * h, 128)] = nn(p, qkv[:, lanes(h, 2)]).astype(BF)

    for h in range(3):
        steps[f"attend_{h}_other"] = functools.partial(attend, h, other_start)
        steps[f"attend_{h}_own"] = functools.partial(attend, h, own_start)

    def back_half(dst, lhs, start, at, count):
        rows = rows_of(start, 256)

        for j in range(2):
            rhs = w[2 * j : 2 * j + 2, :, pl.ds(at, count)].reshape(768, count)
            dst[rows, pl.ds(768 * j, 768)] = nt(lhs[rows, :], rhs).astype(BF)

    for key, dst, lhs, at, count in (("att", part, o, 1152, 384), ("da1", part, qkv, 0, 1152)):
        steps[f"{key}_mm_other"] = functools.partial(back_half, dst, lhs, other_start, at, count)
        steps[f"{key}_mm_own"] = functools.partial(back_half, dst, lhs, own_start, at, count)

    def quarter(name):
        at_xh, at_xl = chip(STEPS[name])
        return 512 * at_xh + 256 * at_xl

    def hidden(name):
        rows = rows_of(quarter(name), 256)

        for at in range(0, 768, 256):
            u = nn(a2[rows, :], weights(1536 + at, 256))
            sq = u * u
            t = jnp.tanh(u * (ROOT + (ROOT * 0.044715) * sq))
            half = 0.5 + 0.5 * t
            act[rows, pl.ds(at, 256)] = (u * half).astype(BF)
            inner = (0.5 * ROOT) + (1.5 * ROOT * 0.044715) * sq
            gp[rows, pl.ds(at, 256)] = (half + u * inner * (1.0 - t * t)).astype(BF)

    def hidden_grad(name):
        rows = rows_of(quarter(name), 256)

        for at in range(0, 768, 256):
            cols = pl.ds(at, 256)
            dg = nn(dm[rows, :], weights(2304 + at, 256))
            gp[rows, cols] = (gp[rows, cols].astype(F32) * dg).astype(BF)

    for name in STEPS:
        steps[f"hidden_{name}"] = functools.partial(hidden, name)
        steps[f"hgrad_{name}"] = functools.partial(hidden_grad, name)
        steps[f"da2_mm_{name}"] = functools.partial(back_half, ring_part, gp, quarter(name), 1536, 768)
        steps[f"ffn_mm_{name}"] = functools.partial(back_half, dm, act, quarter(name), 2304, 768)

    def grad(left, right, right_at, at, count, planes=(0, 4)):
        for j in range(*planes):
            lhs = left[:, pl.ds(384 * j, 384)]
            value = tn(lhs, right[:, pl.ds(right_at, count)]) * scale
            g[j, :, pl.ds(at, count)] = value.astype(BF)

    for i in range(2):
        steps[f"grad_in_{i}"] = functools.partial(grad, a2, gp, 0, 1536, 768, (2 * i, 2 * i + 2))
        steps[f"grad_back_{i}"] = functools.partial(grad, dm, act, 0, 2304, 768, (2 * i, 2 * i + 2))
    steps["grad_out"] = functools.partial(grad, da, o, 0, 1152, 384)
    for h in range(3):
        steps[f"grad_q_{h}"] = functools.partial(grad, a1, qkv, 384 * h, 384 * h, 384)

    def head_grads(start):
        rows = rows_of(start, 256)
        do[rows, :] = nn(da[rows, :], weights(1152, 384)).astype(BF)

    steps["heads_own"] = functools.partial(head_grads, own_start)
    steps["heads_other"] = functools.partial(head_grads, other_start)

    def attend_back(h):
        dv[...] = tn(probs[h], do[:, pl.ds(128 * h, 128)]).astype(BF)
        for i in range(4):
            rows = pl.ds(i * 128, 128)
            dp = nt(do[rows, pl.ds(128 * h, 128)], qkv[:, lanes(h, 2)])
            p = probs[h, rows, :].astype(F32)
            ds = factor * p * (dp - jnp.sum(p * dp, axis=-1, keepdims=True))
            probs[h, rows, :] = ds.astype(BF)
        dk = tn(probs[h], qkv[:, lanes(h, 0)]).astype(BF)
        qkv[:, lanes(h, 0)] = nn(probs[h], qkv[:, lanes(h, 1)]).astype(BF)
        qkv[:, lanes(h, 1)] = dk
        qkv[:, lanes(h, 2)] = dv[...]

    for h in range(3):
        steps[f"attend_back_{h}"] = functools.partial(attend_back, h)

    @step
    def last_out():
        def each(r):
            rows = pl.ds(r, BLOCK)
            final_ref[rows, :] = (mid[rows, :] + mod(5) * reds["ffn"].rows(r, BLOCK)).astype(BF)

        by_rows(each)

    @step
    def first_grad():
        def each(r):
            rows = pl.ds(r, BLOCK)
            n1, r1 = normalize(x_ref[rows, :].astype(F32))
            inner = norm_back(n1, r1, reds["da1"].rows(r, BLOCK) * (1.0 + mod(1)))
            ig_ref[rows, :] = dmid[rows, :] + inner

        by_rows(each)

    @step
    def finish():
        wires.drain()

    names = list(steps)
    for at in ORDER:
        with jax.named_scope(names[at]):
            steps[names[at]]()


def finish_kernel(final, ig, sums, final_out, ig_out, gq_out, go_out, gi_out, gb_out, sem):
    cuts = [(384 * which, 384, gq_out.at[which]) for which in range(3)]
    cuts += [(1152, 384, go_out), (1536, 1536, gi_out), (3072, 1536, gb_out)]
    pairs = [(sums.at[:, pl.ds(at, n)], out) for at, n, out in cuts]
    pairs += [(ig, ig_out), (final, final_out)]
    stores = [pltpu.make_async_copy(held, out, sem.at[i]) for i, (held, out) in enumerate(pairs)]
    for store in stores:
        store.start()
    for store in stores:
        store.wait()


def body(tokens, modulation, w_qkv, w_out, w_in, w_back, out_grad):
    own = w_qkv.shape[3]
    far = pl.BlockSpec(memory_space=pl.ANY)
    near_memory = pl.BlockSpec(memory_space=pltpu.VMEM)
    copies = 34 * len(CHUNKS) + 2 * 6 + 2 * 4 + 2 * 14 + 2 * 10
    rows = lambda n, count=512: pltpu.VMEM((count, n), BF)
    final, grad_in_rows, sums = pl.pallas_call(
        block_kernel,
        out_shape=(
            pltpu.VMEM((128, 1536), BF),
            pltpu.VMEM((128, 1536), F32),
            pltpu.VMEM((48, WIDTH), F32),
        ),
        in_specs=[far] * 7,
        out_specs=(near_memory,) * 3,
        scratch_shapes=[
            pltpu.VMEM((128, 1536), BF),
            pltpu.VMEM((6, 1, 1536), F32),
            pltpu.VMEM((128, 1536), BF),
            pltpu.VMEM((4, 384, HELD), BF),
            pltpu.VMEM((4, 384, HELD), BF),
            pltpu.VMEM((48, HELD), BF),
            pltpu.VMEM((48, 1536), BF),
            rows(1536), rows(1536, 1024), rows(1536, 1024), rows(1536),
            rows(1152), rows(384), rows(384),
            rows(768, 1024), rows(768, 1024), rows(1536), rows(1536, 1024),
            pltpu.VMEM((3, 512, 512), BF),
            pltpu.VMEM((512, 128), BF),
            pltpu.VMEM((2, 128, 1536), BF),
            pltpu.VMEM((128, 1536), BF),
            pltpu.VMEM((4, 128, 1536), BF),
            pltpu.VMEM((2, 64, 1536), BF),
            pltpu.VMEM((2, 128, 1536), BF),
            pltpu.VMEM((4, 128, 1536), BF),
            pltpu.VMEM((2, 64, 1536), BF),
            pltpu.VMEM((2, 128, 1536), BF),
            pltpu.VMEM((128, 1536), F32),
            pltpu.VMEM((128, 1536), F32),
            pltpu.SemaphoreType.DMA((copies,)),
            pltpu.SemaphoreType.DMA((copies,)),
            pltpu.SemaphoreType.DMA((20,)),
            *scatter_buffers(),
        ],
        compiler_params=pltpu.CompilerParams(
            collective_id=0, has_side_effects=True, vmem_limit_bytes=VMEM_LIMIT
        ),
        name="block",
    )(
        tokens[0],
        modulation[0].transpose(1, 0, 2),
        out_grad[0],
        w_qkv[0].transpose(1, 0, 2),
        w_out[0].T,
        w_in[0],
        w_back[0].T,
    )
    outs = pl.pallas_call(
        finish_kernel,
        out_shape=(
            jax.ShapeDtypeStruct((128, 1536), BF),
            jax.ShapeDtypeStruct((128, 1536), F32),
            jax.ShapeDtypeStruct((3, 48, own), F32),
            jax.ShapeDtypeStruct((48, own), F32),
            jax.ShapeDtypeStruct((48, 4 * own), F32),
            jax.ShapeDtypeStruct((48, 4 * own), F32),
        ),
        in_specs=[near_memory] * 3,
        out_specs=(far,) * 6,
        scratch_shapes=[pltpu.SemaphoreType.DMA((8,))],
        name="finish",
    )(*(pltpu.with_memory_space_constraint(held, pltpu.VMEM) for held in (final, grad_in_rows, sums)))
    final, grad_in_rows, gq, go, gi, gb = outs
    return (final[None], grad_in_rows[None], gq.transpose(1, 0, 2)[None], go.T[None], gi[None], gb.T[None])


def solution(mesh):
    torus = Mesh(mesh.devices.reshape(4, 4, 2, 2, 2), FSDP + SP)
    return jax.shard_map(
        body,
        mesh=torus,
        in_specs=(
            P(FSDP, SP, None),
            P(FSDP, None, None, None),
            P(None, FSDP, None, SP),
            P(None, SP, FSDP),
            P(None, FSDP, SP),
            P(None, SP, FSDP),
            P(FSDP, SP, None),
        ),
        out_specs=(
            P(FSDP, SP, None),
            P(FSDP, SP, None),
            P(None, FSDP, None, SP),
            P(None, SP, FSDP),
            P(None, FSDP, SP),
            P(None, SP, FSDP),
        ),
        check_vma=False,
    )
```

```python
import functools
import math

import jax
import jax.numpy as jnp
from jax import lax
from jax.experimental import pallas as pl
from jax.experimental.pallas import tpu as pltpu
from jax.sharding import Mesh
from jax.sharding import PartitionSpec as P

HEAD_DIM = 128
MESH = pl.DeviceIdType.MESH
FSDP = ("z", "y", "xh")
SP = ("xl", "c")
BF = jnp.bfloat16
F32 = jnp.float32

ln_eps = 1e-06
temper = 2.5
VMEM_LIMIT = 64_500_000

TILES = ((2, 1), (1, 2), (2, 1), (1, 2), (3, 3), (3, 3))
OUT, IN, BACK = 3, 4, 5


def split_chunks():
    chunks, at = [], 0
    for tiles in TILES:
        parts = []
        for count in tiles:
            parts.append((at, 128 * count))
            at += 128 * count
        chunks.append(tuple(parts))
    return tuple(chunks)


CHUNKS = split_chunks()
HELD = 3072
STEPS = {"own": 0, "next": 1, "prev": -1, "far": 2}
WIDTH = 4608
ORDER = (
    134, 137, 136, 141, 144, 135,
    0, 12, 36, 24, 138, 48,
    84, 86, 72, 74, 60, 1,
    76, 13, 37, 25, 2, 49,
    14, 89, 38, 26, 3, 15,
    27, 85, 87, 39, 73, 16,
    90, 4, 28, 75, 40, 61,
    88, 77, 50, 17, 146, 150,
    5, 145, 148, 29, 147, 41,
    152, 154, 102, 149, 62, 153,
    91, 51, 104, 151, 63, 155,
    103, 106, 139, 93, 52, 107,
    142, 95, 98, 64, 92, 94,
    105, 53, 96, 158, 99, 162,
    65, 166, 97, 163, 100, 170,
    171, 172, 120, 167, 168, 118,
    121, 164, 116, 175, 119, 177,
    66, 117, 159, 176, 174, 54,
    122, 165, 126, 160, 114, 161,
    124, 67, 173, 130, 169, 128,
    115, 123, 140, 125, 78, 143,
    80, 129, 127, 131, 55, 82,
    182, 68, 79, 81, 56, 69,
    83, 178, 183, 42, 186, 181,
    30, 185, 180, 18, 184, 43,
    70, 179, 6, 132, 156, 108,
    19, 31, 157, 110, 133, 71,
    7, 44, 109, 187, 20, 32,
    57, 8, 21, 33, 45, 112,
    58, 9, 113, 22, 188, 34,
    46, 10, 59, 47, 23, 35,
    11, 189,
)


def turn(axis, step, size):
    return {axis: lax.rem(lax.axis_index(axis) + step + size, size)}


def near(axis, step):
    return lax.rem(lax.axis_index(axis) + step + 4, 4)


class Wires:
    def __init__(self, send, recv):
        self.send, self.recv, self.used, self.open = send, recv, 0, []

    def go(self, src, dst, device):
        at = self.used
        self.used += 1
        copy = pltpu.make_async_remote_copy(
            src_ref=src,
            dst_ref=dst,
            send_sem=self.send.at[at],
            recv_sem=self.recv.at[at],
            device_id=device,
            device_id_type=MESH,
        )
        copy.start()
        self.open.append(copy)
        return copy

    def sent(self, copy):
        copy.wait_send()
        self.open = [other for other in self.open if other is not copy]

    def drain(self):
        for copy in self.open:
            copy.wait_send()
        self.open = []


def chip(step):
    xh, xl = lax.axis_index("xh"), lax.axis_index("xl")
    if step == 0:
        return xh, xl
    if step == 2:
        return 1 - xh, xl
    return lax.rem(xh + xl + (0 if step == 1 else 1), 2), 1 - xl


def along(step):
    xh, xl = chip(step)
    return {"xh": xh, "xl": xl}


def partners():
    return [turn("z", 1, 4), turn("z", -1, 4), turn("y", 1, 4), turn("y", -1, 4)] + [
        turn("xh", 1, 2), turn("c", 1, 2), along(1), along(-1)
    ]


def greet():
    for device in partners():
        pl.semaphore_signal(
            pltpu.get_barrier_semaphore(), inc=1, device_id=device, device_id_type=MESH
        )


def met():
    pl.semaphore_wait(pltpu.get_barrier_semaphore(), len(partners()))


def rows_of(start, count):
    return pl.ds(pl.multiple_of(start, 16), count)


def cols_of(cols):
    return pl.ds(cols[0], cols[1])


class Gather:
    def __init__(self, wires, w, stage):
        self.wires, self.w, self.stage = wires, w, stage
        self.z, self.y, self.xh = (lax.axis_index(a) for a in FSDP)
        self.one, self.two, self.relay2, self.three, self.relay3 = {}, {}, {}, {}, {}

    def same(self, part, device):
        return self.wires.go(part, part, device)

    def s1(self, k):
        (a0, an), (b0, bn) = CHUNKS[k]
        part = self.w.at[self.z, rows_of(96 * self.y + 48 * self.xh, 48), pl.ds(a0, an + bn)]
        source = part if k < IN else self.stage.at[:, pl.ds(a0 - 1536, an + bn)]
        self.one[k] = self.wires.go(source, part, turn("xh", 1, 2))

    def s2(self, k):
        self.one[k].wait_recv()
        ca, cb = map(cols_of, CHUNKS[k])
        pa = self.w.at[self.z, rows_of(96 * self.y, 96), ca]
        pb = self.w.at[self.z, rows_of(96 * self.y, 96), cb]
        self.two[k] = [
            self.same(pa, turn("y", 1, 4)),
            self.same(pa, turn("y", -1, 4)),
            self.same(pb, turn("z", 1, 4)),
            self.same(pb, turn("z", -1, 4)),
        ]

    def s2b(self, k):
        ca, cb = map(cols_of, CHUNKS[k])
        for copy in self.two[k]:
            copy.wait_recv()
        w, z, y = self.w, self.z, self.y
        self.relay2[k] = [
            self.same(w.at[z, rows_of(96 * near("y", -1), 48), ca], turn("y", 1, 4)),
            self.same(w.at[z, rows_of(96 * near("y", 1) + 48, 48), ca], turn("y", -1, 4)),
            self.same(w.at[near("z", -1), rows_of(96 * y, 48), cb], turn("z", 1, 4)),
            self.same(w.at[near("z", 1), rows_of(96 * y + 48, 48), cb], turn("z", -1, 4)),
        ]

    def s3(self, k):
        ca, cb = map(cols_of, CHUNKS[k])
        for copy in self.relay2[k]:
            copy.wait_recv()
        pa = self.w.at[self.z, :, ca]
        pb = self.w.at[:, rows_of(96 * self.y, 96), cb]
        self.three[k] = [
            self.same(pa, turn("z", 1, 4)),
            self.same(pa, turn("z", -1, 4)),
            self.same(pb, turn("y", 1, 4)),
            self.same(pb, turn("y", -1, 4)),
        ]

    def s3b(self, k):
        ca, cb = map(cols_of, CHUNKS[k])
        for copy in self.three[k]:
            copy.wait_recv()
        w = self.w
        self.relay3[k] = [
            self.same(w.at[near("z", -1), pl.ds(0, 192), ca], turn("z", 1, 4)),
            self.same(w.at[near("z", 1), pl.ds(192, 192), ca], turn("z", -1, 4)),
            self.same(w.at[:, rows_of(96 * near("y", -1), 48), cb], turn("y", 1, 4)),
            self.same(w.at[:, rows_of(96 * near("y", 1) + 48, 48), cb], turn("y", -1, 4)),
        ]

    def done(self, k):
        for copy in self.relay3[k]:
            copy.wait_recv()


def add_into(dst, *srcs):
    planes, rows, columns = dst.shape

    @pl.loop(0, planes * (rows // 48))
    def _(i):
        at = (i // (rows // 48), pl.ds(pl.multiple_of((i % (rows // 48)) * 48, 48), 48), slice(None))
        total = dst[at].astype(F32)
        for src in srcs:
            total = total + src[at].astype(F32)
        dst[at] = total.astype(dst.dtype)


class Scatter:
    def __init__(self, wires, g, half_a, full_a, half_b, full_b, half2, full2, last, out):
        self.wires, self.g, self.out = wires, g, out
        self.half_a, self.full_a, self.half_b, self.full_b = half_a, full_a, half_b, full_b
        self.half2, self.full2, self.last = half2, full2, last
        self.z, self.y, self.xh = (lax.axis_index(a) for a in FSDP)
        self.copies = {}

    def block_a(self, step, start, count, cols):
        return self.g.at[pl.ds(near("z", step), 1), pl.ds(start, count), cols]

    def block_b(self, step, start, count, cols):
        return self.g.at[:, rows_of(96 * near("y", step) + start, count), cols]

    def sub_a(self, step, start, count, cols):
        return self.g.at[pl.ds(self.z, 1), rows_of(96 * near("y", step) + start, count), cols]

    def sub_b(self, step, start, count, cols):
        return self.g.at[pl.ds(near("z", step), 1), rows_of(96 * self.y + start, count), cols]

    def r1(self, k):
        ca, cb = map(cols_of, CHUNKS[k])
        go = self.wires.go
        self.copies[k, 1] = [
            go(self.block_a(2, 0, 192, ca), self.half_a[k].at[pl.ds(0, 1)], turn("z", 1, 4)),
            go(self.block_a(2, 192, 192, ca), self.half_a[k].at[pl.ds(1, 1)], turn("z", -1, 4)),
            go(self.block_b(2, 0, 48, cb), self.half_b[k].at[0], turn("y", 1, 4)),
            go(self.block_b(2, 48, 48, cb), self.half_b[k].at[1], turn("y", -1, 4)),
        ]

    def r1b(self, k):
        ca, cb = map(cols_of, CHUNKS[k])
        go, copies = self.wires.go, self.copies[k, 1]
        sent = []
        copies[0].wait_recv()
        add_into(self.block_a(1, 0, 192, ca), self.half_a[k].at[pl.ds(0, 1)])
        sent.append(go(self.block_a(1, 0, 384, ca), self.full_a[k].at[pl.ds(0, 1)], turn("z", 1, 4)))
        copies[1].wait_recv()
        add_into(self.block_a(-1, 192, 192, ca), self.half_a[k].at[pl.ds(1, 1)])
        sent.append(go(self.block_a(-1, 0, 384, ca), self.full_a[k].at[pl.ds(1, 1)], turn("z", -1, 4)))
        copies[2].wait_recv()
        add_into(self.block_b(1, 0, 48, cb), self.half_b[k].at[0])
        sent.append(go(self.block_b(1, 0, 96, cb), self.full_b[k].at[0], turn("y", 1, 4)))
        copies[3].wait_recv()
        add_into(self.block_b(-1, 48, 48, cb), self.half_b[k].at[1])
        sent.append(go(self.block_b(-1, 0, 96, cb), self.full_b[k].at[1], turn("y", -1, 4)))
        self.copies[k, 2] = sent

    def r2(self, k):
        ca, cb = map(cols_of, CHUNKS[k])
        go, copies = self.wires.go, self.copies[k, 2]
        copies[0].wait_recv()
        copies[1].wait_recv()
        add_into(
            self.block_a(0, 0, 384, ca), self.full_a[k].at[pl.ds(0, 1)], self.full_a[k].at[pl.ds(1, 1)]
        )
        sent = [
            go(self.sub_a(2, 0, 48, ca), self.half2[k][0].at[pl.ds(0, 1)], turn("y", 1, 4)),
            go(self.sub_a(2, 48, 48, ca), self.half2[k][0].at[pl.ds(1, 1)], turn("y", -1, 4)),
        ]
        copies[2].wait_recv()
        copies[3].wait_recv()
        add_into(self.block_b(0, 0, 96, cb), self.full_b[k].at[0], self.full_b[k].at[1])
        sent += [
            go(self.sub_b(2, 0, 48, cb), self.half2[k][1].at[pl.ds(0, 1)], turn("z", 1, 4)),
            go(self.sub_b(2, 48, 48, cb), self.half2[k][1].at[pl.ds(1, 1)], turn("z", -1, 4)),
        ]
        self.copies[k, 3] = sent

    def r2b(self, k):
        go, copies = self.wires.go, self.copies[k, 3]
        sent = []
        for colour, (sub, axis) in enumerate(((self.sub_a, "y"), (self.sub_b, "z"))):
            cols = cols_of(CHUNKS[k][colour])
            half, full = self.half2[k][colour], self.full2[k][colour]
            copies[2 * colour].wait_recv()
            add_into(sub(1, 0, 48, cols), half.at[pl.ds(0, 1)])
            sent.append(go(sub(1, 0, 96, cols), full.at[pl.ds(0, 1)], turn(axis, 1, 4)))
            copies[2 * colour + 1].wait_recv()
            add_into(sub(-1, 48, 48, cols), half.at[pl.ds(1, 1)])
            sent.append(go(sub(-1, 0, 96, cols), full.at[pl.ds(1, 1)], turn(axis, -1, 4)))
        self.copies[k, 4] = sent

    def r3(self, k):
        go, copies = self.wires.go, self.copies[k, 4]
        (a0, an), (b0, bn) = CHUNKS[k]
        for colour, sub in enumerate((self.sub_a, self.sub_b)):
            cols, full = cols_of(CHUNKS[k][colour]), self.full2[k][colour]
            copies[2 * colour].wait_recv()
            copies[2 * colour + 1].wait_recv()
            add_into(sub(0, 0, 96, cols), full.at[pl.ds(0, 1)], full.at[pl.ds(1, 1)])
        part = self.g.at[self.z, rows_of(96 * self.y + 48 * (1 - self.xh), 48), pl.ds(a0, an + bn)]
        self.copies[k, 5] = [go(part, self.last.at[:, pl.ds(a0, an + bn)], turn("xh", 1, 2))]

    def done(self, k):
        (a0, an), (b0, bn) = CHUNKS[k]
        self.copies[k, 5][0].wait_recv()
        cols = pl.ds(a0, an + bn)
        own = self.g[self.z, rows_of(96 * self.y + 48 * self.xh, 48), cols].astype(F32)
        came = self.last[:, cols].astype(F32)
        if k >= IN:
            base = 1536 * (k - OUT)
            self.out[:, pl.ds(pl.multiple_of(base + 768 * self.xh, 128), 768)] = own
            self.out[:, pl.ds(pl.multiple_of(base + 768 * (1 - self.xh), 128), 768)] = came
            return
        total = own + came
        if k == OUT:
            self.out[:, cols] = total
            return
        for at in range(0, an + bn, 128):
            head, which = (a0 + at) // 384, (a0 + at) % 384 // 128
            self.out[:, pl.ds(384 * which + 128 * head, 128)] = total[:, at : at + 128]


def scatter_buffers():
    shapes = []
    for (_, an), (_, bn) in CHUNKS:
        shapes += [
            pltpu.VMEM((2, 192, an), BF),
            pltpu.VMEM((2, 384, an), BF),
            pltpu.VMEM((2, 4, 48, bn), BF),
            pltpu.VMEM((2, 4, 96, bn), BF),
            pltpu.VMEM((2, 48, an), BF),
            pltpu.VMEM((2, 96, an), BF),
            pltpu.VMEM((2, 48, bn), BF),
            pltpu.VMEM((2, 96, bn), BF),
        ]
    return shapes


def make_scatter(wires, g, bufs, last, out):
    groups = [bufs[8 * k : 8 * k + 8] for k in range(len(CHUNKS))]
    return Scatter(
        wires,
        g,
        [b[0] for b in groups],
        [b[1] for b in groups],
        [b[2] for b in groups],
        [b[3] for b in groups],
        [(b[4], b[6]) for b in groups],
        [(b[5], b[7]) for b in groups],
        last,
        out,
    )


def nn(a, b):
    return jnp.dot(a, b, preferred_element_type=F32)


def nt(a, b):
    return lax.dot_general(a, b, (((1,), (1,)), ((), ())), preferred_element_type=F32)


def tn(a, b):
    return lax.dot_general(a, b, (((0,), (0,)), ((), ())), preferred_element_type=F32)


class Spread:
    def __init__(self, wires, buf):
        self.wires, self.buf = wires, buf
        self.xl, self.c = (lax.axis_index(a) for a in SP)
        self.far, self.near, self.relays = {}, {}, {}

    def block(self, xl, c, start=0, count=128):
        return self.buf.at[rows_of(256 * xl + 128 * c + start, count), :]

    def start(self, i):
        part = self.block(self.xl, self.c, 64 * i, 64)
        self.far[i] = self.wires.go(part, part, turn("xl", 1, 2))
        self.near[i] = self.wires.go(part, part, turn("c", 1, 2))

    def relay(self, i):
        self.far[i].wait_recv()
        part = self.block(1 - self.xl, self.c, 64 * i, 64)
        self.relays[i] = self.wires.go(part, part, turn("c", 1, 2))

    def own_half(self):
        for copy in self.near.values():
            copy.wait_recv()

    def done(self):
        for copy in self.relays.values():
            copy.wait_recv()

    def release(self):
        for group in (self.far, self.near, self.relays):
            for copy in group.values():
                self.wires.sent(copy)


class Collect:
    def __init__(self, wires, part, pair, cross):
        self.wires, self.part, self.pair, self.cross = wires, part, pair, cross
        self.xl, self.c = (lax.axis_index(a) for a in SP)

    def block(self, xl, c):
        return self.part.at[rows_of(256 * xl + 128 * c, 128), :]

    def other(self):
        self.first = self.wires.go(self.block(1 - self.xl, 1 - self.c), self.pair.at[0], turn("c", 1, 2))

    def send(self):
        self.first.wait_recv()
        self.third = []
        for i in range(2):
            rows = pl.ds(64 * i, 64)
            mine = self.block(1 - self.xl, self.c).at[rows, :]
            add2(mine, self.pair.at[0, rows, :])
            self.third.append(self.wires.go(mine, self.cross.at[rows, :], turn("xl", 1, 2)))

    def own(self):
        self.second = self.wires.go(self.block(self.xl, 1 - self.c), self.pair.at[1], turn("c", 1, 2))

    def wait(self, i):
        if i == 0:
            self.second.wait_recv()
        self.third[i].wait_recv()

    def release(self):
        for copy in (self.first, self.second, *self.third):
            self.wires.sent(copy)

    def rows(self, start, count):
        at = rows_of(256 * self.xl + 128 * self.c + start, count)
        total = self.part[at, :].astype(F32) + self.pair[1, pl.ds(start, count), :].astype(F32)
        return total + self.cross[pl.ds(start, count), :].astype(F32)


class RingSpread:
    def __init__(self, wires, buf):
        self.wires, self.buf, self.c = wires, buf, lax.axis_index("c")
        self.sent = {}

    def part(self, step, i):
        xh, xl = chip(step)
        return self.buf.at[rows_of(512 * xh + 256 * xl + 128 * self.c + 64 * i, 64), :]

    def go(self, key, step, i, device):
        self.sent[key] = self.wires.go(self.part(step, i), self.part(step, i), device)

    def start(self, i):
        self.go(("next", i), 0, i, along(1))
        self.go(("prev", i), 0, i, along(-1))
        self.go(("own", i), 0, i, turn("c", 1, 2))

    def side(self, name, step, i):
        self.sent[name, i].wait_recv()
        if (name, i) in (("next", 0), ("prev", 1)):
            self.go(("far", i), step, i, along(-step))
        self.go(("core", step, i), step, i, turn("c", 1, 2))

    def relay(self, i):
        if i == 0:
            self.side("next", -1, 0)
            self.side("prev", 1, 1)
        else:
            self.side("next", -1, 1)
            self.side("prev", 1, 0)

    def relay_far(self):
        for i in range(2):
            self.sent["far", i].wait_recv()
            self.go(("core", 2, i), 2, i, turn("c", 1, 2))

    def own_half(self):
        for i in range(2):
            self.sent["own", i].wait_recv()

    def done(self):
        for step in (1, -1):
            for i in range(2):
                self.sent["core", step, i].wait_recv()

    def done_far(self):
        for i in range(2):
            self.sent["core", 2, i].wait_recv()

    def release(self):
        for copy in self.sent.values():
            self.wires.sent(copy)


class RingCollect:
    def __init__(self, wires, part, pair, half, full):
        self.wires, self.part, self.pair, self.half, self.full = wires, part, pair, half, full
        self.c = lax.axis_index("c")
        self.sent = {}

    def block(self, step, c, start=0, count=128):
        xh, xl = chip(step)
        return self.part.at[rows_of(512 * xh + 256 * xl + 128 * c + start, count), :]

    def give(self, name):
        step = STEPS[name]
        self.sent[name] = self.wires.go(self.block(step, 1 - self.c), self.pair.at[step % 4], turn("c", 1, 2))

    def take(self, name):
        step = STEPS[name]
        self.sent[name].wait_recv()
        if step == 0:
            return
        add2(self.block(step, self.c), self.pair.at[step % 4])
        if step == 2:
            for i, way in enumerate((1, -1)):
                self.sent["half", way] = self.wires.go(
                    self.block(2, self.c, 64 * i, 64), self.half.at[i], along(way)
                )
            return
        i = 1 if step == 1 else 0
        self.sent["early", step] = self.wires.go(
            self.block(step, self.c, 64 * i, 64), self.full.at[1 - i, pl.ds(64 * i, 64), :], along(step)
        )

    def pass_on(self):
        for i, step in enumerate((1, -1)):
            self.sent["half", step].wait_recv()
            block = self.block(step, self.c, 64 * i, 64)
            add2(block, self.half.at[i])
            self.sent["late", step] = self.wires.go(
                block, self.full.at[i, pl.ds(64 * i, 64), :], along(step)
            )

    def wait(self):
        for step in (1, -1):
            self.sent["early", step].wait_recv()
            self.sent["late", step].wait_recv()

    def rows(self, start, count):
        xh, xl = chip(0)
        total = self.part[rows_of(512 * xh + 256 * xl + 128 * self.c + start, count), :].astype(F32)
        for ref in (self.pair.at[0], self.full.at[0], self.full.at[1]):
            total = total + ref[pl.ds(start, count), :].astype(F32)
        return total


def add2(dst, src):
    rows = dst.shape[0]

    @pl.loop(0, rows // 16)
    def _(i):
        at = (pl.ds(pl.multiple_of(i * 16, 16), 16), slice(None))
        dst[at] = (dst[at].astype(F32) + src[at].astype(F32)).astype(dst.dtype)


def normalize(stream):
    mean_part = jnp.mean(stream, axis=-1, keepdims=True)
    centred = stream - mean_part
    rstd = lax.rsqrt(jnp.mean(centred * centred, axis=-1, keepdims=True) + ln_eps)
    return (centred * rstd, rstd)


def norm_back(normed, rstd, incoming):
    first = jnp.mean(incoming, axis=-1, keepdims=True)
    second = jnp.mean(incoming * normed, axis=-1, keepdims=True)
    return rstd * (incoming - first - normed * second)


BLOCK = 16
ROOT = math.sqrt(2.0 / math.pi)


def by_rows(fn, start=0, count=128):
    for r in range(start, start + count, BLOCK):
        fn(r)


def block_kernel(
    x_in, m_in, og_in, wq_ref, wo_ref, wi_ref, wb_ref,
    final_ref, ig_ref, sums_ref,
    x_ref, m_ref, og_ref,
    w, g, last, stage, a1, dm, a2, da, qkv, o, do, gp, act, part, ring_part, probs, dv, pair, cross,
    pair0, half0, full0, pair1, half1, full1, mid, dmid, send, recv, local_sem, *bufs,
):
    z, y, xh, xl, c = (lax.axis_index(a) for a in FSDP + SP)
    shard_rows = rows_of(96 * y + 48 * xh, 48)
    pieces = [
        (wq_ref.at[which, :, pl.ds(128 * h, 128)], 384 * h + 128 * which, 128)
        for h in range(3)
        for which in range(3)
    ]
    mine = pl.ds(pl.multiple_of(768 * xh, 128), 768)
    theirs = pl.ds(pl.multiple_of(768 * (1 - xh), 128), 768)
    pieces += [(wo_ref, 1152, 384), (wi_ref.at[:, mine], 1536, 768), (wb_ref.at[:, mine], 2304, 768)]
    loads = [
        pltpu.make_async_copy(source, w.at[z, shard_rows, pl.ds(at, count)], local_sem.at[i])
        for i, (source, at, count) in enumerate(pieces)
    ]
    loads += [
        pltpu.make_async_copy(ref.at[:, theirs], stage.at[:, pl.ds(768 * i, 768)], local_sem.at[18 + i])
        for i, ref in enumerate((wi_ref, wb_ref))
    ]
    inputs = [
        pltpu.make_async_copy(a, b, local_sem.at[12 + i])
        for i, (a, b) in enumerate(((x_in, x_ref), (m_in, m_ref), (og_in, og_ref)))
    ]
    greet()
    for load in loads[:3] + inputs[:2] + loads[3:] + inputs[2:]:
        load.start()
    wires = Wires(send, recv)
    ag = Gather(wires, w, stage)
    rs = make_scatter(wires, g, bufs, last, sums_ref)
    own_row = 256 * xl + 128 * c
    own_start, other_start = 256 * xl, 256 * (1 - xl)
    scale = 1.0 / math.sqrt(32 * 512)
    factor = temper / math.sqrt(HEAD_DIM)
    steps = {}

    def step(fn):
        steps[fn.__name__] = fn
        return fn

    def mod(i):
        return m_ref[i]

    def own(start):
        return (rows_of(own_row + start, BLOCK), slice(None))

    def ring_own(start):
        return (rows_of(512 * xh + own_row + start, BLOCK), slice(None))

    def weights(start, count):
        return w[:, :, pl.ds(start, count)].reshape(1536, count)

    for k in range(len(CHUNKS)):
        for name in ("s1", "s2", "s2b", "s3", "s3b", "done"):
            steps[f"ag_{name}_{k}"] = functools.partial(getattr(ag, name), k)
        for name in ("r1", "r1b", "r2", "r2b", "r3", "done"):
            steps[f"rs_{name}_{k}"] = functools.partial(getattr(rs, name), k)
    for key, buf in (("a1", a1), ("da", da)):
        spread = Spread(wires, buf)
        for i in range(2):
            steps[f"{key}_start_{i}"] = functools.partial(spread.start, i)
            steps[f"{key}_relay_{i}"] = functools.partial(spread.relay, i)
        steps[f"{key}_own_half"] = spread.own_half
        steps[f"{key}_done"] = spread.done
    for key, buf in (("dm", dm), ("a2", a2)):
        spread = RingSpread(wires, buf)
        for i in range(2):
            steps[f"{key}_start_{i}"] = functools.partial(spread.start, i)
            steps[f"{key}_relay_{i}"] = functools.partial(spread.relay, i)
        for name in ("relay_far", "own_half", "done", "done_far", "release"):
            steps[f"{key}_{name}"] = getattr(spread, name)
    reds = {"att": Collect(wires, part, pair, cross), "da1": Collect(wires, part, pair, cross)}
    for key, red in reds.items():
        for name in ("other", "own", "send", "release"):
            steps[f"{key}_{name}"] = getattr(red, name)
        for i in range(2):
            steps[f"{key}_wait_{i}"] = functools.partial(red.wait, i)
    reds["da2"] = RingCollect(wires, ring_part, pair0, half0, full0)
    reds["ffn"] = RingCollect(wires, dm, pair1, half1, full1)
    for key in ("da2", "ffn"):
        red = reds[key]
        for name in STEPS:
            steps[f"{key}_give_{name}"] = functools.partial(red.give, name)
            steps[f"{key}_take_{name}"] = functools.partial(red.take, name)
        steps[f"{key}_pass_on"] = red.pass_on
        steps[f"{key}_wait"] = red.wait

    @step
    def load_first():
        for load in loads[:3]:
            load.wait()

    steps["met"] = met

    @step
    def load_inputs():
        inputs[0].wait()
        inputs[1].wait()

    @step
    def load_rest():
        for load in loads[3:]:
            load.wait()
        inputs[2].wait()

    def first_norm(r):
        n1, _ = normalize(x_ref[pl.ds(r, BLOCK), :].astype(F32))
        a1[own(r)] = (n1 * (1.0 + mod(1)) + mod(0)).astype(BF)

    def second_norm(r):
        rows = pl.ds(r, BLOCK)
        value = x_ref[rows, :].astype(F32) + mod(2) * reds["att"].rows(r, BLOCK)
        mid[rows, :] = value
        n2, _ = normalize(value)
        a2[ring_own(r)] = (n2 * (1.0 + mod(4)) + mod(3)).astype(BF)

    def mid_grad(r):
        rows = pl.ds(r, BLOCK)
        n2, r2 = normalize(mid[rows, :])
        inner = norm_back(n2, r2, reds["da2"].rows(r, BLOCK) * (1.0 + mod(4)))
        value = og_ref[rows, :].astype(F32) + inner
        dmid[rows, :] = value
        da[own(r)] = (mod(2) * value).astype(BF)

    for i in range(2):
        for fn in (first_norm, second_norm, mid_grad):
            steps[f"{fn.__name__}_{i}"] = functools.partial(by_rows, fn, 64 * i, 64)

    @step
    def gate_grad():
        def rows(r):
            dm[ring_own(r)] = (mod(5) * og_ref[pl.ds(r, BLOCK), :].astype(F32)).astype(BF)

        by_rows(rows)

    def lanes(h, which):
        return pl.ds(384 * h + 128 * which, 128)

    def project(start, count):
        qkv[:, pl.ds(start, count)] = nn(a1[...], weights(start, count)).astype(BF)

    for h in range(3):

        def project_head(h=h):
            project(384 * h, 384)

        steps[f"project_{h}"] = project_head

    def attend(h, start):
        rows = rows_of(start, 256)
        s = nt(qkv[rows, lanes(h, 0)], qkv[:, lanes(h, 1)])
        e = jnp.exp(factor * (s - jnp.max(s, axis=-1, keepdims=True)))
        p = (e * (1.0 / jnp.sum(e, axis=-1, keepdims=True))).astype(BF)
        probs[h, rows, :] = p
        o[rows, pl.ds(128 * h, 128)] = nn(p, qkv[:, lanes(h, 2)]).astype(BF)

    for h in range(3):
        steps[f"attend_{h}_other"] = functools.partial(attend, h, other_start)
        steps[f"attend_{h}_own"] = functools.partial(attend, h, own_start)

    def back_half(dst, lhs, start, at, count):
        rows = rows_of(start, 256)

        for j in range(2):
            rhs = w[2 * j : 2 * j + 2, :, pl.ds(at, count)].reshape(768, count)
            dst[rows, pl.ds(768 * j, 768)] = nt(lhs[rows, :], rhs).astype(BF)

    for key, dst, lhs, at, count in (("att", part, o, 1152, 384), ("da1", part, qkv, 0, 1152)):
        steps[f"{key}_mm_other"] = functools.partial(back_half, dst, lhs, other_start, at, count)
        steps[f"{key}_mm_own"] = functools.partial(back_half, dst, lhs, own_start, at, count)

    def quarter(name):
        at_xh, at_xl = chip(STEPS[name])
        return 512 * at_xh + 256 * at_xl

    def hidden(name):
        rows = rows_of(quarter(name), 256)

        for at in range(0, 768, 256):
            u = nn(a2[rows, :], weights(1536 + at, 256))
            sq = u * u
            t = jnp.tanh(u * (ROOT + (ROOT * 0.044715) * sq))
            half = 0.5 + 0.5 * t
            act[rows, pl.ds(at, 256)] = (u * half).astype(BF)
            inner = (0.5 * ROOT) + (1.5 * ROOT * 0.044715) * sq
            gp[rows, pl.ds(at, 256)] = (half + u * inner * (1.0 - t * t)).astype(BF)

    def hidden_grad(name):
        rows = rows_of(quarter(name), 256)

        for at in range(0, 768, 256):
            cols = pl.ds(at, 256)
            dg = nn(dm[rows, :], weights(2304 + at, 256))
            gp[rows, cols] = (gp[rows, cols].astype(F32) * dg).astype(BF)

    for name in STEPS:
        steps[f"hidden_{name}"] = functools.partial(hidden, name)
        steps[f"hgrad_{name}"] = functools.partial(hidden_grad, name)
        steps[f"da2_mm_{name}"] = functools.partial(back_half, ring_part, gp, quarter(name), 1536, 768)
        steps[f"ffn_mm_{name}"] = functools.partial(back_half, dm, act, quarter(name), 2304, 768)

    def grad(left, right, right_at, at, count, planes=(0, 4)):
        for j in range(*planes):
            lhs = left[:, pl.ds(384 * j, 384)]
            value = tn(lhs, right[:, pl.ds(right_at, count)]) * scale
            g[j, :, pl.ds(at, count)] = value.astype(BF)

    for i in range(2):
        steps[f"grad_in_{i}"] = functools.partial(grad, a2, gp, 0, 1536, 768, (2 * i, 2 * i + 2))
        steps[f"grad_back_{i}"] = functools.partial(grad, dm, act, 0, 2304, 768, (2 * i, 2 * i + 2))
    steps["grad_out"] = functools.partial(grad, da, o, 0, 1152, 384)
    for h in range(3):
        steps[f"grad_q_{h}"] = functools.partial(grad, a1, qkv, 384 * h, 384 * h, 384)

    def head_grads(start):
        rows = rows_of(start, 256)
        do[rows, :] = nn(da[rows, :], weights(1152, 384)).astype(BF)

    steps["heads_own"] = functools.partial(head_grads, own_start)
    steps["heads_other"] = functools.partial(head_grads, other_start)

    def attend_back(h):
        dv[...] = tn(probs[h], do[:, pl.ds(128 * h, 128)]).astype(BF)
        for i in range(4):
            rows = pl.ds(i * 128, 128)
            dp = nt(do[rows, pl.ds(128 * h, 128)], qkv[:, lanes(h, 2)])
            p = probs[h, rows, :].astype(F32)
            ds = factor * p * (dp - jnp.sum(p * dp, axis=-1, keepdims=True))
            probs[h, rows, :] = ds.astype(BF)
        dk = tn(probs[h], qkv[:, lanes(h, 0)]).astype(BF)
        qkv[:, lanes(h, 0)] = nn(probs[h], qkv[:, lanes(h, 1)]).astype(BF)
        qkv[:, lanes(h, 1)] = dk
        qkv[:, lanes(h, 2)] = dv[...]

    for h in range(3):
        steps[f"attend_back_{h}"] = functools.partial(attend_back, h)

    @step
    def last_out():
        def each(r):
            rows = pl.ds(r, BLOCK)
            final_ref[rows, :] = (mid[rows, :] + mod(5) * reds["ffn"].rows(r, BLOCK)).astype(BF)

        by_rows(each)

    @step
    def first_grad():
        def each(r):
            rows = pl.ds(r, BLOCK)
            n1, r1 = normalize(x_ref[rows, :].astype(F32))
            inner = norm_back(n1, r1, reds["da1"].rows(r, BLOCK) * (1.0 + mod(1)))
            ig_ref[rows, :] = dmid[rows, :] + inner

        by_rows(each)

    @step
    def finish():
        wires.drain()

    names = list(steps)
    for at in ORDER:
        with jax.named_scope(names[at]):
            steps[names[at]]()


def finish_kernel(final, ig, sums, final_out, ig_out, gq_out, go_out, gi_out, gb_out, sem):
    cuts = [(384 * which, 384, gq_out.at[which]) for which in range(3)]
    cuts += [(1152, 384, go_out), (1536, 1536, gi_out), (3072, 1536, gb_out)]
    pairs = [(sums.at[:, pl.ds(at, n)], out) for at, n, out in cuts]
    pairs += [(ig, ig_out), (final, final_out)]
    stores = [pltpu.make_async_copy(held, out, sem.at[i]) for i, (held, out) in enumerate(pairs)]
    for store in stores:
        store.start()
    for store in stores:
        store.wait()


def body(tokens, modulation, w_qkv, w_out, w_in, w_back, out_grad):
    own = w_qkv.shape[3]
    far = pl.BlockSpec(memory_space=pl.ANY)
    near_memory = pl.BlockSpec(memory_space=pltpu.VMEM)
    copies = 34 * len(CHUNKS) + 2 * 6 + 2 * 4 + 2 * 14 + 2 * 10
    rows = lambda n, count=512: pltpu.VMEM((count, n), BF)
    final, grad_in_rows, sums = pl.pallas_call(
        block_kernel,
        out_shape=(
            pltpu.VMEM((128, 1536), BF),
            pltpu.VMEM((128, 1536), F32),
            pltpu.VMEM((48, WIDTH), F32),
        ),
        in_specs=[far] * 7,
        out_specs=(near_memory,) * 3,
        scratch_shapes=[
            pltpu.VMEM((128, 1536), BF),
            pltpu.VMEM((6, 1, 1536), F32),
            pltpu.VMEM((128, 1536), BF),
            pltpu.VMEM((4, 384, HELD), BF),
            pltpu.VMEM((4, 384, HELD), BF),
            pltpu.VMEM((48, HELD), BF),
            pltpu.VMEM((48, 1536), BF),
            rows(1536), rows(1536, 1024), rows(1536, 1024), rows(1536),
            rows(1152), rows(384), rows(384),
            rows(768, 1024), rows(768, 1024), rows(1536), rows(1536, 1024),
            pltpu.VMEM((3, 512, 512), BF),
            pltpu.VMEM((512, 128), BF),
            pltpu.VMEM((2, 128, 1536), BF),
            pltpu.VMEM((128, 1536), BF),
            pltpu.VMEM((4, 128, 1536), BF),
            pltpu.VMEM((2, 64, 1536), BF),
            pltpu.VMEM((2, 128, 1536), BF),
            pltpu.VMEM((4, 128, 1536), BF),
            pltpu.VMEM((2, 64, 1536), BF),
            pltpu.VMEM((2, 128, 1536), BF),
            pltpu.VMEM((128, 1536), F32),
            pltpu.VMEM((128, 1536), F32),
            pltpu.SemaphoreType.DMA((copies,)),
            pltpu.SemaphoreType.DMA((copies,)),
            pltpu.SemaphoreType.DMA((20,)),
            *scatter_buffers(),
        ],
        compiler_params=pltpu.CompilerParams(
            collective_id=0, has_side_effects=True, vmem_limit_bytes=VMEM_LIMIT
        ),
        name="block",
    )(
        tokens[0],
        modulation[0].transpose(1, 0, 2),
        out_grad[0],
        w_qkv[0].transpose(1, 0, 2),
        w_out[0].T,
        w_in[0],
        w_back[0].T,
    )
    outs = pl.pallas_call(
        finish_kernel,
        out_shape=(
            jax.ShapeDtypeStruct((128, 1536), BF),
            jax.ShapeDtypeStruct((128, 1536), F32),
            jax.ShapeDtypeStruct((3, 48, own), F32),
            jax.ShapeDtypeStruct((48, own), F32),
            jax.ShapeDtypeStruct((48, 4 * own), F32),
            jax.ShapeDtypeStruct((48, 4 * own), F32),
        ),
        in_specs=[near_memory] * 3,
        out_specs=(far,) * 6,
        scratch_shapes=[pltpu.SemaphoreType.DMA((8,))],
        name="finish",
    )(*(pltpu.with_memory_space_constraint(held, pltpu.VMEM) for held in (final, grad_in_rows, sums)))
    final, grad_in_rows, gq, go, gi, gb = outs
    return (final[None], grad_in_rows[None], gq.transpose(1, 0, 2)[None], go.T[None], gi[None], gb.T[None])


def solution(mesh):
    torus = Mesh(mesh.devices.reshape(4, 4, 2, 2, 2), FSDP + SP)
    return jax.shard_map(
        body,
        mesh=torus,
        in_specs=(
            P(FSDP, SP, None),
            P(FSDP, None, None, None),
            P(None, FSDP, None, SP),
            P(None, SP, FSDP),
            P(None, FSDP, SP),
            P(None, SP, FSDP),
            P(FSDP, SP, None),
        ),
        out_specs=(
            P(FSDP, SP, None),
            P(FSDP, SP, None),
            P(None, FSDP, None, SP),
            P(None, SP, FSDP),
            P(None, FSDP, SP),
            P(None, SP, FSDP),
        ),
        check_vma=False,
    )
```
